8 devices in a mesh: dp: 2 (over z, y), tp: 4 (over x, core).
Axes of the slice: x: 2, y: 2, z: 1, core: 2. Of those that a mesh axis runs over, the one named last changes fastest.
Arguments:
- hidden: bfloat16 [4096, 576], P('dp')
- w_final: float32 [576], replicated
- emb_table: bfloat16 [49152, 576], P('tp')
- teacher: bfloat16 [4096, 49152], P('dp', 'tp')
- tok_mask: float32 [4096], P('dp')
Outputs:
- output 1: float32 [], replicated
- output 2: bfloat16 [4096, 576], P('dp')
- output 3: float32 [576], replicated
- output 4: float32 [49152, 576], P('tp')
All inputs are finite; a program needn't handle non-finite values.
Results may differ from the reference program's by a relative error of at most 0.00105127.
Values sent between devices are 32-bit elements.
A program may use at most 1 GiB of HBM per device.

```python
import math
import jax
import jax.numpy as jnp
from jax import lax

MODEL_DIM = 576
VOCAB_SIZE = 49152
NUM_TOKENS = 4096
SEQ_LEN = 16
ROW_BLOCK = math.gcd(NUM_TOKENS, 64)
SOFT_CAP = 30.0
NORM_EPS = 1e-6


def setup_inputs(seed: int = 0) -> dict:
    root_key = jax.random.key(seed)
    k_hid, k_gain, k_dir, k_tab, k_off, k_tea, k_seq, k_tok = jax.random.split(root_key, 8)
    fan_scale = 1.0 / math.sqrt(MODEL_DIM)
    hidden = 3.0 * jax.random.normal(k_hid, (NUM_TOKENS, MODEL_DIM), jnp.float32)
    w_final = 0.3 * jax.random.normal(k_gain, (MODEL_DIM,), jnp.float32)
    direction = 15.0 * fan_scale * jax.random.normal(k_dir, (MODEL_DIM,), jnp.float32)
    emb_table = direction[None, :] + 2.0 * fan_scale * jax.random.normal(k_tab, (VOCAB_SIZE, MODEL_DIM), jnp.float32)
    offset = 15.0 * jax.random.normal(k_off, (NUM_TOKENS, 1), jnp.float32)
    teacher = offset + 3.0 * jax.random.normal(k_tea, (NUM_TOKENS, VOCAB_SIZE), jnp.float32)
    seq_keep = (jax.random.randint(k_seq, (NUM_TOKENS // SEQ_LEN,), 0, 4) > 0).at[0].set(True)
    tok_keep = (jax.random.randint(k_tok, (NUM_TOKENS,), 0, 8) > 0).at[0].set(True)
    tok_mask = jnp.logical_and(jnp.repeat(seq_keep, SEQ_LEN), tok_keep).astype(jnp.float32)
    return {'hidden': hidden.astype(jnp.bfloat16), 'w_final': w_final, 'emb_table': emb_table.astype(jnp.bfloat16), 'teacher': teacher.astype(jnp.bfloat16), 'tok_mask': tok_mask}


def final_norm(hid_rows, w_final):
    hid_f = hid_rows.astype(jnp.float32)
    inv_rms = lax.rsqrt(jnp.mean(hid_f * hid_f, axis=-1, keepdims=True) + NORM_EPS)
    normed = hid_f * inv_rms
    return inv_rms, normed, (normed * (1.0 + w_final)).astype(jnp.bfloat16)


def reference(hidden, w_final, emb_table, teacher, tok_mask):
    mask_sum = jnp.sum(tok_mask)
    num_blocks = NUM_TOKENS // ROW_BLOCK
    hid_blocks = hidden.reshape(num_blocks, ROW_BLOCK, MODEL_DIM)
    tea_blocks = teacher.reshape(num_blocks, ROW_BLOCK, VOCAB_SIZE)
    mask_blocks = tok_mask.reshape(num_blocks, ROW_BLOCK)

    def block_step(scan_carry, block_in):
        loss_acc, gain_acc, table_acc = scan_carry
        hid_rows, tea_rows, mask_rows = block_in
        inv_rms, normed, x_rows = final_norm(hid_rows, w_final)
        logits = jnp.dot(x_rows, emb_table.T, preferred_element_type=jnp.float32)
        stu_cap = SOFT_CAP * jnp.tanh(logits / SOFT_CAP)
        tea_cap = SOFT_CAP * jnp.tanh(tea_rows.astype(jnp.float32) / SOFT_CAP)
        stu_logp = stu_cap - jax.nn.logsumexp(stu_cap, axis=-1, keepdims=True)
        tea_logp = tea_cap - jax.nn.logsumexp(tea_cap, axis=-1, keepdims=True)
        tea_prob = jnp.exp(tea_logp)
        kl_rows = jnp.sum(tea_prob * (tea_logp - stu_logp), axis=-1)
        weight = (mask_rows / mask_sum)[:, None]
        cap_ratio = stu_cap / SOFT_CAP
        grad_z = ((jnp.exp(stu_logp) - tea_prob) * weight * (1.0 - cap_ratio * cap_ratio)).astype(jnp.bfloat16)
        grad_x = jnp.dot(grad_z, emb_table, preferred_element_type=jnp.float32)
        grad_n = grad_x * (1.0 + w_final)
        grad_h = inv_rms * (grad_n - normed * jnp.mean(grad_n * normed, axis=-1, keepdims=True))
        loss_acc = loss_acc + jnp.sum(mask_rows * kl_rows)
        gain_acc = gain_acc + jnp.sum(grad_x * normed, axis=0)
        table_acc = table_acc + jnp.dot(grad_z.T, x_rows, preferred_element_type=jnp.float32)
        return (loss_acc, gain_acc, table_acc), grad_h.astype(jnp.bfloat16)

    init_carry = (jnp.zeros((), jnp.float32), jnp.zeros((MODEL_DIM,), jnp.float32), jnp.zeros((VOCAB_SIZE, MODEL_DIM), jnp.float32))
    (loss_acc, gain_acc, table_acc), grad_blocks = lax.scan(block_step, init_carry, (hid_blocks, tea_blocks, mask_blocks))
    return loss_acc / mask_sum, grad_blocks.reshape(NUM_TOKENS, MODEL_DIM), gain_acc, table_acc
```

```python
import functools
import math

import jax
import jax.numpy as jnp
from jax import lax
from jax.experimental import pallas as pl
from jax.experimental.pallas import tpu as pltpu
from jax.sharding import PartitionSpec as P

SOFT_CAP = 30.0
NORM_EPS = 1e-6
INV_CAP = 1.0 / SOFT_CAP
CAP_LOG2E = SOFT_CAP * math.log2(math.e)
MESH = pl.DeviceIdType.MESH
F32 = jnp.float32
BF16 = jnp.bfloat16
GROUP = 16
VMEM = pltpu.VMEM
NT_DIMS = (((1,), (1,)), ((), ()))


def full_spec(shape, single=True):
    zeros = (0,) * len(shape)
    if single:
        return pl.BlockSpec(shape, lambda j: zeros, pipeline_mode=pl.Buffered(1))
    return pl.BlockSpec(shape, lambda j: zeros)


STAT_TILE = 512
STAT_ROWS = 256


def stats_kernel(hid_ref, gain_ref, mask_ref, tab_ref, tea_ref, x_ref, xt_ref, stat_ref,
                 stu_acc, tea_acc, z_even, z_odd, count_vmem, count_smem, groups, live, sem):
    step = pl.program_id(0)
    dim, tokens = hid_ref.shape
    n_groups = tokens // GROUP
    per_block = STAT_ROWS // GROUP

    @pl.when(step == 0)
    def _():
        rows = lax.broadcasted_iota(jnp.int32, (128, 128), 0) // GROUP
        cols = lax.broadcasted_iota(jnp.int32, (128, 128), 1)
        pick = jnp.where(rows == cols, 1.0, 0.0).astype(BF16)
        counts = jnp.dot(mask_ref[...].astype(BF16), pick, preferred_element_type=F32)
        count_vmem[...] = counts.astype(jnp.int32)
        copy = pltpu.make_async_copy(count_vmem, count_smem, sem)
        copy.start()
        gain = jnp.broadcast_to(1.0 + gain_ref[...], (128, gain_ref.shape[1])).T[:dim, :]
        for blk in range(tokens // 128):
            hid = hid_ref[:, blk * 128:(blk + 1) * 128].astype(F32)
            inv_rms = lax.rsqrt(jnp.sum(hid * hid, axis=0, keepdims=True) * (1.0 / dim) + NORM_EPS)
            x_t = hid * inv_rms * gain
            xt_ref[:, blk * 128:(blk + 1) * 128] = x_t.astype(BF16)
            x_ref[blk * 128:(blk + 1) * 128, :] = x_t.T.astype(BF16)
        stu_acc[...] = jnp.zeros_like(stu_acc)
        tea_acc[...] = jnp.zeros_like(tea_acc)
        copy.wait()

        def add_group(g, n):
            groups[n] = g
            keep = count_smem[g // 8, g % 8] > 0
            return n + jnp.where(keep, 1, 0)

        n_live = lax.fori_loop(0, n_groups, add_group, 0)

        def pad(i, c):
            groups[n_live + i] = n_groups
            return c

        lax.fori_loop(0, 2 * per_block, pad, 0)
        live[0] = n_live

    n_pairs = (live[0] + 2 * per_block - 1) // (2 * per_block)

    def source(i):
        return pl.ds(pl.multiple_of(jnp.minimum(groups[i], n_groups - 1) * GROUP, GROUP), GROUP)

    def logits(first, z_ref):
        rows = jnp.concatenate([x_ref[source(first + i), :] for i in range(per_block)], axis=0)
        z_ref[...] = jnp.dot(rows, tab_ref[...], preferred_element_type=F32)

    def lane_sum(val):
        total = val[:, :128]
        for lane in range(128, STAT_TILE, 128):
            total = total + val[:, lane:lane + 128]
        return total

    def accumulate(first, z_ref):
        for i in range(per_block):
            dest = pl.ds(pl.multiple_of(groups[first + i] * GROUP, GROUP), GROUP)
            tea = jnp.tanh(tea_ref[source(first + i), :].astype(F32) * INV_CAP)
            tea_acc[dest, :] += lane_sum(jnp.exp2(tea * CAP_LOG2E))
            stu = jnp.tanh(z_ref[i * GROUP:(i + 1) * GROUP, :] * INV_CAP)
            stu_acc[dest, :] += lane_sum(jnp.exp2(stu * CAP_LOG2E))

    logits(0, z_even)

    def pair(p, c):
        first = p * 2 * per_block
        logits(first + per_block, z_odd)
        accumulate(first, z_even)
        logits(jnp.minimum(first + 2 * per_block, n_groups), z_even)
        accumulate(first + per_block, z_odd)
        return c

    lax.fori_loop(0, n_pairs, pair, 0)

    @pl.when(step == pl.num_programs(0) - 1)
    def _():
        for blk in range(tokens // 128):
            for k, acc in enumerate((stu_acc, tea_acc)):
                part = acc[blk * 128:(blk + 1) * 128, :].T
                stat_ref[k * 16 + blk:k * 16 + blk + 1, :] = jnp.sum(part, axis=0, keepdims=True)


def stats(hid_t, gain, mask, tab_t, tea):
    dim, tokens = hid_t.shape
    vocab = tab_t.shape[1]
    n_groups = tokens // GROUP
    extra = 2 * (STAT_ROWS // GROUP)
    return pl.pallas_call(
        stats_kernel,
        grid=(vocab // STAT_TILE,),
        in_specs=[
            full_spec(hid_t.shape), full_spec(gain.shape), full_spec(mask.shape),
            pl.BlockSpec((dim, STAT_TILE), lambda j: (0, j)),
            pl.BlockSpec((tokens, STAT_TILE), lambda j: (0, j)),
        ],
        out_specs=[full_spec((tokens, dim)), full_spec((dim, tokens)), full_spec((32, 128))],
        out_shape=[
            jax.ShapeDtypeStruct((tokens, dim), BF16),
            jax.ShapeDtypeStruct((dim, tokens), BF16),
            jax.ShapeDtypeStruct((32, 128), F32),
        ],
        scratch_shapes=[
            VMEM((tokens + GROUP, 128), F32), VMEM((tokens + GROUP, 128), F32),
            VMEM((STAT_ROWS, STAT_TILE), F32), VMEM((STAT_ROWS, STAT_TILE), F32),
            VMEM((16, 128), jnp.int32), pltpu.SMEM((16, 128), jnp.int32),
            pltpu.SMEM((n_groups + 2 * extra,), jnp.int32), pltpu.SMEM((1,), jnp.int32),
            pltpu.SemaphoreType.DMA,
        ],
        compiler_params=pltpu.CompilerParams(dimension_semantics=("arbitrary",), vmem_limit_bytes=40 * 2**20),
        cost_estimate=pl.CostEstimate(flops=50_000_000_000, bytes_accessed=70_000_000, transcendentals=0),
        name="stats",
    )(hid_t, gain, mask, tab_t, tea)


def gather_kernel(n_tp, stat_ref, mask_ref, stu_col, tea_col, base_ref, slots, mask_slot, send_sem, recv_sem):
    tp = lax.axis_index("tp")
    dp = lax.axis_index("dp")
    barrier = pltpu.get_barrier_semaphore()
    peers = [(dp, lax.rem(tp + k, n_tp)) for k in range(1, n_tp)] + [(1 - dp, tp)]
    for peer in peers:
        pl.semaphore_signal(barrier, inc=1, device_id=peer, device_id_type=MESH)
    pl.semaphore_wait(barrier, len(peers))
    copies = []
    for k, peer in enumerate(peers):
        last = k == n_tp - 1
        copies.append(pltpu.make_async_remote_copy(
            src_ref=mask_ref if last else stat_ref,
            dst_ref=mask_slot if last else slots.at[k],
            send_sem=send_sem.at[k], recv_sem=recv_sem.at[k], device_id=peer, device_id_type=MESH))
        copies[-1].start()
    for copy in copies:
        copy.wait()
    parts = [stat_ref[...]] + [slots[k] for k in range(n_tp - 1)]
    total = jnp.zeros_like(parts[0])
    for owner in range(n_tp):
        gap = lax.rem(tp - owner + n_tp, n_tp)
        part = parts[0]
        for k in range(1, n_tp):
            part = jnp.where(gap == k, parts[k], part)
        total = total + part
    total = jnp.where(total > 0.0, total, 1.0)
    mask = mask_ref[...]
    mask_sum = jnp.sum(mask) + jnp.sum(mask_slot[...])
    weight = mask / mask_sum
    stu_sum, tea_sum = total[:16, :], total[16:, :]
    base = jnp.sum(weight * (jnp.log(stu_sum) - jnp.log(tea_sum)))
    base_ref[...] = jnp.full((8, 128), base, F32)
    stu_row, tea_row = weight / stu_sum, weight / tea_sum
    for blk in range(16):
        rows = slice(blk * 128, (blk + 1) * 128)
        stu_col[rows, :] = jnp.broadcast_to(stu_row[blk:blk + 1, :], (128, 128)).T
        tea_col[rows, :] = jnp.broadcast_to(tea_row[blk:blk + 1, :], (128, 128)).T


def gather_stats(stat, mask, n_tp):
    tokens = mask.size
    whole = pl.BlockSpec(memory_space=VMEM)
    return pl.pallas_call(
        functools.partial(gather_kernel, n_tp),
        in_specs=[whole, whole],
        out_specs=[whole, whole, whole],
        out_shape=[
            jax.ShapeDtypeStruct((tokens, 128), F32),
            jax.ShapeDtypeStruct((tokens, 128), F32),
            jax.ShapeDtypeStruct((8, 128), F32),
        ],
        scratch_shapes=[
            VMEM((n_tp - 1,) + stat.shape, F32), VMEM(mask.shape, F32),
            pltpu.SemaphoreType.DMA((n_tp,)), pltpu.SemaphoreType.DMA((n_tp,)),
        ],
        compiler_params=pltpu.CompilerParams(collective_id=0, has_side_effects=True, vmem_limit_bytes=8 * 2**20),
        cost_estimate=pl.CostEstimate(flops=5_000_000, bytes_accessed=2_000_000, transcendentals=0),
        name="gather_stats",
    )(stat, mask)


GRAD_TILE = 256
GRAD_ROWS = 256


def chunk_kernel(first, x_ref, xt_ref, stu_col, tea_col, tab_ref, tea_ref, *refs):
    if first:
        de_ref, dx_out, kl_out, dx_acc, kl_acc, g_ref, sem = refs
    else:
        dx_in, kl_in, de_ref, dx_out, kl_out, dx_acc, kl_acc, g_ref, sem = refs
    step = pl.program_id(0)
    tokens = x_ref.shape[0]

    @pl.when(step == 0)
    def _():
        if first:
            dx_acc[...] = jnp.zeros_like(dx_acc)
            kl_acc[...] = jnp.zeros_like(kl_acc)
        else:
            loads = [pltpu.make_async_copy(dx_in, dx_acc, sem.at[0]), pltpu.make_async_copy(kl_in, kl_acc, sem.at[1])]
            for load in loads:
                load.start()
            for load in loads:
                load.wait()

    def block(b, c):
        rows = pl.ds(pl.multiple_of(b * GRAD_ROWS, GRAD_ROWS), GRAD_ROWS)
        z = jnp.dot(x_ref[rows, :], tab_ref[...], preferred_element_type=F32)
        stu_scale = stu_col[rows, :]
        tea_scale = tea_col[rows, :]
        kl = kl_acc[rows, :]
        parts = []
        for lane in range(0, GRAD_TILE, 128):
            stu = jnp.tanh(z[:, lane:lane + 128] * INV_CAP)
            tea = jnp.tanh(tea_ref[rows, lane:lane + 128].astype(F32) * INV_CAP)
            stu_p = jnp.exp2(stu * CAP_LOG2E) * stu_scale
            tea_p = jnp.exp2(tea * CAP_LOG2E) * tea_scale
            kl = kl + tea_p * (tea - stu)
            parts.append(((stu_p - tea_p) * (1.0 - stu * stu)).astype(BF16))
        kl_acc[rows, :] = kl
        g = jnp.concatenate(parts, axis=1)
        g_ref[rows, :] = g
        dx_acc[rows, :] += lax.dot_general(g, tab_ref[...], NT_DIMS, preferred_element_type=F32)
        return c

    lax.fori_loop(0, tokens // GRAD_ROWS, block, 0)
    de_ref[...] = jnp.dot(xt_ref[...], g_ref[...], preferred_element_type=F32)

    @pl.when(step == pl.num_programs(0) - 1)
    def _():
        saves = [pltpu.make_async_copy(dx_acc, dx_out, sem.at[0]), pltpu.make_async_copy(kl_acc, kl_out, sem.at[1])]
        for save in saves:
            save.start()
        for save in saves:
            save.wait()


def chunk_grad(start, size, x, x_t, stu_col, tea_col, tab_t, tea, carry):
    tokens, dim = x.shape
    off = start // GRAD_TILE
    hbm = pl.BlockSpec(memory_space=pl.ANY)
    first = carry is None
    work = tokens * size
    return pl.pallas_call(
        functools.partial(chunk_kernel, first),
        grid=(size // GRAD_TILE,),
        in_specs=[
            full_spec((tokens, dim)), full_spec((dim, tokens)), full_spec((tokens, 128)), full_spec((tokens, 128)),
            pl.BlockSpec((dim, GRAD_TILE), lambda j: (0, j + off)),
            pl.BlockSpec((tokens, GRAD_TILE), lambda j: (0, j + off)),
        ] + ([] if first else [hbm, hbm]),
        out_specs=[pl.BlockSpec((dim, GRAD_TILE), lambda j: (0, j)), hbm, hbm],
        out_shape=[
            jax.ShapeDtypeStruct((dim, size), F32),
            jax.ShapeDtypeStruct((tokens, dim), F32),
            jax.ShapeDtypeStruct((tokens, 128), F32),
        ],
        scratch_shapes=[
            VMEM((tokens, dim), F32), VMEM((tokens, 128), F32), VMEM((tokens, GRAD_TILE), BF16),
            pltpu.SemaphoreType.DMA((2,)),
        ],
        input_output_aliases={} if first else {6: 1, 7: 2},
        compiler_params=pltpu.CompilerParams(dimension_semantics=("arbitrary",), vmem_limit_bytes=40 * 2**20),
        cost_estimate=pl.CostEstimate(flops=work * 3 * 2 * dim, bytes_accessed=work * 2, transcendentals=0),
        name="chunk_grad",
    )(x, x_t, stu_col, tea_col, tab_t, tea, *(() if first else carry))


def dx_kernel(n_tp, dx_ref, kl_ref, base_ref, hid_ref, gain_ref, gh_ref, part_ref,
              dxt, slots, own, parts_buf, part_out, local_sem, send_sem, recv_sem):
    tp = lax.axis_index("tp")
    dp = lax.axis_index("dp")
    dim, tokens = hid_ref.shape
    width = tokens // n_tp
    load = pltpu.make_async_copy(dx_ref, dxt, local_sem.at[0])
    load.start()
    barrier = pltpu.get_barrier_semaphore()
    peers = [lax.rem(tp + k, n_tp) for k in range(1, n_tp)]
    for peer in peers:
        pl.semaphore_signal(barrier, inc=1, device_id=(dp, peer), device_id_type=MESH)
    pl.semaphore_wait(barrier, n_tp - 1)
    load.wait()

    def window(index):
        return pl.ds(pl.multiple_of(index * width, width), width)

    reduce = []
    for k, peer in enumerate(peers):
        reduce.append(pltpu.make_async_remote_copy(
            src_ref=dxt.at[window(peer), :], dst_ref=slots.at[k],
            send_sem=send_sem.at[0, k], recv_sem=recv_sem.at[0, k], device_id=(dp, peer), device_id_type=MESH))
        reduce[-1].start()
    for copy in reduce:
        copy.wait()
    mine = window(tp)
    total = jnp.zeros((width, dim), F32)
    for owner in range(n_tp):
        gap = lax.rem(tp - owner + n_tp, n_tp)
        part = dxt[mine, :]
        for k in range(1, n_tp):
            part = jnp.where(gap == k, slots[k - 1], part)
        total = total + part
    grad_x = total.T
    gain = jnp.broadcast_to(1.0 + gain_ref[...], (128, gain_ref.shape[1])).T[:dim, :1]
    hid = hid_ref[:, mine].astype(F32)
    inv_rms = lax.rsqrt(jnp.sum(hid * hid, axis=0, keepdims=True) * (1.0 / dim) + NORM_EPS)
    normed = hid * inv_rms
    grad_n = grad_x * gain
    corr = jnp.sum(grad_n * normed, axis=0, keepdims=True) * (1.0 / dim)
    own[...] = inv_rms * (grad_n - normed * corr)

    prod = grad_x * normed
    col = prod[:, :128]
    for lane in range(128, width, 128):
        col = col + prod[:, lane:lane + 128]
    row = jnp.sum(col.T, axis=0, keepdims=True)
    part_out[0:1, :dim] = row
    part_out[0:1, dim:] = jnp.zeros((1, part_out.shape[1] - dim), F32)
    loss = SOFT_CAP * jnp.sum(kl_ref[...]) + jnp.sum(base_ref[0:1, 0:1]) * (1.0 / n_tp)
    part_out[1:2, :] = jnp.full((1, part_out.shape[1]), loss, F32)
    part_out[2:8, :] = jnp.zeros((6, part_out.shape[1]), F32)

    spread = []
    for k, peer in enumerate(peers):
        spread.append(pltpu.make_async_remote_copy(
            src_ref=own, dst_ref=gh_ref.at[:, mine],
            send_sem=send_sem.at[1, k], recv_sem=recv_sem.at[1, k], device_id=(dp, peer), device_id_type=MESH))
        spread.append(pltpu.make_async_remote_copy(
            src_ref=part_out, dst_ref=parts_buf.at[tp],
            send_sem=send_sem.at[2, k], recv_sem=recv_sem.at[2, k], device_id=(dp, peer), device_id_type=MESH))
    for copy in spread:
        copy.start()
    gh_ref[:, mine] = own[...]
    parts_buf[tp] = part_out[...]
    for copy in spread:
        copy.wait()
    share = parts_buf[0]
    for k in range(1, n_tp):
        share = share + parts_buf[k]
    part_ref[...] = share


def reduce_dx(dx, kl, base, hid_t, gain, n_tp):
    tokens, dim = dx.shape
    width = tokens // n_tp
    whole = pl.BlockSpec(memory_space=VMEM)
    return pl.pallas_call(
        functools.partial(dx_kernel, n_tp),
        in_specs=[pl.BlockSpec(memory_space=pl.ANY), whole, whole, whole, whole],
        out_specs=[whole, whole],
        out_shape=[
            jax.ShapeDtypeStruct((dim, tokens), F32),
            jax.ShapeDtypeStruct((8, gain.shape[1]), F32),
        ],
        scratch_shapes=[
            VMEM((tokens, dim), F32), VMEM((n_tp - 1, width, dim), F32), VMEM((dim, width), F32),
            VMEM((n_tp, 8, gain.shape[1]), F32), VMEM((8, gain.shape[1]), F32),
            pltpu.SemaphoreType.DMA((1,)), pltpu.SemaphoreType.DMA((3, n_tp - 1)), pltpu.SemaphoreType.DMA((3, n_tp - 1)),
        ],
        compiler_params=pltpu.CompilerParams(collective_id=1, has_side_effects=True, vmem_limit_bytes=48 * 2**20),
        cost_estimate=pl.CostEstimate(flops=50_000_000_000, bytes_accessed=20_000_000, transcendentals=0),
        name="reduce_dx",
    )(dx, kl, base, hid_t, gain)


def add_kernel(*refs):
    a_ref, b_ref, out_ref = refs[-3], refs[-2], refs[-1]
    out_ref[...] = a_ref[...] + b_ref[...]


def add_chunk(start, size, vocab, own, other, out, after):
    dim = own.shape[0]
    tile = math.gcd(math.gcd(start, size), 512)
    off = start // tile
    hbm = pl.BlockSpec(memory_space=pl.ANY)
    block = pl.BlockSpec((dim, tile), lambda j: (0, j))
    lead = (after,) if out is None else (out,)
    return pl.pallas_call(
        add_kernel,
        grid=(size // tile,),
        in_specs=[hbm, block, block],
        out_specs=pl.BlockSpec((dim, tile), lambda j: (0, j + off)),
        out_shape=jax.ShapeDtypeStruct((dim, vocab), F32),
        input_output_aliases={} if out is None else {0: 0},
        compiler_params=pltpu.CompilerParams(dimension_semantics=("arbitrary",), vmem_limit_bytes=16 * 2**20),
        cost_estimate=pl.CostEstimate(flops=dim * size, bytes_accessed=12 * dim * size, transcendentals=0),
        name="add_chunk",
    )(*lead, own, other)


CHUNKS = (256, 512, 1024, 2048, 3072, 3072, 1536, 512, 256)


def solution(mesh):
    n_tp = mesh.shape["tp"]
    swap = [(0, 1), (1, 0)]

    def step(hid_rows, w_final, tab_rows, tea_rows, mask_rows):
        tokens, dim = hid_rows.shape
        vocab = tab_rows.shape[0]
        hid_t = hid_rows.T
        tab_t = tab_rows.T
        mask = mask_rows.reshape(tokens // 128, 128)
        gain = jnp.pad(w_final, (0, 640 - dim)).reshape(1, 640)
        x, x_t, stat = stats(hid_t, gain, mask, tab_t, tea_rows)
        stu_col, tea_col, base = gather_stats(stat, mask, n_tp)
        carry = None
        own, other = [], []
        start = 0
        for size in CHUNKS:
            part, dx, kl = chunk_grad(start, size, x, x_t, stu_col, tea_col, tab_t, tea_rows, carry)
            carry = (dx, kl)
            other.append(lax.ppermute(part, "dp", swap))
            own.append(part)
            start += size
        gh_t, share = reduce_dx(*carry, base, hid_t, gain, n_tp)
        share = share + lax.ppermute(share, "dp", swap)
        out = None
        start = 0
        for size, a, b in zip(CHUNKS, own, other):
            out = add_chunk(start, size, vocab, a, b, out, gh_t)
            start += size
        return share[1, 0], gh_t.T.astype(BF16), share[0, :dim], out.T

    return jax.shard_map(
        step, mesh=mesh,
        in_specs=(P("dp", None), P(None), P("tp", None), P("dp", "tp"), P("dp")),
        out_specs=(P(), P("dp", None), P(None), P("tp", None)), check_vma=False)
```

```python
import functools
import math

import jax
import jax.numpy as jnp
from jax import lax
from jax.experimental import pallas as pl
from jax.experimental.pallas import tpu as pltpu
from jax.sharding import PartitionSpec as P

SOFT_CAP = 30.0
NORM_EPS = 1e-6
INV_CAP = 1.0 / SOFT_CAP
CAP_LOG2E = SOFT_CAP * math.log2(math.e)
MESH = pl.DeviceIdType.MESH
F32 = jnp.float32
BF16 = jnp.bfloat16
GROUP = 16
VMEM = pltpu.VMEM
NT_DIMS = (((1,), (1,)), ((), ()))


STAT_TILE = 512
STAT_ROWS = 256
PER_BLOCK = STAT_ROWS // GROUP
TAIL_STEP = 4


def stats_kernel(hid_ref, gain_ref, mask_ref, tab_ref, tea_ref, x_ref, xt_ref, stat_ref,
                 stu_acc, tea_acc, z_even, z_odd, count_vmem, count_smem, groups, live, sem):
    step = pl.program_id(0)
    dim, tokens = hid_ref.shape
    n_groups = tokens // GROUP

    @pl.when(step == 0)
    def _():
        stu_acc[...] = jnp.zeros_like(stu_acc)
        tea_acc[...] = jnp.zeros_like(tea_acc)
        rows = lax.broadcasted_iota(jnp.int32, (128, 128), 0) // GROUP
        cols = lax.broadcasted_iota(jnp.int32, (128, 128), 1)
        pick = jnp.where(rows == cols, 1.0, 0.0).astype(BF16)
        counts = jnp.dot(mask_ref[...].astype(BF16), pick, preferred_element_type=F32)
        count_vmem[...] = counts.astype(jnp.int32)
        copy = pltpu.make_async_copy(count_vmem, count_smem, sem)
        copy.start()
        gain = jnp.broadcast_to(1.0 + gain_ref[...], (128, gain_ref.shape[1])).T[:dim, :]
        for blk in range(tokens // 128):
            hid = hid_ref[:, blk * 128:(blk + 1) * 128].astype(F32)
            inv_rms = lax.rsqrt(jnp.sum(hid * hid, axis=0, keepdims=True) * (1.0 / dim) + NORM_EPS)
            x_t = hid * inv_rms * gain
            xt_ref[:, blk * 128:(blk + 1) * 128] = x_t.astype(BF16)
            x_ref[blk * 128:(blk + 1) * 128, :] = x_t.T.astype(BF16)
        copy.wait()

        def add_group(g, n):
            groups[n] = g
            keep = count_smem[g // 8, g % 8] > 0
            return n + jnp.where(keep, 1, 0)

        n_live = lax.fori_loop(0, n_groups, add_group, 0)

        def pad(i, c):
            groups[n_live + i] = n_groups
            return c

        lax.fori_loop(0, PER_BLOCK, pad, 0)
        live[0] = n_live

    n_live = live[0]
    n_full = n_live // PER_BLOCK

    def source(i):
        return pl.ds(pl.multiple_of(jnp.minimum(groups[i], n_groups - 1) * GROUP, GROUP), GROUP)

    def dest(i):
        return pl.ds(pl.multiple_of(groups[i] * GROUP, GROUP), GROUP)

    def logits(block, z_ref):
        rows = jnp.concatenate([x_ref[source(block * PER_BLOCK + i), :] for i in range(PER_BLOCK)], axis=0)
        z_ref[...] = jnp.dot(rows, tab_ref[...], preferred_element_type=F32)

    def exp_sum(val):
        val = jnp.exp2(jnp.tanh(val * INV_CAP) * CAP_LOG2E)
        total = val[:, :128]
        for lane in range(128, STAT_TILE, 128):
            total = total + val[:, lane:lane + 128]
        return total

    def teacher_group(i):
        tea_acc[dest(i), :] += exp_sum(tea_ref[source(i), :].astype(F32))

    def student_group(i, z):
        stu_acc[dest(i), :] += exp_sum(z)

    def accumulate(block, z_ref):
        for i in range(PER_BLOCK):
            teacher_group(block * PER_BLOCK + i)
            student_group(block * PER_BLOCK + i, z_ref[i * GROUP:(i + 1) * GROUP, :])

    logits(0, z_even)
    for i in range(PER_BLOCK):
        teacher_group(n_full * PER_BLOCK + i)

    def pair(p, c):
        logits(2 * p + 1, z_odd)
        accumulate(2 * p, z_even)
        logits(2 * p + 2, z_even)
        accumulate(2 * p + 1, z_odd)
        return c

    lax.fori_loop(0, n_full // 2, pair, 0)

    def tail(z_ref):
        def some(q, c):
            for i in range(TAIL_STEP):
                row = pl.multiple_of((q * TAIL_STEP + i) * GROUP, GROUP)
                student_group(n_full * PER_BLOCK + q * TAIL_STEP + i, z_ref[pl.ds(row, GROUP), :])
            return c

        lax.fori_loop(0, (n_live - n_full * PER_BLOCK + TAIL_STEP - 1) // TAIL_STEP, some, 0)

    @pl.when(n_full % 2 == 1)
    def _():
        logits(n_full, z_odd)
        accumulate(n_full - 1, z_even)
        tail(z_odd)

    @pl.when(n_full % 2 == 0)
    def _():
        tail(z_even)

    @pl.when(step == pl.num_programs(0) - 1)
    def _():
        for blk in range(tokens // 128):
            for k, acc in enumerate((stu_acc, tea_acc)):
                part = acc[blk * 128:(blk + 1) * 128, :].T
                stat_ref[k * 16 + blk:k * 16 + blk + 1, :] = jnp.sum(part, axis=0, keepdims=True)


def stats(hid_t, gain, mask, tab_t, tea):
    dim, tokens = hid_t.shape
    vocab = tab_t.shape[1]
    n_groups = tokens // GROUP
    whole = pl.BlockSpec(memory_space=VMEM)
    return pl.pallas_call(
        stats_kernel,
        grid=(vocab // STAT_TILE,),
        in_specs=[
            whole, whole, whole,
            pl.BlockSpec((dim, STAT_TILE), lambda j: (0, j)),
            pl.BlockSpec((tokens, STAT_TILE), lambda j: (0, j)),
        ],
        out_specs=[whole, whole, whole],
        out_shape=[
            jax.ShapeDtypeStruct((tokens, dim), BF16),
            jax.ShapeDtypeStruct((dim, tokens), BF16),
            jax.ShapeDtypeStruct((32, 128), F32),
        ],
        scratch_shapes=[
            VMEM((tokens + GROUP, 128), F32), VMEM((tokens + GROUP, 128), F32),
            VMEM((STAT_ROWS, STAT_TILE), F32), VMEM((STAT_ROWS, STAT_TILE), F32),
            VMEM((16, 128), jnp.int32), pltpu.SMEM((16, 128), jnp.int32),
            pltpu.SMEM((n_groups + 2 * PER_BLOCK,), jnp.int32), pltpu.SMEM((1,), jnp.int32),
            pltpu.SemaphoreType.DMA,
        ],
        compiler_params=pltpu.CompilerParams(dimension_semantics=("arbitrary",), vmem_limit_bytes=46 * 2**20),
        cost_estimate=pl.CostEstimate(flops=50_000_000_000, bytes_accessed=70_000_000, transcendentals=0),
        name="stats",
    )(hid_t, gain, mask, tab_t, tea)


def gather_kernel(n_tp, stat_ref, mask_ref, stu_col, tea_col, base_ref, slots, mask_slot, send_sem, recv_sem):
    tp = lax.axis_index("tp")
    dp = lax.axis_index("dp")
    barrier = pltpu.get_barrier_semaphore()
    peers = [(dp, lax.rem(tp + k, n_tp)) for k in range(1, n_tp)] + [(1 - dp, tp)]
    for peer in peers:
        pl.semaphore_signal(barrier, inc=1, device_id=peer, device_id_type=MESH)
    pl.semaphore_wait(barrier, len(peers))
    copies = []
    for k, peer in enumerate(peers):
        last = k == n_tp - 1
        copies.append(pltpu.make_async_remote_copy(
            src_ref=mask_ref if last else stat_ref,
            dst_ref=mask_slot if last else slots.at[k],
            send_sem=send_sem.at[k], recv_sem=recv_sem.at[k], device_id=peer, device_id_type=MESH))
        copies[-1].start()
    for copy in copies:
        copy.wait()
    parts = [stat_ref[...]] + [slots[k] for k in range(n_tp - 1)]
    total = jnp.zeros_like(parts[0])
    for owner in range(n_tp):
        gap = lax.rem(tp - owner + n_tp, n_tp)
        part = parts[0]
        for k in range(1, n_tp):
            part = jnp.where(gap == k, parts[k], part)
        total = total + part
    total = jnp.where(total > 0.0, total, 1.0)
    mask = mask_ref[...]
    mask_sum = jnp.sum(mask) + jnp.sum(mask_slot[...])
    weight = mask / mask_sum
    stu_sum, tea_sum = total[:16, :], total[16:, :]
    base = jnp.sum(weight * (jnp.log(stu_sum) - jnp.log(tea_sum)))
    base_ref[...] = jnp.full((8, 128), base, F32)
    stu_row, tea_row = weight / stu_sum, weight / tea_sum
    for blk in range(16):
        rows = slice(blk * 128, (blk + 1) * 128)
        stu_col[rows, :] = jnp.broadcast_to(stu_row[blk:blk + 1, :], (128, 128)).T
        tea_col[rows, :] = jnp.broadcast_to(tea_row[blk:blk + 1, :], (128, 128)).T


def gather_stats(stat, mask, n_tp):
    tokens = mask.size
    whole = pl.BlockSpec(memory_space=VMEM)
    return pl.pallas_call(
        functools.partial(gather_kernel, n_tp),
        in_specs=[whole, whole],
        out_specs=[whole, whole, whole],
        out_shape=[
            jax.ShapeDtypeStruct((tokens, 128), F32),
            jax.ShapeDtypeStruct((tokens, 128), F32),
            jax.ShapeDtypeStruct((8, 128), F32),
        ],
        scratch_shapes=[
            VMEM((n_tp - 1,) + stat.shape, F32), VMEM(mask.shape, F32),
            pltpu.SemaphoreType.DMA((n_tp,)), pltpu.SemaphoreType.DMA((n_tp,)),
        ],
        compiler_params=pltpu.CompilerParams(collective_id=0, has_side_effects=True, vmem_limit_bytes=8 * 2**20),
        cost_estimate=pl.CostEstimate(flops=5_000_000, bytes_accessed=2_000_000, transcendentals=0),
        name="gather_stats",
    )(stat, mask)


GRAD_TILE = 256
GRAD_ROWS = 256
SLICE = 16


def chunk_kernel(first, x_ref, xt_ref, stu_col, tea_col, tab_ref, tea_ref, *refs):
    if first:
        de_ref, dx_acc, kl_acc, g_ref, z_even, z_odd = refs
    else:
        _, _, de_ref, dx_acc, kl_acc, g_ref, z_even, z_odd = refs
    tokens = x_ref.shape[0]
    n_blocks = tokens // GRAD_ROWS

    if first:
        @pl.when(pl.program_id(0) == 0)
        def _():
            dx_acc[...] = jnp.zeros_like(dx_acc)
            kl_acc[...] = jnp.zeros_like(kl_acc)

    def window(b, size=GRAD_ROWS, skip=0):
        return pl.ds(pl.multiple_of(b * GRAD_ROWS + skip, size), size)

    def logits(b, z_ref):
        z_ref[...] = jnp.dot(x_ref[window(b), :], tab_ref[...], preferred_element_type=F32)

    def grads(b, z_ref):
        for skip in range(0, GRAD_ROWS, SLICE):
            rows = window(b, SLICE, skip)
            stu_scale = stu_col[rows, :]
            tea_scale = tea_col[rows, :]
            kl = kl_acc[rows, :]
            parts = []
            for lane in range(0, GRAD_TILE, 128):
                stu = jnp.tanh(z_ref[skip:skip + SLICE, lane:lane + 128] * INV_CAP)
                tea = jnp.tanh(tea_ref[rows, lane:lane + 128].astype(F32) * INV_CAP)
                stu_p = jnp.exp2(stu * CAP_LOG2E) * stu_scale
                tea_p = jnp.exp2(tea * CAP_LOG2E) * tea_scale
                kl = kl + tea_p * (tea - stu)
                parts.append(((stu_p - tea_p) * (1.0 - stu * stu)).astype(BF16))
            kl_acc[rows, :] = kl
            g_ref[rows, :] = jnp.concatenate(parts, axis=1)

    def add_dx(b):
        dx_acc[window(b), :] += lax.dot_general(g_ref[window(b), :], tab_ref[...], NT_DIMS, preferred_element_type=F32)

    logits(0, z_even)
    logits(1, z_odd)
    grads(0, z_even)

    def pair(p, c):
        add_dx(2 * p)
        logits(2 * p + 2, z_even)
        grads(2 * p + 1, z_odd)
        add_dx(2 * p + 1)
        logits(2 * p + 3, z_odd)
        grads(2 * p + 2, z_even)
        return c

    lax.fori_loop(0, n_blocks // 2 - 1, pair, 0)
    add_dx(n_blocks - 2)
    grads(n_blocks - 1, z_odd)
    de_ref[...] = jnp.dot(xt_ref[...], g_ref[...], preferred_element_type=F32)
    add_dx(n_blocks - 1)


def chunk_grad(start, size, x, x_t, stu_col, tea_col, tab_t, tea, carry):
    tokens, dim = x.shape
    off = start // GRAD_TILE
    whole = pl.BlockSpec(memory_space=VMEM)
    first = carry is None
    work = tokens * size
    return pl.pallas_call(
        functools.partial(chunk_kernel, first),
        grid=(size // GRAD_TILE,),
        in_specs=[
            whole, whole, whole, whole,
            pl.BlockSpec((dim, GRAD_TILE), lambda j: (0, j + off)),
            pl.BlockSpec((tokens, GRAD_TILE), lambda j: (0, j + off)),
        ] + ([] if first else [whole, whole]),
        out_specs=[pl.BlockSpec((dim, GRAD_TILE), lambda j: (0, j)), whole, whole],
        out_shape=[
            jax.ShapeDtypeStruct((dim, size), F32),
            jax.ShapeDtypeStruct((tokens, dim), F32),
            jax.ShapeDtypeStruct((tokens, 128), F32),
        ],
        scratch_shapes=[
            VMEM((tokens, GRAD_TILE), BF16), VMEM((GRAD_ROWS, GRAD_TILE), F32), VMEM((GRAD_ROWS, GRAD_TILE), F32),
        ],
        input_output_aliases={} if first else {6: 1, 7: 2},
        compiler_params=pltpu.CompilerParams(dimension_semantics=("arbitrary",), vmem_limit_bytes=32 * 2**20),
        cost_estimate=pl.CostEstimate(flops=work * 3 * 2 * dim, bytes_accessed=work * 2, transcendentals=0),
        name="chunk_grad",
    )(x, x_t, stu_col, tea_col, tab_t, tea, *(() if first else carry))


def dx_kernel(n_tp, dx_ref, kl_ref, base_ref, hid_ref, gain_ref, gh_ref, part_ref,
              slots, own, parts_buf, part_out, send_sem, recv_sem):
    tp = lax.axis_index("tp")
    dp = lax.axis_index("dp")
    dim, tokens = hid_ref.shape
    width = tokens // n_tp
    barrier = pltpu.get_barrier_semaphore()
    peers = [lax.rem(tp + k, n_tp) for k in range(1, n_tp)]
    for peer in peers:
        pl.semaphore_signal(barrier, inc=1, device_id=(dp, peer), device_id_type=MESH)
    pl.semaphore_wait(barrier, n_tp - 1)

    def window(index):
        return pl.ds(pl.multiple_of(index * width, width), width)

    reduce = []
    for k, peer in enumerate(peers):
        reduce.append(pltpu.make_async_remote_copy(
            src_ref=dx_ref.at[window(peer), :], dst_ref=slots.at[k],
            send_sem=send_sem.at[0, k], recv_sem=recv_sem.at[0, k], device_id=(dp, peer), device_id_type=MESH))
        reduce[-1].start()
    for copy in reduce:
        copy.wait()
    mine = window(tp)
    total = jnp.zeros((width, dim), F32)
    for owner in range(n_tp):
        gap = lax.rem(tp - owner + n_tp, n_tp)
        part = dx_ref[mine, :]
        for k in range(1, n_tp):
            part = jnp.where(gap == k, slots[k - 1], part)
        total = total + part
    grad_x = total.T
    gain = jnp.broadcast_to(1.0 + gain_ref[...], (128, gain_ref.shape[1])).T[:dim, :1]
    hid = hid_ref[:, mine].astype(F32)
    inv_rms = lax.rsqrt(jnp.sum(hid * hid, axis=0, keepdims=True) * (1.0 / dim) + NORM_EPS)
    normed = hid * inv_rms
    grad_n = grad_x * gain
    corr = jnp.sum(grad_n * normed, axis=0, keepdims=True) * (1.0 / dim)
    own[...] = inv_rms * (grad_n - normed * corr)

    prod = grad_x * normed
    col = prod[:, :128]
    for lane in range(128, width, 128):
        col = col + prod[:, lane:lane + 128]
    row = jnp.sum(col.T, axis=0, keepdims=True)
    part_out[0:1, :dim] = row
    part_out[0:1, dim:] = jnp.zeros((1, part_out.shape[1] - dim), F32)
    loss = SOFT_CAP * jnp.sum(kl_ref[...]) + jnp.sum(base_ref[0:1, 0:1]) * (1.0 / n_tp)
    part_out[1:2, :] = jnp.full((1, part_out.shape[1]), loss, F32)
    part_out[2:8, :] = jnp.zeros((6, part_out.shape[1]), F32)

    spread = []
    for k, peer in enumerate(peers):
        spread.append(pltpu.make_async_remote_copy(
            src_ref=own, dst_ref=gh_ref.at[:, mine],
            send_sem=send_sem.at[1, k], recv_sem=recv_sem.at[1, k], device_id=(dp, peer), device_id_type=MESH))
        spread.append(pltpu.make_async_remote_copy(
            src_ref=part_out, dst_ref=parts_buf.at[tp],
            send_sem=send_sem.at[2, k], recv_sem=recv_sem.at[2, k], device_id=(dp, peer), device_id_type=MESH))
    for copy in spread:
        copy.start()
    gh_ref[:, mine] = own[...]
    parts_buf[tp] = part_out[...]
    for copy in spread:
        copy.wait()
    share = parts_buf[0]
    for k in range(1, n_tp):
        share = share + parts_buf[k]
    part_ref[...] = share


def reduce_dx(dx, kl, base, hid_t, gain, n_tp):
    tokens, dim = dx.shape
    width = tokens // n_tp
    whole = pl.BlockSpec(memory_space=VMEM)
    return pl.pallas_call(
        functools.partial(dx_kernel, n_tp),
        in_specs=[whole, whole, whole, whole, whole],
        out_specs=[whole, whole],
        out_shape=[
            jax.ShapeDtypeStruct((dim, tokens), F32),
            jax.ShapeDtypeStruct((8, 640), F32),
        ],
        scratch_shapes=[
            VMEM((n_tp - 1, width, dim), F32), VMEM((dim, width), F32),
            VMEM((n_tp, 8, 640), F32), VMEM((8, 640), F32),
            pltpu.SemaphoreType.DMA((3, n_tp - 1)), pltpu.SemaphoreType.DMA((3, n_tp - 1)),
        ],
        compiler_params=pltpu.CompilerParams(collective_id=1, has_side_effects=True, vmem_limit_bytes=24 * 2**20),
        cost_estimate=pl.CostEstimate(flops=50_000_000_000, bytes_accessed=20_000_000, transcendentals=0),
        name="reduce_dx",
    )(dx, kl, base, hid_t, gain)


def add_kernel(*refs):
    a_ref, b_ref, out_ref = refs[-3], refs[-2], refs[-1]
    out_ref[...] = a_ref[...] + b_ref[...]


def add_chunk(start, size, vocab, own, other, out, after):
    dim = own.shape[0]
    tile = math.gcd(math.gcd(start, size), 512)
    off = start // tile
    hbm = pl.BlockSpec(memory_space=pl.ANY)
    block = pl.BlockSpec((dim, tile), lambda j: (0, j))
    lead = (after,) if out is None else (out,)
    return pl.pallas_call(
        add_kernel,
        grid=(size // tile,),
        in_specs=[hbm, block, block],
        out_specs=pl.BlockSpec((dim, tile), lambda j: (0, j + off)),
        out_shape=jax.ShapeDtypeStruct((dim, vocab), F32),
        input_output_aliases={} if out is None else {0: 0},
        compiler_params=pltpu.CompilerParams(dimension_semantics=("arbitrary",), vmem_limit_bytes=16 * 2**20),
        cost_estimate=pl.CostEstimate(flops=dim * size, bytes_accessed=12 * dim * size, transcendentals=0),
        name="add_chunk",
    )(*lead, own, other)


CHUNKS = (256, 512, 1536, 3584, 3584, 2048, 512, 256)


def solution(mesh):
    n_tp = mesh.shape["tp"]
    swap = [(0, 1), (1, 0)]

    def step(hid_rows, w_final, tab_rows, tea_rows, mask_rows):
        tokens, dim = hid_rows.shape
        vocab = tab_rows.shape[0]
        hid_t = hid_rows.T
        tab_t = tab_rows.T
        mask = mask_rows.reshape(tokens // 128, 128)
        gain = w_final.reshape(1, dim)
        x, x_t, stat = stats(hid_t, gain, mask, tab_t, tea_rows)
        stu_col, tea_col, base = gather_stats(stat, mask, n_tp)
        carry = None
        own, other = [], []
        start = 0
        for size in CHUNKS:
            part, dx, kl = chunk_grad(start, size, x, x_t, stu_col, tea_col, tab_t, tea_rows, carry)
            carry = (dx, kl)
            other.append(lax.ppermute(part, "dp", swap))
            own.append(part)
            start += size
        gh_t, share = reduce_dx(*carry, base, hid_t, gain, n_tp)
        share_other = lax.ppermute(share, "dp", swap)
        share = share + share_other
        out = None
        start = 0
        for size, a, b in zip(CHUNKS, own, other):
            out = add_chunk(start, size, vocab, a, b, out, gh_t)
            start += size
        return share[1, 0], gh_t.T.astype(BF16), share[0, :dim], out.T

    return jax.shard_map(
        step, mesh=mesh,
        in_specs=(P("dp", None), P(None), P("tp", None), P("dp", "tp"), P("dp")),
        out_specs=(P(), P("dp", None), P(None), P("tp", None)), check_vma=False)
```

```python
import functools
import math

import jax
import jax.numpy as jnp
from jax import lax
from jax.experimental import pallas as pl
from jax.experimental.pallas import tpu as pltpu
from jax.sharding import PartitionSpec as P

SOFT_CAP = 30.0
NORM_EPS = 1e-6
INV_CAP = 1.0 / SOFT_CAP
CAP_LOG2E = SOFT_CAP * math.log2(math.e)
MESH = pl.DeviceIdType.MESH
F32 = jnp.float32
BF16 = jnp.bfloat16
GROUP = 16
VMEM = pltpu.VMEM
NT_DIMS = (((1,), (1,)), ((), ()))


STAT_TILE = 1024
STAT_ROWS = 128
PER_BLOCK = STAT_ROWS // GROUP


def stats_kernel(hid_ref, gain_ref, mask_ref, tab_ref, next_ref, tea_ref, x_ref, xt_ref, stat_ref,
                 stu_acc, tea_acc, z_even, z_odd, count_vmem, count_smem, groups, live, sem):
    step = pl.program_id(0)
    dim, tokens = hid_ref.shape
    n_groups = tokens // GROUP

    def source(i):
        return pl.ds(pl.multiple_of(jnp.minimum(groups[i], n_groups - 1) * GROUP, GROUP), GROUP)

    def dest(i):
        return pl.ds(pl.multiple_of(groups[i] * GROUP, GROUP), GROUP)

    def logits(block, table, z_ref):
        rows = jnp.concatenate([x_ref[source(block * PER_BLOCK + i), :] for i in range(PER_BLOCK)], axis=0)
        z_ref[...] = jnp.dot(rows, table[...], preferred_element_type=F32)

    def exp_sum(val):
        val = jnp.exp2(jnp.tanh(val * INV_CAP) * CAP_LOG2E)
        total = val[:, :128]
        for lane in range(128, STAT_TILE, 128):
            total = total + val[:, lane:lane + 128]
        return total

    def accumulate(block, z_ref):
        for i in range(PER_BLOCK):
            at = block * PER_BLOCK + i
            tea_acc[dest(at), :] += exp_sum(tea_ref[source(at), :].astype(F32))
            stu_acc[dest(at), :] += exp_sum(z_ref[i * GROUP:(i + 1) * GROUP, :])

    @pl.when(step == 0)
    def _():
        stu_acc[...] = jnp.zeros_like(stu_acc)
        tea_acc[...] = jnp.zeros_like(tea_acc)
        rows = lax.broadcasted_iota(jnp.int32, (128, 128), 0) // GROUP
        cols = lax.broadcasted_iota(jnp.int32, (128, 128), 1)
        pick = jnp.where(rows == cols, 1.0, 0.0).astype(BF16)
        counts = jnp.dot(mask_ref[...].astype(BF16), pick, preferred_element_type=F32)
        count_vmem[...] = counts.astype(jnp.int32)
        copy = pltpu.make_async_copy(count_vmem, count_smem, sem)
        copy.start()
        gain = jnp.broadcast_to(1.0 + gain_ref[...], (128, gain_ref.shape[1])).T[:dim, :]
        for blk in range(tokens // 128):
            hid = hid_ref[:, blk * 128:(blk + 1) * 128].astype(F32)
            inv_rms = lax.rsqrt(jnp.sum(hid * hid, axis=0, keepdims=True) * (1.0 / dim) + NORM_EPS)
            x_t = hid * inv_rms * gain
            xt_ref[:, blk * 128:(blk + 1) * 128] = x_t.astype(BF16)
            x_ref[blk * 128:(blk + 1) * 128, :] = x_t.T.astype(BF16)
        copy.wait()

        def add_group(g, n):
            groups[n] = g
            keep = count_smem[g // 8, g % 8] > 0
            return n + jnp.where(keep, 1, 0)

        n_live = lax.fori_loop(0, n_groups, add_group, 0)

        def pad(i, c):
            groups[n_live + i] = n_groups
            return c

        lax.fori_loop(0, 2 * PER_BLOCK, pad, 0)
        live[0] = n_live
        logits(0, tab_ref, z_even)

    more = jnp.maximum((live[0] + 2 * PER_BLOCK - 1) // (2 * PER_BLOCK) - 1, 0)

    def pair(p, c):
        logits(2 * p + 1, tab_ref, z_odd)
        accumulate(2 * p, z_even)
        logits(2 * p + 2, tab_ref, z_even)
        accumulate(2 * p + 1, z_odd)
        return c

    lax.fori_loop(0, more, pair, 0)
    logits(2 * more + 1, tab_ref, z_odd)
    accumulate(2 * more, z_even)
    logits(0, next_ref, z_even)
    accumulate(2 * more + 1, z_odd)

    @pl.when(step == pl.num_programs(0) - 1)
    def _():
        for blk in range(tokens // 128):
            for k, acc in enumerate((stu_acc, tea_acc)):
                part = acc[blk * 128:(blk + 1) * 128, :].T
                stat_ref[k * 16 + blk:k * 16 + blk + 1, :] = jnp.sum(part, axis=0, keepdims=True)


def stats(hid_t, gain, mask, tab_t, tea):
    dim, tokens = hid_t.shape
    vocab = tab_t.shape[1]
    n_groups = tokens // GROUP
    whole = pl.BlockSpec(memory_space=VMEM)
    return pl.pallas_call(
        stats_kernel,
        grid=(vocab // STAT_TILE,),
        in_specs=[
            whole, whole, whole,
            pl.BlockSpec((dim, STAT_TILE), lambda j: (0, j)),
            pl.BlockSpec((dim, STAT_TILE), lambda j: (0, jnp.minimum(j + 1, vocab // STAT_TILE - 1))),
            pl.BlockSpec((tokens, STAT_TILE), lambda j: (0, j)),
        ],
        out_specs=[whole, whole, whole],
        out_shape=[
            jax.ShapeDtypeStruct((tokens, dim), BF16),
            jax.ShapeDtypeStruct((dim, tokens), BF16),
            jax.ShapeDtypeStruct((32, 128), F32),
        ],
        scratch_shapes=[
            VMEM((tokens + GROUP, 128), F32), VMEM((tokens + GROUP, 128), F32),
            VMEM((STAT_ROWS, STAT_TILE), F32), VMEM((STAT_ROWS, STAT_TILE), F32),
            VMEM((16, 128), jnp.int32), pltpu.SMEM((16, 128), jnp.int32),
            pltpu.SMEM((n_groups + 4 * PER_BLOCK,), jnp.int32), pltpu.SMEM((1,), jnp.int32),
            pltpu.SemaphoreType.DMA,
        ],
        compiler_params=pltpu.CompilerParams(dimension_semantics=("arbitrary",), vmem_limit_bytes=46 * 2**20),
        cost_estimate=pl.CostEstimate(flops=50_000_000_000, bytes_accessed=70_000_000, transcendentals=0),
        name="stats",
    )(hid_t, gain, mask, tab_t, tab_t, tea)


def gather_kernel(n_tp, stat_ref, mask_ref, stu_col, tea_col, base_ref, slots, mask_slot, send_sem, recv_sem):
    tp = lax.axis_index("tp")
    dp = lax.axis_index("dp")
    barrier = pltpu.get_barrier_semaphore()
    peers = [(dp, lax.rem(tp + k, n_tp)) for k in range(1, n_tp)] + [(1 - dp, tp)]
    for peer in peers:
        pl.semaphore_signal(barrier, inc=1, device_id=peer, device_id_type=MESH)
    pl.semaphore_wait(barrier, len(peers))
    copies = []
    for k, peer in enumerate(peers):
        last = k == n_tp - 1
        copies.append(pltpu.make_async_remote_copy(
            src_ref=mask_ref if last else stat_ref,
            dst_ref=mask_slot if last else slots.at[k],
            send_sem=send_sem.at[k], recv_sem=recv_sem.at[k], device_id=peer, device_id_type=MESH))
        copies[-1].start()
    for copy in copies:
        copy.wait()
    parts = [stat_ref[...]] + [slots[k] for k in range(n_tp - 1)]
    total = jnp.zeros_like(parts[0])
    for owner in range(n_tp):
        gap = lax.rem(tp - owner + n_tp, n_tp)
        part = parts[0]
        for k in range(1, n_tp):
            part = jnp.where(gap == k, parts[k], part)
        total = total + part
    total = jnp.where(total > 0.0, total, 1.0)
    mask = mask_ref[...]
    mask_sum = jnp.sum(mask) + jnp.sum(mask_slot[...])
    weight = mask / mask_sum
    stu_sum, tea_sum = total[:16, :], total[16:, :]
    base = jnp.sum(weight * (jnp.log(stu_sum) - jnp.log(tea_sum)))
    base_ref[...] = jnp.full((8, 128), base, F32)
    stu_row, tea_row = weight / stu_sum, weight / tea_sum
    for blk in range(16):
        rows = slice(blk * 128, (blk + 1) * 128)
        stu_col[rows, :] = jnp.broadcast_to(stu_row[blk:blk + 1, :], (128, 128)).T
        tea_col[rows, :] = jnp.broadcast_to(tea_row[blk:blk + 1, :], (128, 128)).T


def gather_stats(stat, mask, n_tp):
    tokens = mask.size
    whole = pl.BlockSpec(memory_space=VMEM)
    return pl.pallas_call(
        functools.partial(gather_kernel, n_tp),
        in_specs=[whole, whole],
        out_specs=[whole, whole, whole],
        out_shape=[
            jax.ShapeDtypeStruct((tokens, 128), F32),
            jax.ShapeDtypeStruct((tokens, 128), F32),
            jax.ShapeDtypeStruct((8, 128), F32),
        ],
        scratch_shapes=[
            VMEM((n_tp - 1,) + stat.shape, F32), VMEM(mask.shape, F32),
            pltpu.SemaphoreType.DMA((n_tp,)), pltpu.SemaphoreType.DMA((n_tp,)),
        ],
        compiler_params=pltpu.CompilerParams(collective_id=0, has_side_effects=True, vmem_limit_bytes=8 * 2**20),
        cost_estimate=pl.CostEstimate(flops=5_000_000, bytes_accessed=2_000_000, transcendentals=0),
        name="gather_stats",
    )(stat, mask)


GRAD_TILE = 256
GRAD_ROWS = 256
SLICE = 16


def chunk_kernel(first, x_ref, xt_ref, stu_col, tea_col, tab_ref, tea_ref, *refs):
    if first:
        de_ref, dx_acc, kl_acc, g_ref, z_even, z_odd = refs
    else:
        _, _, de_ref, dx_acc, kl_acc, g_ref, z_even, z_odd = refs
    tokens = x_ref.shape[0]
    n_blocks = tokens // GRAD_ROWS

    if first:
        @pl.when(pl.program_id(0) == 0)
        def _():
            dx_acc[...] = jnp.zeros_like(dx_acc)
            kl_acc[...] = jnp.zeros_like(kl_acc)

    def window(b, size=GRAD_ROWS, skip=0):
        return pl.ds(pl.multiple_of(b * GRAD_ROWS + skip, size), size)

    def logits(b, z_ref):
        z_ref[...] = jnp.dot(x_ref[window(b), :], tab_ref[...], preferred_element_type=F32)

    def grads(b, z_ref):
        for skip in range(0, GRAD_ROWS, SLICE):
            rows = window(b, SLICE, skip)
            stu_scale = stu_col[rows, :]
            tea_scale = tea_col[rows, :]
            kl = kl_acc[rows, :]
            parts = []
            for lane in range(0, GRAD_TILE, 128):
                stu = jnp.tanh(z_ref[skip:skip + SLICE, lane:lane + 128] * INV_CAP)
                tea = jnp.tanh(tea_ref[rows, lane:lane + 128].astype(F32) * INV_CAP)
                stu_p = jnp.exp2(stu * CAP_LOG2E) * stu_scale
                tea_p = jnp.exp2(tea * CAP_LOG2E) * tea_scale
                kl = kl + tea_p * (tea - stu)
                parts.append(((stu_p - tea_p) * (1.0 - stu * stu)).astype(BF16))
            kl_acc[rows, :] = kl
            g_ref[rows, :] = jnp.concatenate(parts, axis=1)

    def add_dx(b):
        dx_acc[window(b), :] += lax.dot_general(g_ref[window(b), :], tab_ref[...], NT_DIMS, preferred_element_type=F32)

    logits(0, z_even)
    logits(1, z_odd)
    grads(0, z_even)

    def pair(p, c):
        add_dx(2 * p)
        logits(2 * p + 2, z_even)
        grads(2 * p + 1, z_odd)
        add_dx(2 * p + 1)
        logits(2 * p + 3, z_odd)
        grads(2 * p + 2, z_even)
        return c

    lax.fori_loop(0, n_blocks // 2 - 1, pair, 0)
    add_dx(n_blocks - 2)
    grads(n_blocks - 1, z_odd)
    de_ref[...] = jnp.dot(xt_ref[...], g_ref[...], preferred_element_type=F32)
    add_dx(n_blocks - 1)


def chunk_grad(start, size, x, x_t, stu_col, tea_col, tab_t, tea, carry):
    tokens, dim = x.shape
    off = start // GRAD_TILE
    whole = pl.BlockSpec(memory_space=VMEM)
    first = carry is None
    work = tokens * size
    return pl.pallas_call(
        functools.partial(chunk_kernel, first),
        grid=(size // GRAD_TILE,),
        in_specs=[
            whole, whole, whole, whole,
            pl.BlockSpec((dim, GRAD_TILE), lambda j: (0, j + off)),
            pl.BlockSpec((tokens, GRAD_TILE), lambda j: (0, j + off)),
        ] + ([] if first else [whole, whole]),
        out_specs=[pl.BlockSpec((dim, GRAD_TILE), lambda j: (0, j)), whole, whole],
        out_shape=[
            jax.ShapeDtypeStruct((dim, size), F32),
            jax.ShapeDtypeStruct((tokens, dim), F32),
            jax.ShapeDtypeStruct((tokens, 128), F32),
        ],
        scratch_shapes=[
            VMEM((tokens, GRAD_TILE), BF16), VMEM((GRAD_ROWS, GRAD_TILE), F32), VMEM((GRAD_ROWS, GRAD_TILE), F32),
        ],
        input_output_aliases={} if first else {6: 1, 7: 2},
        compiler_params=pltpu.CompilerParams(dimension_semantics=("arbitrary",), vmem_limit_bytes=32 * 2**20),
        cost_estimate=pl.CostEstimate(flops=work * 3 * 2 * dim, bytes_accessed=work * 2, transcendentals=0),
        name="chunk_grad",
    )(x, x_t, stu_col, tea_col, tab_t, tea, *(() if first else carry))


def dx_kernel(n_tp, dx_ref, kl_ref, base_ref, hid_ref, gain_ref, gh_ref, part_ref,
              slots, own, parts_buf, part_out, send_sem, recv_sem):
    tp = lax.axis_index("tp")
    dp = lax.axis_index("dp")
    dim, tokens = hid_ref.shape
    width = tokens // n_tp
    barrier = pltpu.get_barrier_semaphore()
    peers = [lax.rem(tp + k, n_tp) for k in range(1, n_tp)]
    for peer in peers:
        pl.semaphore_signal(barrier, inc=1, device_id=(dp, peer), device_id_type=MESH)
    pl.semaphore_wait(barrier, n_tp - 1)

    def window(index):
        return pl.ds(pl.multiple_of(index * width, width), width)

    reduce = []
    for k, peer in enumerate(peers):
        reduce.append(pltpu.make_async_remote_copy(
            src_ref=dx_ref.at[window(peer), :], dst_ref=slots.at[k],
            send_sem=send_sem.at[0, k], recv_sem=recv_sem.at[0, k], device_id=(dp, peer), device_id_type=MESH))
        reduce[-1].start()
    for copy in reduce:
        copy.wait()
    mine = window(tp)
    total = jnp.zeros((width, dim), F32)
    for owner in range(n_tp):
        gap = lax.rem(tp - owner + n_tp, n_tp)
        part = dx_ref[mine, :]
        for k in range(1, n_tp):
            part = jnp.where(gap == k, slots[k - 1], part)
        total = total + part
    grad_x = total.T
    gain = jnp.broadcast_to(1.0 + gain_ref[...], (128, gain_ref.shape[1])).T[:dim, :1]
    hid = hid_ref[:, mine].astype(F32)
    inv_rms = lax.rsqrt(jnp.sum(hid * hid, axis=0, keepdims=True) * (1.0 / dim) + NORM_EPS)
    normed = hid * inv_rms
    grad_n = grad_x * gain
    corr = jnp.sum(grad_n * normed, axis=0, keepdims=True) * (1.0 / dim)
    own[...] = inv_rms * (grad_n - normed * corr)

    prod = grad_x * normed
    col = prod[:, :128]
    for lane in range(128, width, 128):
        col = col + prod[:, lane:lane + 128]
    row = jnp.sum(col.T, axis=0, keepdims=True)
    part_out[0:1, :dim] = row
    part_out[0:1, dim:] = jnp.zeros((1, part_out.shape[1] - dim), F32)
    loss = SOFT_CAP * jnp.sum(kl_ref[...]) + jnp.sum(base_ref[0:1, 0:1]) * (1.0 / n_tp)
    part_out[1:2, :] = jnp.full((1, part_out.shape[1]), loss, F32)
    part_out[2:8, :] = jnp.zeros((6, part_out.shape[1]), F32)

    spread = []
    for k, peer in enumerate(peers):
        spread.append(pltpu.make_async_remote_copy(
            src_ref=own, dst_ref=gh_ref.at[:, mine],
            send_sem=send_sem.at[1, k], recv_sem=recv_sem.at[1, k], device_id=(dp, peer), device_id_type=MESH))
        spread.append(pltpu.make_async_remote_copy(
            src_ref=part_out, dst_ref=parts_buf.at[tp],
            send_sem=send_sem.at[2, k], recv_sem=recv_sem.at[2, k], device_id=(dp, peer), device_id_type=MESH))
    for copy in spread:
        copy.start()
    gh_ref[:, mine] = own[...]
    parts_buf[tp] = part_out[...]
    for copy in spread:
        copy.wait()
    share = parts_buf[0]
    for k in range(1, n_tp):
        share = share + parts_buf[k]
    part_ref[...] = share


def reduce_dx(dx, kl, base, hid_t, gain, n_tp):
    tokens, dim = dx.shape
    width = tokens // n_tp
    whole = pl.BlockSpec(memory_space=VMEM)
    return pl.pallas_call(
        functools.partial(dx_kernel, n_tp),
        in_specs=[whole, whole, whole, whole, whole],
        out_specs=[whole, whole],
        out_shape=[
            jax.ShapeDtypeStruct((dim, tokens), F32),
            jax.ShapeDtypeStruct((8, 640), F32),
        ],
        scratch_shapes=[
            VMEM((n_tp - 1, width, dim), F32), VMEM((dim, width), F32),
            VMEM((n_tp, 8, 640), F32), VMEM((8, 640), F32),
            pltpu.SemaphoreType.DMA((3, n_tp - 1)), pltpu.SemaphoreType.DMA((3, n_tp - 1)),
        ],
        compiler_params=pltpu.CompilerParams(collective_id=1, has_side_effects=True, vmem_limit_bytes=24 * 2**20),
        cost_estimate=pl.CostEstimate(flops=50_000_000_000, bytes_accessed=20_000_000, transcendentals=0),
        name="reduce_dx",
    )(dx, kl, base, hid_t, gain)


def add_kernel(*refs):
    a_ref, b_ref, out_ref = refs[-3], refs[-2], refs[-1]
    out_ref[...] = a_ref[...] + b_ref[...]


def add_chunk(start, size, vocab, own, other, out, after):
    dim = own.shape[0]
    tile = math.gcd(math.gcd(start, size), 512)
    off = start // tile
    hbm = pl.BlockSpec(memory_space=pl.ANY)
    block = pl.BlockSpec((dim, tile), lambda j: (0, j))
    lead = (after,) if out is None else (out,)
    return pl.pallas_call(
        add_kernel,
        grid=(size // tile,),
        in_specs=[hbm, block, block],
        out_specs=pl.BlockSpec((dim, tile), lambda j: (0, j + off)),
        out_shape=jax.ShapeDtypeStruct((dim, vocab), F32),
        input_output_aliases={} if out is None else {0: 0},
        compiler_params=pltpu.CompilerParams(dimension_semantics=("arbitrary",), vmem_limit_bytes=16 * 2**20),
        cost_estimate=pl.CostEstimate(flops=dim * size, bytes_accessed=12 * dim * size, transcendentals=0),
        name="add_chunk",
    )(*lead, own, other)


CHUNKS = (256, 512, 1536, 3584, 3584, 2048, 512, 256)


def solution(mesh):
    n_tp = mesh.shape["tp"]
    swap = [(0, 1), (1, 0)]

    def step(hid_rows, w_final, tab_rows, tea_rows, mask_rows):
        tokens, dim = hid_rows.shape
        vocab = tab_rows.shape[0]
        hid_t = hid_rows.T
        tab_t = tab_rows.T
        mask = mask_rows.reshape(tokens // 128, 128)
        gain = w_final.reshape(1, dim)
        x, x_t, stat = stats(hid_t, gain, mask, tab_t, tea_rows)
        stu_col, tea_col, base = gather_stats(stat, mask, n_tp)
        carry = None
        own, other = [], []
        start = 0
        for size in CHUNKS:
            part, dx, kl = chunk_grad(start, size, x, x_t, stu_col, tea_col, tab_t, tea_rows, carry)
            carry = (dx, kl)
            other.append(lax.ppermute(part, "dp", swap))
            own.append(part)
            start += size
        gh_t, share = reduce_dx(*carry, base, hid_t, gain, n_tp)
        share_other = lax.ppermute(share, "dp", swap)
        share = share + share_other
        out = None
        start = 0
        for size, a, b in zip(CHUNKS, own, other):
            out = add_chunk(start, size, vocab, a, b, out, gh_t)
            start += size
        return share[1, 0], gh_t.T.astype(BF16), share[0, :dim], out.T

    return jax.shard_map(
        step, mesh=mesh,
        in_specs=(P("dp", None), P(None), P("tp", None), P("dp", "tp"), P("dp")),
        out_specs=(P(), P("dp", None), P(None), P("tp", None)), check_vma=False)
```

```python
import functools
import math

import jax
import jax.numpy as jnp
from jax import lax
from jax.experimental import pallas as pl
from jax.experimental.pallas import tpu as pltpu
from jax.sharding import PartitionSpec as P

SOFT_CAP = 30.0
NORM_EPS = 1e-6
INV_CAP = 1.0 / SOFT_CAP
CAP_LOG2E = SOFT_CAP * math.log2(math.e)
MESH = pl.DeviceIdType.MESH
F32 = jnp.float32
BF16 = jnp.bfloat16
GROUP = 16
VMEM = pltpu.VMEM
NT_DIMS = (((1,), (1,)), ((), ()))


STAT_TILE = 1024
STAT_ROWS = 128
PER_BLOCK = STAT_ROWS // GROUP


def stats_kernel(hid_ref, gain_ref, mask_ref, tab_ref, next_ref, tea_ref, x_ref, xt_ref, stat_ref,
                 stu_acc, tea_acc, z_even, z_odd, count_vmem, count_smem, groups, live, sem):
    step = pl.program_id(0)
    dim, tokens = hid_ref.shape
    n_groups = tokens // GROUP

    def source(i):
        return pl.ds(pl.multiple_of(jnp.minimum(groups[i], n_groups - 1) * GROUP, GROUP), GROUP)

    def dest(i):
        return pl.ds(pl.multiple_of(groups[i] * GROUP, GROUP), GROUP)

    def logits(block, table, z_ref):
        rows = jnp.concatenate([x_ref[source(block * PER_BLOCK + i), :] for i in range(PER_BLOCK)], axis=0)
        z_ref[...] = jnp.dot(rows, table[...], preferred_element_type=F32)

    def exp_sum(val):
        val = jnp.exp2(jnp.tanh(val * INV_CAP) * CAP_LOG2E)
        total = val[:, :128]
        for lane in range(128, STAT_TILE, 128):
            total = total + val[:, lane:lane + 128]
        return total

    def accumulate(block, z_ref):
        for i in range(PER_BLOCK):
            at = block * PER_BLOCK + i
            tea_acc[dest(at), :] += exp_sum(tea_ref[source(at), :].astype(F32))
            stu_acc[dest(at), :] += exp_sum(z_ref[i * GROUP:(i + 1) * GROUP, :])

    @pl.when(step == 0)
    def _():
        stu_acc[...] = jnp.zeros_like(stu_acc)
        tea_acc[...] = jnp.zeros_like(tea_acc)
        rows = lax.broadcasted_iota(jnp.int32, (128, 128), 0) // GROUP
        cols = lax.broadcasted_iota(jnp.int32, (128, 128), 1)
        pick = jnp.where(rows == cols, 1.0, 0.0).astype(BF16)
        counts = jnp.dot(mask_ref[...].astype(BF16), pick, preferred_element_type=F32)
        count_vmem[...] = counts.astype(jnp.int32)
        copy = pltpu.make_async_copy(count_vmem, count_smem, sem)
        copy.start()
        gain = jnp.broadcast_to(1.0 + gain_ref[...], (128, gain_ref.shape[1])).T[:dim, :]
        for blk in range(tokens // 128):
            hid = hid_ref[:, blk * 128:(blk + 1) * 128].astype(F32)
            inv_rms = lax.rsqrt(jnp.sum(hid * hid, axis=0, keepdims=True) * (1.0 / dim) + NORM_EPS)
            x_t = hid * inv_rms * gain
            x_t = x_t.astype(BF16)
            xt_ref[:, blk * 128:(blk + 1) * 128] = x_t
            x_ref[blk * 128:(blk + 1) * 128, :] = x_t.T
        copy.wait()

        def add_group(g, n):
            groups[n] = g
            keep = count_smem[g // 8, g % 8] > 0
            return n + jnp.where(keep, 1, 0)

        n_live = lax.fori_loop(0, n_groups, add_group, 0)

        def pad(i, c):
            groups[n_live + i] = n_groups
            return c

        lax.fori_loop(0, 2 * PER_BLOCK, pad, 0)
        live[0] = n_live
        logits(0, tab_ref, z_even)

    more = jnp.maximum((live[0] + 2 * PER_BLOCK - 1) // (2 * PER_BLOCK) - 1, 0)

    def pair(p, c):
        logits(2 * p + 1, tab_ref, z_odd)
        accumulate(2 * p, z_even)
        logits(2 * p + 2, tab_ref, z_even)
        accumulate(2 * p + 1, z_odd)
        return c

    lax.fori_loop(0, more, pair, 0)
    logits(2 * more + 1, tab_ref, z_odd)
    accumulate(2 * more, z_even)
    logits(0, next_ref, z_even)
    accumulate(2 * more + 1, z_odd)

    @pl.when(step == pl.num_programs(0) - 1)
    def _():
        for blk in range(tokens // 128):
            for k, acc in enumerate((stu_acc, tea_acc)):
                part = acc[blk * 128:(blk + 1) * 128, :].T
                stat_ref[k * 16 + blk:k * 16 + blk + 1, :] = jnp.sum(part, axis=0, keepdims=True)


def stats(hid_t, gain, mask, tab_t, tea):
    dim, tokens = hid_t.shape
    vocab = tab_t.shape[1]
    n_groups = tokens // GROUP
    whole = pl.BlockSpec(memory_space=VMEM)
    return pl.pallas_call(
        stats_kernel,
        grid=(vocab // STAT_TILE,),
        in_specs=[
            whole, whole, whole,
            pl.BlockSpec((dim, STAT_TILE), lambda j: (0, j)),
            pl.BlockSpec((dim, STAT_TILE), lambda j: (0, jnp.minimum(j + 1, vocab // STAT_TILE - 1))),
            pl.BlockSpec((tokens, STAT_TILE), lambda j: (0, j)),
        ],
        out_specs=[whole, whole, whole],
        out_shape=[
            jax.ShapeDtypeStruct((tokens, dim), BF16),
            jax.ShapeDtypeStruct((dim, tokens), BF16),
            jax.ShapeDtypeStruct((32, 128), F32),
        ],
        scratch_shapes=[
            VMEM((tokens + GROUP, 128), F32), VMEM((tokens + GROUP, 128), F32),
            VMEM((STAT_ROWS, STAT_TILE), F32), VMEM((STAT_ROWS, STAT_TILE), F32),
            VMEM((16, 128), jnp.int32), pltpu.SMEM((16, 128), jnp.int32),
            pltpu.SMEM((n_groups + 4 * PER_BLOCK,), jnp.int32), pltpu.SMEM((1,), jnp.int32),
            pltpu.SemaphoreType.DMA,
        ],
        compiler_params=pltpu.CompilerParams(dimension_semantics=("arbitrary",), vmem_limit_bytes=46 * 2**20),
        cost_estimate=pl.CostEstimate(flops=50_000_000_000, bytes_accessed=70_000_000, transcendentals=0),
        name="stats",
    )(hid_t, gain, mask, tab_t, tab_t, tea)


GRAD_TILE = 256
GRAD_ROWS = 256
SLICE = 16


def head_kernel(n_tp, stat_ref, mask_ref, x_ref, xt_ref, tab_hbm, tea_hbm, stu_col, tea_col, base_ref, de_ref, kl_acc, g_ref,
                slots, mask_slot, tab_ref, tea_ref, stu_q, tea_q, z_even, z_odd, load_sem, send_sem, recv_sem):
    tp = lax.axis_index("tp")
    dp = lax.axis_index("dp")
    tokens = x_ref.shape[0]
    n_blocks = tokens // GRAD_ROWS
    load_tab = pltpu.make_async_copy(tab_hbm.at[:, 0:GRAD_TILE], tab_ref, load_sem.at[0])
    load_tea = pltpu.make_async_copy(tea_hbm.at[:, 0:GRAD_TILE], tea_ref, load_sem.at[1])
    load_tab.start()
    load_tea.start()
    barrier = pltpu.get_barrier_semaphore()
    peers = [(dp, lax.rem(tp + k, n_tp)) for k in range(1, n_tp)] + [(1 - dp, tp)]
    for peer in peers:
        pl.semaphore_signal(barrier, inc=1, device_id=peer, device_id_type=MESH)
    pl.semaphore_wait(barrier, len(peers))
    copies = []
    for k, peer in enumerate(peers):
        last = k == n_tp - 1
        copies.append(pltpu.make_async_remote_copy(
            src_ref=mask_ref if last else stat_ref,
            dst_ref=mask_slot if last else slots.at[k],
            send_sem=send_sem.at[k], recv_sem=recv_sem.at[k], device_id=peer, device_id_type=MESH))
        copies[-1].start()
    load_tab.wait()
    load_tea.wait()

    def window(b, size=GRAD_ROWS, skip=0):
        return pl.ds(pl.multiple_of(b * GRAD_ROWS + skip, size), size)

    def logits(b, z_ref):
        z_ref[...] = jnp.dot(x_ref[window(b), :], tab_ref[...], preferred_element_type=F32)

    def factors(b, z_ref):
        for skip in range(0, GRAD_ROWS, SLICE):
            rows = window(b, SLICE, skip)
            kl = 0.0
            for lane in range(0, GRAD_TILE, 128):
                stu = jnp.tanh(z_ref[skip:skip + SLICE, lane:lane + 128] * INV_CAP)
                tea = jnp.tanh(tea_ref[rows, lane:lane + 128].astype(F32) * INV_CAP)
                tea_e = jnp.exp2(tea * CAP_LOG2E)
                slope = 1.0 - stu * stu
                kl = kl + tea_e * (tea - stu)
                stu_q[rows, lane:lane + 128] = jnp.exp2(stu * CAP_LOG2E) * slope
                tea_q[rows, lane:lane + 128] = tea_e * slope
            kl_acc[rows, :] = kl

    logits(0, z_even)

    def pair(p, c):
        logits(2 * p + 1, z_odd)
        factors(2 * p, z_even)
        logits(lax.rem(2 * p + 2, n_blocks), z_even)
        factors(2 * p + 1, z_odd)
        return c

    lax.fori_loop(0, n_blocks // 2, pair, 0)

    for copy in copies:
        copy.wait()
    parts = [stat_ref[...]] + [slots[k] for k in range(n_tp - 1)]
    total = jnp.zeros_like(parts[0])
    for owner in range(n_tp):
        gap = lax.rem(tp - owner + n_tp, n_tp)
        part = parts[0]
        for k in range(1, n_tp):
            part = jnp.where(gap == k, parts[k], part)
        total = total + part
    total = jnp.where(total > 0.0, total, 1.0)
    mask = mask_ref[...]
    mask_sum = jnp.sum(mask) + jnp.sum(mask_slot[...])
    weight = mask / mask_sum
    stu_sum, tea_sum = total[:16, :], total[16:, :]
    base = jnp.sum(weight * (jnp.log(stu_sum) - jnp.log(tea_sum)))
    base_ref[...] = jnp.full((8, 128), base, F32)
    stu_row, tea_row = weight / stu_sum, weight / tea_sum
    for blk in range(tokens // 128):
        rows = slice(blk * 128, (blk + 1) * 128)
        stu_scale = jnp.broadcast_to(stu_row[blk:blk + 1, :], (128, 128)).T
        tea_scale = jnp.broadcast_to(tea_row[blk:blk + 1, :], (128, 128)).T
        stu_col[rows, :] = stu_scale
        tea_col[rows, :] = tea_scale
        kl_acc[rows, :] = kl_acc[rows, :] * tea_scale
        for lane in range(0, GRAD_TILE, 128):
            lanes = slice(lane, lane + 128)
            g_ref[rows, lanes] = (stu_q[rows, lanes] * stu_scale - tea_q[rows, lanes] * tea_scale).astype(BF16)
    de_ref[...] = jnp.dot(xt_ref[...], g_ref[...], preferred_element_type=F32)


def head(stat, mask, x, x_t, tab_t, tea, n_tp):
    tokens, dim = x.shape
    whole = pl.BlockSpec(memory_space=VMEM)
    hbm = pl.BlockSpec(memory_space=pl.ANY)
    return pl.pallas_call(
        functools.partial(head_kernel, n_tp),
        in_specs=[whole, whole, whole, whole, hbm, hbm],
        out_specs=[whole] * 6,
        out_shape=[
            jax.ShapeDtypeStruct((tokens, 128), F32),
            jax.ShapeDtypeStruct((tokens, 128), F32),
            jax.ShapeDtypeStruct((8, 128), F32),
            jax.ShapeDtypeStruct((dim, GRAD_TILE), F32),
            jax.ShapeDtypeStruct((tokens, 128), F32),
            jax.ShapeDtypeStruct((tokens, GRAD_TILE), BF16),
        ],
        scratch_shapes=[
            VMEM((n_tp - 1,) + stat.shape, F32), VMEM(mask.shape, F32),
            VMEM((dim, GRAD_TILE), BF16), VMEM((tokens, GRAD_TILE), BF16),
            VMEM((tokens, GRAD_TILE), F32), VMEM((tokens, GRAD_TILE), F32),
            VMEM((GRAD_ROWS, GRAD_TILE), F32), VMEM((GRAD_ROWS, GRAD_TILE), F32),
            pltpu.SemaphoreType.DMA((2,)), pltpu.SemaphoreType.DMA((n_tp,)), pltpu.SemaphoreType.DMA((n_tp,)),
        ],
        compiler_params=pltpu.CompilerParams(collective_id=0, has_side_effects=True, vmem_limit_bytes=40 * 2**20),
        cost_estimate=pl.CostEstimate(flops=5_000_000_000, bytes_accessed=2_000_000, transcendentals=0),
        name="head",
    )(stat, mask, x, x_t, tab_t, tea)


def chunk_kernel(first, x_ref, xt_ref, stu_col, tea_col, tab_ref, tea_ref, _, *refs):
    if first:
        head_g, head_tab, de_ref, kl_acc, dx_acc, g_ref, z_even, z_odd = refs
    else:
        _, de_ref, kl_acc, dx_acc, g_ref, z_even, z_odd = refs
    tokens = x_ref.shape[0]
    n_blocks = tokens // GRAD_ROWS

    if first:
        @pl.when(pl.program_id(0) == 0)
        def _():
            def block(b, c):
                rows = pl.ds(pl.multiple_of(b * GRAD_ROWS, GRAD_ROWS), GRAD_ROWS)
                dx_acc[rows, :] = lax.dot_general(head_g[rows, :], head_tab[...], NT_DIMS, preferred_element_type=F32)
                return c

            lax.fori_loop(0, n_blocks, block, 0)

    def window(b, size=GRAD_ROWS, skip=0):
        return pl.ds(pl.multiple_of(b * GRAD_ROWS + skip, size), size)

    def logits(b, z_ref):
        z_ref[...] = jnp.dot(x_ref[window(b), :], tab_ref[...], preferred_element_type=F32)

    def grads(b, z_ref):
        for skip in range(0, GRAD_ROWS, SLICE):
            rows = window(b, SLICE, skip)
            stu_scale = stu_col[rows, :]
            tea_scale = tea_col[rows, :]
            kl = kl_acc[rows, :]
            parts = []
            for lane in range(0, GRAD_TILE, 128):
                stu = jnp.tanh(z_ref[skip:skip + SLICE, lane:lane + 128] * INV_CAP)
                tea = jnp.tanh(tea_ref[rows, lane:lane + 128].astype(F32) * INV_CAP)
                stu_p = jnp.exp2(stu * CAP_LOG2E) * stu_scale
                tea_p = jnp.exp2(tea * CAP_LOG2E) * tea_scale
                kl = kl + tea_p * (tea - stu)
                parts.append(((stu_p - tea_p) * (1.0 - stu * stu)).astype(BF16))
            kl_acc[rows, :] = kl
            g_ref[rows, :] = jnp.concatenate(parts, axis=1)

    def add_dx(b):
        dx_acc[window(b), :] += lax.dot_general(g_ref[window(b), :], tab_ref[...], NT_DIMS, preferred_element_type=F32)

    logits(0, z_even)
    logits(1, z_odd)
    grads(0, z_even)

    def pair(p, c):
        add_dx(2 * p)
        logits(2 * p + 2, z_even)
        grads(2 * p + 1, z_odd)
        add_dx(2 * p + 1)
        logits(2 * p + 3, z_odd)
        grads(2 * p + 2, z_even)
        return c

    lax.fori_loop(0, n_blocks // 2 - 1, pair, 0)
    add_dx(n_blocks - 2)
    grads(n_blocks - 1, z_odd)
    de_ref[...] = jnp.dot(xt_ref[...], g_ref[...], preferred_element_type=F32)
    add_dx(n_blocks - 1)


def chunk_grad(start, size, x, x_t, stu_col, tea_col, tab_t, tea, kl, dx, head_g):
    tokens, dim = x.shape
    off = start // GRAD_TILE
    whole = pl.BlockSpec(memory_space=VMEM)
    first = dx is None
    work = tokens * size
    return pl.pallas_call(
        functools.partial(chunk_kernel, first),
        grid=(size // GRAD_TILE,),
        in_specs=[
            whole, whole, whole, whole,
            pl.BlockSpec((dim, GRAD_TILE), lambda j: (0, j + off)),
            pl.BlockSpec((tokens, GRAD_TILE), lambda j: (0, j + off)),
            whole,
        ] + ([whole, pl.BlockSpec((dim, GRAD_TILE), lambda j: (0, 0))] if first else [whole]),
        out_specs=[pl.BlockSpec((dim, GRAD_TILE), lambda j: (0, j)), whole, whole],
        out_shape=[
            jax.ShapeDtypeStruct((dim, size), F32),
            jax.ShapeDtypeStruct((tokens, 128), F32),
            jax.ShapeDtypeStruct((tokens, dim), F32),
        ],
        scratch_shapes=[
            VMEM((tokens, GRAD_TILE), BF16), VMEM((GRAD_ROWS, GRAD_TILE), F32), VMEM((GRAD_ROWS, GRAD_TILE), F32),
        ],
        input_output_aliases={6: 1} if first else {6: 1, 7: 2},
        compiler_params=pltpu.CompilerParams(dimension_semantics=("arbitrary",), vmem_limit_bytes=32 * 2**20),
        cost_estimate=pl.CostEstimate(flops=work * 3 * 2 * dim, bytes_accessed=work * 2, transcendentals=0),
        name="chunk_grad",
    )(x, x_t, stu_col, tea_col, tab_t, tea, kl, *((head_g, tab_t) if first else (dx,)))


def dx_kernel(n_tp, dx_ref, kl_ref, base_ref, hid_ref, gain_ref, gh_ref, part_ref,
              slots, own, parts_buf, part_out, send_sem, recv_sem):
    tp = lax.axis_index("tp")
    dp = lax.axis_index("dp")
    dim, tokens = hid_ref.shape
    width = tokens // n_tp
    barrier = pltpu.get_barrier_semaphore()
    peers = [lax.rem(tp + k, n_tp) for k in range(1, n_tp)]
    for peer in peers:
        pl.semaphore_signal(barrier, inc=1, device_id=(dp, peer), device_id_type=MESH)
    pl.semaphore_wait(barrier, n_tp - 1)

    def window(index):
        return pl.ds(pl.multiple_of(index * width, width), width)

    reduce = []
    for k, peer in enumerate(peers):
        reduce.append(pltpu.make_async_remote_copy(
            src_ref=dx_ref.at[window(peer), :], dst_ref=slots.at[k],
            send_sem=send_sem.at[0, k], recv_sem=recv_sem.at[0, k], device_id=(dp, peer), device_id_type=MESH))
        reduce[-1].start()
    for copy in reduce:
        copy.wait()
    mine = window(tp)
    total = jnp.zeros((width, dim), F32)
    for owner in range(n_tp):
        gap = lax.rem(tp - owner + n_tp, n_tp)
        part = dx_ref[mine, :]
        for k in range(1, n_tp):
            part = jnp.where(gap == k, slots[k - 1], part)
        total = total + part
    grad_x = total.T
    gain = jnp.broadcast_to(1.0 + gain_ref[...], (128, gain_ref.shape[1])).T[:dim, :1]
    hid = hid_ref[:, mine].astype(F32)
    inv_rms = lax.rsqrt(jnp.sum(hid * hid, axis=0, keepdims=True) * (1.0 / dim) + NORM_EPS)
    normed = hid * inv_rms
    grad_n = grad_x * gain
    corr = jnp.sum(grad_n * normed, axis=0, keepdims=True) * (1.0 / dim)
    own[...] = inv_rms * (grad_n - normed * corr)

    prod = grad_x * normed
    col = prod[:, :128]
    for lane in range(128, width, 128):
        col = col + prod[:, lane:lane + 128]
    row = jnp.sum(col.T, axis=0, keepdims=True)
    part_out[0:1, :dim] = row
    part_out[0:1, dim:] = jnp.zeros((1, part_out.shape[1] - dim), F32)
    loss = SOFT_CAP * jnp.sum(kl_ref[...]) + jnp.sum(base_ref[0:1, 0:1]) * (1.0 / n_tp)
    part_out[1:2, :] = jnp.full((1, part_out.shape[1]), loss, F32)
    part_out[2:8, :] = jnp.zeros((6, part_out.shape[1]), F32)

    spread = []
    for k, peer in enumerate(peers):
        spread.append(pltpu.make_async_remote_copy(
            src_ref=own, dst_ref=gh_ref.at[:, mine],
            send_sem=send_sem.at[1, k], recv_sem=recv_sem.at[1, k], device_id=(dp, peer), device_id_type=MESH))
        spread.append(pltpu.make_async_remote_copy(
            src_ref=part_out, dst_ref=parts_buf.at[tp],
            send_sem=send_sem.at[2, k], recv_sem=recv_sem.at[2, k], device_id=(dp, peer), device_id_type=MESH))
    for copy in spread:
        copy.start()
    gh_ref[:, mine] = own[...]
    parts_buf[tp] = part_out[...]
    for copy in spread:
        copy.wait()
    share = parts_buf[0]
    for k in range(1, n_tp):
        share = share + parts_buf[k]
    part_ref[...] = share


def reduce_dx(dx, kl, base, hid_t, gain, n_tp):
    tokens, dim = dx.shape
    width = tokens // n_tp
    whole = pl.BlockSpec(memory_space=VMEM)
    return pl.pallas_call(
        functools.partial(dx_kernel, n_tp),
        in_specs=[whole, whole, whole, whole, whole],
        out_specs=[whole, whole],
        out_shape=[
            jax.ShapeDtypeStruct((dim, tokens), F32),
            jax.ShapeDtypeStruct((8, 640), F32),
        ],
        scratch_shapes=[
            VMEM((n_tp - 1, width, dim), F32), VMEM((dim, width), F32),
            VMEM((n_tp, 8, 640), F32), VMEM((8, 640), F32),
            pltpu.SemaphoreType.DMA((3, n_tp - 1)), pltpu.SemaphoreType.DMA((3, n_tp - 1)),
        ],
        compiler_params=pltpu.CompilerParams(collective_id=1, has_side_effects=True, vmem_limit_bytes=24 * 2**20),
        cost_estimate=pl.CostEstimate(flops=50_000_000_000, bytes_accessed=20_000_000, transcendentals=0),
        name="reduce_dx",
    )(dx, kl, base, hid_t, gain)


def add_kernel(*refs):
    a_ref, b_ref, out_ref = refs[-3], refs[-2], refs[-1]
    out_ref[...] = a_ref[...] + b_ref[...]


def add_chunk(start, size, vocab, own, other, out, after):
    dim = own.shape[0]
    tile = math.gcd(math.gcd(start, size), 512)
    off = start // tile
    hbm = pl.BlockSpec(memory_space=pl.ANY)
    block = pl.BlockSpec((dim, tile), lambda j: (0, j))
    lead = (after,) if out is None else (out,)
    return pl.pallas_call(
        add_kernel,
        grid=(size // tile,),
        in_specs=[hbm, block, block],
        out_specs=pl.BlockSpec((dim, tile), lambda j: (0, j + off)),
        out_shape=jax.ShapeDtypeStruct((dim, vocab), F32),
        input_output_aliases={} if out is None else {0: 0},
        compiler_params=pltpu.CompilerParams(dimension_semantics=("arbitrary",), vmem_limit_bytes=16 * 2**20),
        cost_estimate=pl.CostEstimate(flops=dim * size, bytes_accessed=12 * dim * size, transcendentals=0),
        name="add_chunk",
    )(*lead, own, other)


CHUNKS = (GRAD_TILE, 512, 1536, 3584, 3584, 2048, 512, 256)


def solution(mesh):
    n_tp = mesh.shape["tp"]
    swap = [(0, 1), (1, 0)]

    def step(hid_rows, w_final, tab_rows, tea_rows, mask_rows):
        tokens, dim = hid_rows.shape
        vocab = tab_rows.shape[0]
        hid_t = hid_rows.T
        tab_t = tab_rows.T
        mask = mask_rows.reshape(tokens // 128, 128)
        gain = w_final.reshape(1, dim)
        x, x_t, stat = stats(hid_t, gain, mask, tab_t, tea_rows)
        stu_col, tea_col, base, part, kl, head_g = head(stat, mask, x, x_t, tab_t, tea_rows, n_tp)
        dx = None
        own, other = [], []
        start = 0
        for c, size in enumerate(CHUNKS):
            if c:
                part, kl, dx = chunk_grad(start, size, x, x_t, stu_col, tea_col, tab_t, tea_rows, kl, dx, head_g)
            other.append(lax.ppermute(part, "dp", swap))
            own.append(part)
            start += size
        gh_t, share = reduce_dx(dx, kl, base, hid_t, gain, n_tp)
        share_other = lax.ppermute(share, "dp", swap)
        share = share + share_other
        out = None
        start = 0
        for size, a, b in zip(CHUNKS, own, other):
            out = add_chunk(start, size, vocab, a, b, out, gh_t)
            start += size
        return share[1, 0], gh_t.T.astype(BF16), share[0, :dim], out.T

    return jax.shard_map(
        step, mesh=mesh,
        in_specs=(P("dp", None), P(None), P("tp", None), P("dp", "tp"), P("dp")),
        out_specs=(P(), P("dp", None), P(None), P("tp", None)), check_vma=False)
```

```python
import functools
import math

import jax
import jax.numpy as jnp
from jax import lax
from jax.experimental import pallas as pl
from jax.experimental.pallas import tpu as pltpu
from jax.sharding import PartitionSpec as P

SOFT_CAP = 30.0
NORM_EPS = 1e-6
INV_CAP = 1.0 / SOFT_CAP
CAP_LOG2E = SOFT_CAP * math.log2(math.e)
MESH = pl.DeviceIdType.MESH
F32 = jnp.float32
BF16 = jnp.bfloat16
GROUP = 16
VMEM = pltpu.VMEM
NT_DIMS = (((1,), (1,)), ((), ()))


SHARED = 256


def lift_kernel(hid_hbm, tea_hbm, hid_ref, hid_out, tea_out, tea_ref, sem):
    tp = lax.axis_index("tp")
    width = hid_out.shape[1]
    start = tea_hbm.shape[1] - SHARED
    loads = [
        pltpu.make_async_copy(hid_hbm, hid_ref, sem.at[0]),
        pltpu.make_async_copy(tea_hbm.at[:, start:start + SHARED], tea_ref, sem.at[1]),
    ]
    for load in loads:
        load.start()
    loads[0].wait()
    hid_out[...] = hid_ref[:, pl.ds(pl.multiple_of(tp * width, width), width)].astype(F32)
    loads[1].wait()
    tea_out[...] = tea_ref[...].astype(F32)


def lift(hid_t, tea, n_tp):
    dim, tokens = hid_t.shape
    hbm = pl.BlockSpec(memory_space=pl.ANY)
    whole = pl.BlockSpec(memory_space=VMEM)
    return pl.pallas_call(
        lift_kernel,
        in_specs=[hbm, hbm],
        out_specs=[whole, whole, whole],
        out_shape=[
            jax.ShapeDtypeStruct((dim, tokens), BF16),
            jax.ShapeDtypeStruct((dim, tokens // n_tp), F32),
            jax.ShapeDtypeStruct((tokens, SHARED), F32),
        ],
        scratch_shapes=[VMEM((tokens, SHARED), BF16), pltpu.SemaphoreType.DMA((2,))],
        compiler_params=pltpu.CompilerParams(vmem_limit_bytes=48 * 2**20),
        cost_estimate=pl.CostEstimate(flops=3_000_000, bytes_accessed=5_000_000, transcendentals=0),
        name="lift",
    )(hid_t, tea)


def join_kernel(n_tp, *refs):
    out_ref = refs[-1]
    tp = lax.axis_index("tp")
    width = refs[0].shape[1]
    for k, ref in enumerate(refs[:-1]):
        owner = lax.rem(tp - k + n_tp, n_tp)
        out_ref[:, pl.ds(pl.multiple_of(owner * width, width), width)] = ref[...].astype(BF16)


def join(parts, n_tp):
    dim, width = parts[0].shape
    whole = pl.BlockSpec(memory_space=VMEM)
    return pl.pallas_call(
        functools.partial(join_kernel, n_tp),
        in_specs=[whole] * n_tp,
        out_specs=whole,
        out_shape=jax.ShapeDtypeStruct((dim, width * n_tp), BF16),
        compiler_params=pltpu.CompilerParams(vmem_limit_bytes=16 * 2**20),
        cost_estimate=pl.CostEstimate(flops=3_000_000, bytes_accessed=5_000_000, transcendentals=0),
        name="join",
    )(*parts)


def make_x(hid_ref, gain_ref, x_ref, xt_ref):
    dim, tokens = hid_ref.shape
    gain = jnp.broadcast_to(1.0 + gain_ref[...], (128, gain_ref.shape[1])).T[:dim, :]
    for blk in range(tokens // 128):
        hid = hid_ref[:, blk * 128:(blk + 1) * 128].astype(F32)
        inv_rms = lax.rsqrt(jnp.sum(hid * hid, axis=0, keepdims=True) * (1.0 / dim) + NORM_EPS)
        x_t = (hid * inv_rms * gain).astype(BF16)
        xt_ref[:, blk * 128:(blk + 1) * 128] = x_t
        x_ref[blk * 128:(blk + 1) * 128, :] = x_t.T


def shared_kernel(hid_ref, gain_ref, row_ref, tab_ref, tea_ref, de_ref, x_ref, xt_ref, g_ref):
    tokens = x_ref.shape[0]
    make_x(hid_ref, gain_ref, x_ref, xt_ref)
    for blk in range(tokens // 128):
        rows = slice(blk * 128, (blk + 1) * 128)
        stu_scale = jnp.broadcast_to(row_ref[blk:blk + 1, :], (128, 128)).T
        tea_scale = jnp.broadcast_to(row_ref[16 + blk:17 + blk, :], (128, 128)).T
        z = jnp.dot(x_ref[rows, :], tab_ref[...], preferred_element_type=F32)
        for lane in range(0, SHARED, 128):
            lanes = slice(lane, lane + 128)
            stu = jnp.tanh(z[:, lanes] * INV_CAP)
            tea = jnp.tanh(tea_ref[rows, lanes] * INV_CAP)
            stu_p = jnp.exp2(stu * CAP_LOG2E) * stu_scale
            tea_p = jnp.exp2(tea * CAP_LOG2E) * tea_scale
            g_ref[rows, lanes] = ((stu_p - tea_p) * (1.0 - stu * stu)).astype(BF16)
    de_ref[...] = jnp.dot(xt_ref[...], g_ref[...], preferred_element_type=F32)


def shared_grad(hid_t, gain, scale_rows, tab_t, tea):
    dim, tokens = hid_t.shape
    last = tab_t.shape[1] // SHARED - 1

    def spec(shape):
        return pl.BlockSpec(shape, lambda j: (0, 0))

    return pl.pallas_call(
        shared_kernel,
        grid=(1,),
        in_specs=[
            spec(hid_t.shape), spec(gain.shape), spec(scale_rows.shape),
            pl.BlockSpec((dim, SHARED), lambda j: (0, last)), spec(tea.shape),
        ],
        out_specs=spec((dim, SHARED)),
        out_shape=jax.ShapeDtypeStruct((dim, SHARED), F32),
        scratch_shapes=[VMEM((tokens, dim), BF16), VMEM((dim, tokens), BF16), VMEM((tokens, SHARED), BF16)],
        compiler_params=pltpu.CompilerParams(dimension_semantics=("arbitrary",), vmem_limit_bytes=40 * 2**20),
        cost_estimate=pl.CostEstimate(flops=tokens * SHARED * 4 * dim, bytes_accessed=tokens * SHARED * 4, transcendentals=0),
        name="shared_grad",
    )(hid_t, gain, scale_rows, tab_t, tea)


STAT_TILE = 1024
STAT_ROWS = 128
PER_BLOCK = STAT_ROWS // GROUP


def stats_kernel(hid_ref, gain_ref, mask_ref, tab_ref, next_ref, tea_ref, x_ref, xt_ref, stat_ref,
                 stu_acc, tea_acc, z_even, z_odd, count_vmem, count_smem, groups, live, sem):
    step = pl.program_id(0)
    _, tokens = hid_ref.shape
    n_groups = tokens // GROUP

    def source(i):
        return pl.ds(pl.multiple_of(jnp.minimum(groups[i], n_groups - 1) * GROUP, GROUP), GROUP)

    def dest(i):
        return pl.ds(pl.multiple_of(groups[i] * GROUP, GROUP), GROUP)

    def logits(block, table, z_ref):
        rows = jnp.concatenate([x_ref[source(block * PER_BLOCK + i), :] for i in range(PER_BLOCK)], axis=0)
        z_ref[...] = jnp.dot(rows, table[...], preferred_element_type=F32)

    def exp_sum(val):
        val = jnp.exp2(jnp.tanh(val * INV_CAP) * CAP_LOG2E)
        total = val[:, :128]
        for lane in range(128, STAT_TILE, 128):
            total = total + val[:, lane:lane + 128]
        return total

    def accumulate(block, z_ref):
        for i in range(PER_BLOCK):
            at = block * PER_BLOCK + i
            tea_acc[dest(at), :] += exp_sum(tea_ref[source(at), :].astype(F32))
            stu_acc[dest(at), :] += exp_sum(z_ref[i * GROUP:(i + 1) * GROUP, :])

    @pl.when(step == 0)
    def _():
        stu_acc[...] = jnp.zeros_like(stu_acc)
        tea_acc[...] = jnp.zeros_like(tea_acc)
        rows = lax.broadcasted_iota(jnp.int32, (128, 128), 0) // GROUP
        cols = lax.broadcasted_iota(jnp.int32, (128, 128), 1)
        pick = jnp.where(rows == cols, 1.0, 0.0).astype(BF16)
        counts = jnp.dot(mask_ref[...].astype(BF16), pick, preferred_element_type=F32)
        count_vmem[...] = counts.astype(jnp.int32)
        copy = pltpu.make_async_copy(count_vmem, count_smem, sem)
        copy.start()
        make_x(hid_ref, gain_ref, x_ref, xt_ref)
        copy.wait()

        def add_group(g, n):
            groups[n] = g
            keep = count_smem[g // 8, g % 8] > 0
            return n + jnp.where(keep, 1, 0)

        n_live = lax.fori_loop(0, n_groups, add_group, 0)

        def pad(i, c):
            groups[n_live + i] = n_groups
            return c

        lax.fori_loop(0, 2 * PER_BLOCK, pad, 0)
        live[0] = n_live
        logits(0, tab_ref, z_even)

    n_blocks = jnp.maximum((live[0] + PER_BLOCK - 1) // PER_BLOCK, 1)
    more = (n_blocks - 1) // 2

    def pair(p, c):
        logits(2 * p + 1, tab_ref, z_odd)
        accumulate(2 * p, z_even)
        logits(2 * p + 2, tab_ref, z_even)
        accumulate(2 * p + 1, z_odd)
        return c

    lax.fori_loop(0, more, pair, 0)

    @pl.when(n_blocks % 2 == 0)
    def _():
        logits(2 * more + 1, tab_ref, z_odd)
        accumulate(2 * more, z_even)
        logits(0, next_ref, z_even)
        accumulate(2 * more + 1, z_odd)

    @pl.when(n_blocks % 2 == 1)
    def _():
        logits(0, next_ref, z_odd)
        accumulate(2 * more, z_even)
        z_even[...] = z_odd[...]

    @pl.when(step == pl.num_programs(0) - 1)
    def _():
        for blk in range(tokens // 128):
            for k, acc in enumerate((stu_acc, tea_acc)):
                part = acc[blk * 128:(blk + 1) * 128, :].T
                stat_ref[k * 16 + blk:k * 16 + blk + 1, :] = jnp.sum(part, axis=0, keepdims=True)


def stats(hid_t, gain, mask, tab_t, tea):
    dim, tokens = hid_t.shape
    vocab = tab_t.shape[1]
    n_groups = tokens // GROUP
    whole = pl.BlockSpec(memory_space=VMEM)
    return pl.pallas_call(
        stats_kernel,
        grid=(vocab // STAT_TILE,),
        in_specs=[
            whole, whole, whole,
            pl.BlockSpec((dim, STAT_TILE), lambda j: (0, j)),
            pl.BlockSpec((dim, STAT_TILE), lambda j: (0, jnp.minimum(j + 1, vocab // STAT_TILE - 1))),
            pl.BlockSpec((tokens, STAT_TILE), lambda j: (0, j)),
        ],
        out_specs=[whole, whole, whole],
        out_shape=[
            jax.ShapeDtypeStruct((tokens, dim), BF16),
            jax.ShapeDtypeStruct((dim, tokens), BF16),
            jax.ShapeDtypeStruct((32, 128), F32),
        ],
        scratch_shapes=[
            VMEM((tokens + GROUP, 128), F32), VMEM((tokens + GROUP, 128), F32),
            VMEM((STAT_ROWS, STAT_TILE), F32), VMEM((STAT_ROWS, STAT_TILE), F32),
            VMEM((16, 128), jnp.int32), pltpu.SMEM((16, 128), jnp.int32),
            pltpu.SMEM((n_groups + 4 * PER_BLOCK,), jnp.int32), pltpu.SMEM((1,), jnp.int32),
            pltpu.SemaphoreType.DMA,
        ],
        compiler_params=pltpu.CompilerParams(dimension_semantics=("arbitrary",), vmem_limit_bytes=46 * 2**20),
        cost_estimate=pl.CostEstimate(flops=50_000_000_000, bytes_accessed=70_000_000, transcendentals=0),
        name="stats",
    )(hid_t, gain, mask, tab_t, tab_t, tea)


GRAD_TILE = 256
GRAD_ROWS = 256
SLICE = 16


def head_kernel(n_tp, stat_ref, mask_ref, x_ref, xt_ref, tab_hbm, tea_hbm, stu_col, tea_col, base_ref, row_ref, de_ref, kl_acc, g_ref,
                slots, mask_slot, tab_ref, tea_ref, stu_q, tea_q, z_even, z_odd, load_sem, send_sem, recv_sem):
    tp = lax.axis_index("tp")
    dp = lax.axis_index("dp")
    tokens = x_ref.shape[0]
    n_blocks = tokens // GRAD_ROWS
    load_tab = pltpu.make_async_copy(tab_hbm.at[:, 0:GRAD_TILE], tab_ref, load_sem.at[0])
    load_tea = pltpu.make_async_copy(tea_hbm.at[:, 0:GRAD_TILE], tea_ref, load_sem.at[1])
    load_tab.start()
    load_tea.start()
    barrier = pltpu.get_barrier_semaphore()
    peers = [(dp, lax.rem(tp + k, n_tp)) for k in range(1, n_tp)] + [(1 - dp, tp)]
    for peer in peers:
        pl.semaphore_signal(barrier, inc=1, device_id=peer, device_id_type=MESH)
    pl.semaphore_wait(barrier, len(peers))
    copies = []
    for k, peer in enumerate(peers):
        last = k == n_tp - 1
        copies.append(pltpu.make_async_remote_copy(
            src_ref=mask_ref if last else stat_ref,
            dst_ref=mask_slot if last else slots.at[k],
            send_sem=send_sem.at[k], recv_sem=recv_sem.at[k], device_id=peer, device_id_type=MESH))
        copies[-1].start()
    load_tab.wait()
    load_tea.wait()

    def window(b, size=GRAD_ROWS, skip=0):
        return pl.ds(pl.multiple_of(b * GRAD_ROWS + skip, size), size)

    def logits(b, z_ref):
        z_ref[...] = jnp.dot(x_ref[window(b), :], tab_ref[...], preferred_element_type=F32)

    def factors(b, z_ref):
        for skip in range(0, GRAD_ROWS, SLICE):
            rows = window(b, SLICE, skip)
            kl = 0.0
            for lane in range(0, GRAD_TILE, 128):
                stu = jnp.tanh(z_ref[skip:skip + SLICE, lane:lane + 128] * INV_CAP)
                tea = jnp.tanh(tea_ref[rows, lane:lane + 128].astype(F32) * INV_CAP)
                tea_e = jnp.exp2(tea * CAP_LOG2E)
                slope = 1.0 - stu * stu
                kl = kl + tea_e * (tea - stu)
                stu_q[rows, lane:lane + 128] = jnp.exp2(stu * CAP_LOG2E) * slope
                tea_q[rows, lane:lane + 128] = tea_e * slope
            kl_acc[rows, :] = kl

    logits(0, z_even)

    def pair(p, c):
        logits(2 * p + 1, z_odd)
        factors(2 * p, z_even)
        logits(lax.rem(2 * p + 2, n_blocks), z_even)
        factors(2 * p + 1, z_odd)
        return c

    lax.fori_loop(0, n_blocks // 2, pair, 0)

    for copy in copies:
        copy.wait()
    parts = [stat_ref[...]] + [slots[k] for k in range(n_tp - 1)]
    total = jnp.zeros_like(parts[0])
    for owner in range(n_tp):
        gap = lax.rem(tp - owner + n_tp, n_tp)
        part = parts[0]
        for k in range(1, n_tp):
            part = jnp.where(gap == k, parts[k], part)
        total = total + part
    total = jnp.where(total > 0.0, total, 1.0)
    mask = mask_ref[...]
    mask_sum = jnp.sum(mask) + jnp.sum(mask_slot[...])
    weight = mask / mask_sum
    stu_sum, tea_sum = total[:16, :], total[16:, :]
    base = jnp.sum(weight * (jnp.log(stu_sum) - jnp.log(tea_sum)))
    base_ref[...] = jnp.full((8, 128), base, F32)
    stu_row, tea_row = weight / stu_sum, weight / tea_sum
    row_ref[:16, :] = stu_row
    row_ref[16:, :] = tea_row
    for blk in range(tokens // 128):
        rows = slice(blk * 128, (blk + 1) * 128)
        stu_scale = jnp.broadcast_to(stu_row[blk:blk + 1, :], (128, 128)).T
        tea_scale = jnp.broadcast_to(tea_row[blk:blk + 1, :], (128, 128)).T
        stu_col[rows, :] = stu_scale
        tea_col[rows, :] = tea_scale
        kl_acc[rows, :] = kl_acc[rows, :] * tea_scale
        for lane in range(0, GRAD_TILE, 128):
            lanes = slice(lane, lane + 128)
            g_ref[rows, lanes] = (stu_q[rows, lanes] * stu_scale - tea_q[rows, lanes] * tea_scale).astype(BF16)
    de_ref[...] = jnp.dot(xt_ref[...], g_ref[...], preferred_element_type=F32)


def head(stat, mask, x, x_t, tab_t, tea, n_tp):
    tokens, dim = x.shape
    whole = pl.BlockSpec(memory_space=VMEM)
    hbm = pl.BlockSpec(memory_space=pl.ANY)
    return pl.pallas_call(
        functools.partial(head_kernel, n_tp),
        in_specs=[whole, whole, whole, whole, hbm, hbm],
        out_specs=[whole] * 7,
        out_shape=[
            jax.ShapeDtypeStruct((tokens, 128), F32),
            jax.ShapeDtypeStruct((tokens, 128), F32),
            jax.ShapeDtypeStruct((8, 128), F32),
            jax.ShapeDtypeStruct((32, 128), F32),
            jax.ShapeDtypeStruct((dim, GRAD_TILE), F32),
            jax.ShapeDtypeStruct((tokens, 128), F32),
            jax.ShapeDtypeStruct((tokens, GRAD_TILE), BF16),
        ],
        scratch_shapes=[
            VMEM((n_tp - 1,) + stat.shape, F32), VMEM(mask.shape, F32),
            VMEM((dim, GRAD_TILE), BF16), VMEM((tokens, GRAD_TILE), BF16),
            VMEM((tokens, GRAD_TILE), F32), VMEM((tokens, GRAD_TILE), F32),
            VMEM((GRAD_ROWS, GRAD_TILE), F32), VMEM((GRAD_ROWS, GRAD_TILE), F32),
            pltpu.SemaphoreType.DMA((2,)), pltpu.SemaphoreType.DMA((n_tp,)), pltpu.SemaphoreType.DMA((n_tp,)),
        ],
        compiler_params=pltpu.CompilerParams(collective_id=0, has_side_effects=True, vmem_limit_bytes=40 * 2**20),
        cost_estimate=pl.CostEstimate(flops=5_000_000_000, bytes_accessed=2_000_000, transcendentals=0),
        name="head",
    )(stat, mask, x, x_t, tab_t, tea)


def chunk_kernel(first, x_ref, xt_ref, stu_col, tea_col, tab_ref, tea_ref, _, *refs):
    if first:
        head_g, head_tab, de_ref, kl_acc, dx_acc, g_ref, z_even, z_odd = refs
    else:
        _, de_ref, kl_acc, dx_acc, g_ref, z_even, z_odd = refs
    tokens = x_ref.shape[0]
    n_blocks = tokens // GRAD_ROWS

    if first:
        @pl.when(pl.program_id(0) == 0)
        def _():
            def block(b, c):
                rows = pl.ds(pl.multiple_of(b * GRAD_ROWS, GRAD_ROWS), GRAD_ROWS)
                dx_acc[rows, :] = lax.dot_general(head_g[rows, :], head_tab[...], NT_DIMS, preferred_element_type=F32)
                return c

            lax.fori_loop(0, n_blocks, block, 0)

    def window(b, size=GRAD_ROWS, skip=0):
        return pl.ds(pl.multiple_of(b * GRAD_ROWS + skip, size), size)

    def logits(b, z_ref):
        z_ref[...] = jnp.dot(x_ref[window(b), :], tab_ref[...], preferred_element_type=F32)

    def grads(b, z_ref):
        for skip in range(0, GRAD_ROWS, SLICE):
            rows = window(b, SLICE, skip)
            stu_scale = stu_col[rows, :]
            tea_scale = tea_col[rows, :]
            kl = kl_acc[rows, :]
            parts = []
            for lane in range(0, GRAD_TILE, 128):
                stu = jnp.tanh(z_ref[skip:skip + SLICE, lane:lane + 128] * INV_CAP)
                tea = jnp.tanh(tea_ref[rows, lane:lane + 128].astype(F32) * INV_CAP)
                stu_p = jnp.exp2(stu * CAP_LOG2E) * stu_scale
                tea_p = jnp.exp2(tea * CAP_LOG2E) * tea_scale
                kl = kl + tea_p * (tea - stu)
                parts.append(((stu_p - tea_p) * (1.0 - stu * stu)).astype(BF16))
            kl_acc[rows, :] = kl
            g_ref[rows, :] = jnp.concatenate(parts, axis=1)

    def add_dx(b):
        dx_acc[window(b), :] += lax.dot_general(g_ref[window(b), :], tab_ref[...], NT_DIMS, preferred_element_type=F32)

    logits(0, z_even)
    logits(1, z_odd)
    grads(0, z_even)

    def pair(p, c):
        add_dx(2 * p)
        logits(2 * p + 2, z_even)
        grads(2 * p + 1, z_odd)
        add_dx(2 * p + 1)
        logits(2 * p + 3, z_odd)
        grads(2 * p + 2, z_even)
        return c

    lax.fori_loop(0, n_blocks // 2 - 1, pair, 0)
    add_dx(n_blocks - 2)
    grads(n_blocks - 1, z_odd)
    de_ref[...] = jnp.dot(xt_ref[...], g_ref[...], preferred_element_type=F32)
    add_dx(n_blocks - 1)


def chunk_grad(start, size, x, x_t, stu_col, tea_col, tab_t, tea, kl, dx, head_g):
    tokens, dim = x.shape
    off = start // GRAD_TILE
    whole = pl.BlockSpec(memory_space=VMEM)
    first = dx is None
    work = tokens * size
    return pl.pallas_call(
        functools.partial(chunk_kernel, first),
        grid=(size // GRAD_TILE,),
        in_specs=[
            whole, whole, whole, whole,
            pl.BlockSpec((dim, GRAD_TILE), lambda j: (0, j + off)),
            pl.BlockSpec((tokens, GRAD_TILE), lambda j: (0, j + off)),
            whole,
        ] + ([whole, pl.BlockSpec((dim, GRAD_TILE), lambda j: (0, 0))] if first else [whole]),
        out_specs=[pl.BlockSpec((dim, GRAD_TILE), lambda j: (0, j)), whole, whole],
        out_shape=[
            jax.ShapeDtypeStruct((dim, size), F32),
            jax.ShapeDtypeStruct((tokens, 128), F32),
            jax.ShapeDtypeStruct((tokens, dim), F32),
        ],
        scratch_shapes=[
            VMEM((tokens, GRAD_TILE), BF16), VMEM((GRAD_ROWS, GRAD_TILE), F32), VMEM((GRAD_ROWS, GRAD_TILE), F32),
        ],
        input_output_aliases={6: 1} if first else {6: 1, 7: 2},
        compiler_params=pltpu.CompilerParams(dimension_semantics=("arbitrary",), vmem_limit_bytes=32 * 2**20),
        cost_estimate=pl.CostEstimate(flops=work * 3 * 2 * dim, bytes_accessed=work * 2, transcendentals=0),
        name="chunk_grad",
    )(x, x_t, stu_col, tea_col, tab_t, tea, kl, *((head_g, tab_t) if first else (dx,)))


def dx_kernel(n_tp, dx_ref, kl_ref, base_ref, hid_ref, gain_ref, gh_ref, part_ref,
              slots, own, parts_buf, part_out, send_sem, recv_sem):
    tp = lax.axis_index("tp")
    dp = lax.axis_index("dp")
    dim, tokens = hid_ref.shape
    width = tokens // n_tp
    barrier = pltpu.get_barrier_semaphore()
    peers = [lax.rem(tp + k, n_tp) for k in range(1, n_tp)]
    for peer in peers:
        pl.semaphore_signal(barrier, inc=1, device_id=(dp, peer), device_id_type=MESH)
    pl.semaphore_wait(barrier, n_tp - 1)

    def window(index):
        return pl.ds(pl.multiple_of(index * width, width), width)

    reduce = []
    for k, peer in enumerate(peers):
        reduce.append(pltpu.make_async_remote_copy(
            src_ref=dx_ref.at[window(peer), :], dst_ref=slots.at[k],
            send_sem=send_sem.at[0, k], recv_sem=recv_sem.at[0, k], device_id=(dp, peer), device_id_type=MESH))
        reduce[-1].start()
    for copy in reduce:
        copy.wait()
    mine = window(tp)
    total = jnp.zeros((width, dim), F32)
    for owner in range(n_tp):
        gap = lax.rem(tp - owner + n_tp, n_tp)
        part = dx_ref[mine, :]
        for k in range(1, n_tp):
            part = jnp.where(gap == k, slots[k - 1], part)
        total = total + part
    grad_x = total.T
    gain = jnp.broadcast_to(1.0 + gain_ref[...], (128, gain_ref.shape[1])).T[:dim, :1]
    hid = hid_ref[:, mine].astype(F32)
    inv_rms = lax.rsqrt(jnp.sum(hid * hid, axis=0, keepdims=True) * (1.0 / dim) + NORM_EPS)
    normed = hid * inv_rms
    grad_n = grad_x * gain
    corr = jnp.sum(grad_n * normed, axis=0, keepdims=True) * (1.0 / dim)
    own[...] = inv_rms * (grad_n - normed * corr)

    prod = grad_x * normed
    col = prod[:, :128]
    for lane in range(128, width, 128):
        col = col + prod[:, lane:lane + 128]
    row = jnp.sum(col.T, axis=0, keepdims=True)
    part_out[0:1, :dim] = row
    part_out[0:1, dim:] = jnp.zeros((1, part_out.shape[1] - dim), F32)
    loss = SOFT_CAP * jnp.sum(kl_ref[...]) + jnp.sum(base_ref[0:1, 0:1]) * (1.0 / n_tp)
    part_out[1:2, :] = jnp.full((1, part_out.shape[1]), loss, F32)
    part_out[2:8, :] = jnp.zeros((6, part_out.shape[1]), F32)

    spread = []
    for k, peer in enumerate(peers):
        spread.append(pltpu.make_async_remote_copy(
            src_ref=own, dst_ref=gh_ref.at[:, mine],
            send_sem=send_sem.at[1, k], recv_sem=recv_sem.at[1, k], device_id=(dp, peer), device_id_type=MESH))
        spread.append(pltpu.make_async_remote_copy(
            src_ref=part_out, dst_ref=parts_buf.at[tp],
            send_sem=send_sem.at[2, k], recv_sem=recv_sem.at[2, k], device_id=(dp, peer), device_id_type=MESH))
    for copy in spread:
        copy.start()
    gh_ref[:, mine] = own[...]
    parts_buf[tp] = part_out[...]
    for copy in spread:
        copy.wait()
    share = parts_buf[0]
    for k in range(1, n_tp):
        share = share + parts_buf[k]
    part_ref[...] = share


def reduce_dx(dx, kl, base, hid_t, gain, n_tp):
    tokens, dim = dx.shape
    width = tokens // n_tp
    whole = pl.BlockSpec(memory_space=VMEM)
    return pl.pallas_call(
        functools.partial(dx_kernel, n_tp),
        in_specs=[whole, whole, whole, whole, whole],
        out_specs=[whole, whole],
        out_shape=[
            jax.ShapeDtypeStruct((dim, tokens), F32),
            jax.ShapeDtypeStruct((8, 640), F32),
        ],
        scratch_shapes=[
            VMEM((n_tp - 1, width, dim), F32), VMEM((dim, width), F32),
            VMEM((n_tp, 8, 640), F32), VMEM((8, 640), F32),
            pltpu.SemaphoreType.DMA((3, n_tp - 1)), pltpu.SemaphoreType.DMA((3, n_tp - 1)),
        ],
        compiler_params=pltpu.CompilerParams(collective_id=1, has_side_effects=True, vmem_limit_bytes=24 * 2**20),
        cost_estimate=pl.CostEstimate(flops=50_000_000_000, bytes_accessed=20_000_000, transcendentals=0),
        name="reduce_dx",
    )(dx, kl, base, hid_t, gain)


def add_kernel(*refs):
    a_ref, b_ref, out_ref = refs[-3], refs[-2], refs[-1]
    out_ref[...] = a_ref[...] + b_ref[...]


def add_chunk(start, size, vocab, own, other, out, after):
    dim = own.shape[0]
    tile = math.gcd(math.gcd(start, size), 512)
    off = start // tile
    hbm = pl.BlockSpec(memory_space=pl.ANY)
    block = pl.BlockSpec((dim, tile), lambda j: (0, j))
    lead = (after,) if out is None else (out,)
    return pl.pallas_call(
        add_kernel,
        grid=(size // tile,),
        in_specs=[hbm, block, block],
        out_specs=pl.BlockSpec((dim, tile), lambda j: (0, j + off)),
        out_shape=jax.ShapeDtypeStruct((dim, vocab), F32),
        input_output_aliases={} if out is None else {0: 0},
        compiler_params=pltpu.CompilerParams(dimension_semantics=("arbitrary",), vmem_limit_bytes=16 * 2**20),
        cost_estimate=pl.CostEstimate(flops=dim * size, bytes_accessed=12 * dim * size, transcendentals=0),
        name="add_chunk",
    )(*lead, own, other)


CHUNKS = (GRAD_TILE, 512, 1536, 3584, 3584, 2048, 256, 256)


def solution(mesh):
    n_tp = mesh.shape["tp"]
    swap = [(0, 1), (1, 0)]

    def step(hid_rows, w_final, tab_rows, tea_rows, mask_rows):
        tokens, dim = hid_rows.shape
        vocab = tab_rows.shape[0]
        hid_t = hid_rows.T
        tab_t = tab_rows.T
        mask = mask_rows.reshape(tokens // 128, 128)
        gain = w_final.reshape(1, dim)
        hid_v, hid_own, tea_own = lift(hid_t, tea_rows, n_tp)
        hid_part = lax.ppermute(hid_own, "dp", swap)
        tea_other = lax.ppermute(tea_own, "dp", swap)
        x, x_t, stat = stats(hid_v, gain, mask, tab_t, tea_rows)
        stu_col, tea_col, base, scale_rows, part, kl, head_g = head(stat, mask, x, x_t, tab_t, tea_rows, n_tp)
        dx = None
        own, other = [], []
        start = 0
        for c, size in enumerate(CHUNKS):
            if c:
                part, kl, dx = chunk_grad(start, size, x, x_t, stu_col, tea_col, tab_t, tea_rows, kl, dx, head_g)
            other.append(lax.ppermute(part, "dp", swap))
            own.append(part)
            start += size
        _, kl, dx = chunk_grad(start, SHARED, x, x_t, stu_col, tea_col, tab_t, tea_rows, kl, dx, head_g)
        rows_other = lax.ppermute(scale_rows, "dp", swap)
        parts = [hid_part]
        for k in range(1, n_tp):
            parts.append(lax.ppermute(hid_part, "tp", [(i, (i + k) % n_tp) for i in range(n_tp)]))
        gh_t, share = reduce_dx(dx, kl, base, hid_t, gain, n_tp)
        share_other = lax.ppermute(share, "dp", swap)
        share = share + share_other
        hid_other = join(parts, n_tp)
        term_own = shared_grad(hid_t, gain, scale_rows, tab_t, tea_own)
        term_other = shared_grad(hid_other, gain, rows_other, tab_t, tea_other)
        out = add_chunk(start, SHARED, vocab, term_own, term_other, None, gh_t)
        start = 0
        for size, a, b in zip(CHUNKS, own, other):
            out = add_chunk(start, size, vocab, a, b, out, gh_t)
            start += size
        return share[1, 0], gh_t.T.astype(BF16), share[0, :dim], out.T

    return jax.shard_map(
        step, mesh=mesh,
        in_specs=(P("dp", None), P(None), P("tp", None), P("dp", "tp"), P("dp")),
        out_specs=(P(), P("dp", None), P(None), P("tp", None)), check_vma=False)
```

```python
import functools
import math

import jax
import jax.numpy as jnp
from jax import lax
from jax.experimental import pallas as pl
from jax.experimental.pallas import tpu as pltpu
from jax.sharding import PartitionSpec as P

SOFT_CAP = 30.0
NORM_EPS = 1e-6
INV_CAP = 1.0 / SOFT_CAP
CAP_LOG2E = SOFT_CAP * math.log2(math.e)
MESH = pl.DeviceIdType.MESH
F32 = jnp.float32
BF16 = jnp.bfloat16
GROUP = 16
VMEM = pltpu.VMEM
NT_DIMS = (((1,), (1,)), ((), ()))


SHARED = 256


def lift_hidden_kernel(hid_hbm, hid_ref, out_ref, run_ref, sem):
    tp = lax.axis_index("tp")
    width = out_ref.shape[1]
    run = pltpu.make_async_copy(hid_hbm.at[:, pl.ds(pl.multiple_of(tp * width, width), width)], run_ref, sem.at[0])
    run.start()
    load = pltpu.make_async_copy(hid_hbm, hid_ref, sem.at[1])
    load.start()
    run.wait()
    out_ref[...] = run_ref[...].astype(F32)
    load.wait()


def lift_hidden(hid_t, n_tp):
    dim, tokens = hid_t.shape
    whole = pl.BlockSpec(memory_space=VMEM)
    return pl.pallas_call(
        lift_hidden_kernel,
        in_specs=[pl.BlockSpec(memory_space=pl.ANY)],
        out_specs=[whole, whole],
        out_shape=[jax.ShapeDtypeStruct((dim, tokens), BF16), jax.ShapeDtypeStruct((dim, tokens // n_tp), F32)],
        scratch_shapes=[VMEM((dim, tokens // n_tp), BF16), pltpu.SemaphoreType.DMA((2,))],
        compiler_params=pltpu.CompilerParams(vmem_limit_bytes=99 * 2**19),
        cost_estimate=pl.CostEstimate(flops=3_000_000, bytes_accessed=5_000_000, transcendentals=0),
        name="lift_hidden",
    )(hid_t)


def lift_teacher_kernel(tea_ref, out_ref):
    out_ref[...] = tea_ref[...].astype(F32)


def lift_teacher(tea):
    tokens, vocab = tea.shape
    rows, last = tokens // 4, vocab // SHARED - 1
    return pl.pallas_call(
        lift_teacher_kernel,
        grid=(4,),
        in_specs=[pl.BlockSpec((rows, SHARED), lambda j: (j, last))],
        out_specs=pl.BlockSpec((rows, SHARED), lambda j: (j, 0)),
        out_shape=jax.ShapeDtypeStruct((tokens, SHARED), F32),
        compiler_params=pltpu.CompilerParams(dimension_semantics=("arbitrary",), vmem_limit_bytes=48 * 2**20),
        cost_estimate=pl.CostEstimate(flops=3_000_000, bytes_accessed=5_000_000, transcendentals=0),
        name="lift_teacher",
    )(tea)


def join_kernel(n_tp, *refs):
    out_ref = refs[-1]
    tp = lax.axis_index("tp")
    width = refs[0].shape[1]
    for k, ref in enumerate(refs[:-1]):
        owner = lax.rem(tp - k + n_tp, n_tp)
        out_ref[:, pl.ds(pl.multiple_of(owner * width, width), width)] = ref[...].astype(BF16)


def join(parts, n_tp):
    dim, width = parts[0].shape
    whole = pl.BlockSpec(memory_space=VMEM)
    return pl.pallas_call(
        functools.partial(join_kernel, n_tp),
        in_specs=[whole] * n_tp,
        out_specs=whole,
        out_shape=jax.ShapeDtypeStruct((dim, width * n_tp), BF16),
        compiler_params=pltpu.CompilerParams(vmem_limit_bytes=16 * 2**20),
        cost_estimate=pl.CostEstimate(flops=3_000_000, bytes_accessed=5_000_000, transcendentals=0),
        name="join",
    )(*parts)


def make_x(hid_ref, gain_ref, x_ref, xt_ref):
    dim, tokens = hid_ref.shape
    gain = jnp.broadcast_to(1.0 + gain_ref[...], (128, gain_ref.shape[1])).T[:dim, :]
    for blk in range(tokens // 128):
        hid = hid_ref[:, blk * 128:(blk + 1) * 128].astype(F32)
        inv_rms = lax.rsqrt(jnp.sum(hid * hid, axis=0, keepdims=True) * (1.0 / dim) + NORM_EPS)
        x_t = (hid * inv_rms * gain).astype(BF16)
        xt_ref[:, blk * 128:(blk + 1) * 128] = x_t
        x_ref[blk * 128:(blk + 1) * 128, :] = x_t.T


def shared_kernel(hid_ref, gain_ref, row_ref, tab_ref, tea_ref, de_ref, x_ref, xt_ref, g_ref):
    tokens = x_ref.shape[0]
    make_x(hid_ref, gain_ref, x_ref, xt_ref)
    for blk in range(tokens // 128):
        rows = slice(blk * 128, (blk + 1) * 128)
        stu_scale = jnp.broadcast_to(row_ref[blk:blk + 1, :], (128, 128)).T
        tea_scale = jnp.broadcast_to(row_ref[16 + blk:17 + blk, :], (128, 128)).T
        z = jnp.dot(x_ref[rows, :], tab_ref[...], preferred_element_type=F32)
        for lane in range(0, SHARED, 128):
            lanes = slice(lane, lane + 128)
            stu = jnp.tanh(z[:, lanes] * INV_CAP)
            tea = jnp.tanh(tea_ref[rows, lanes] * INV_CAP)
            stu_p = jnp.exp2(stu * CAP_LOG2E) * stu_scale
            tea_p = jnp.exp2(tea * CAP_LOG2E) * tea_scale
            g_ref[rows, lanes] = ((stu_p - tea_p) * (1.0 - stu * stu)).astype(BF16)
    de_ref[...] = jnp.dot(xt_ref[...], g_ref[...], preferred_element_type=F32)


def shared_grad(hid_t, gain, scale_rows, tab_t, tea):
    dim, tokens = hid_t.shape
    last = tab_t.shape[1] // SHARED - 1

    def spec(shape):
        return pl.BlockSpec(shape, lambda j: (0, 0))

    return pl.pallas_call(
        shared_kernel,
        grid=(1,),
        in_specs=[
            spec(hid_t.shape), spec(gain.shape), spec(scale_rows.shape),
            pl.BlockSpec((dim, SHARED), lambda j: (0, last)), spec(tea.shape),
        ],
        out_specs=spec((dim, SHARED)),
        out_shape=jax.ShapeDtypeStruct((dim, SHARED), F32),
        scratch_shapes=[VMEM((tokens, dim), BF16), VMEM((dim, tokens), BF16), VMEM((tokens, SHARED), BF16)],
        compiler_params=pltpu.CompilerParams(dimension_semantics=("arbitrary",), vmem_limit_bytes=40 * 2**20),
        cost_estimate=pl.CostEstimate(flops=tokens * SHARED * 4 * dim, bytes_accessed=tokens * SHARED * 4, transcendentals=0),
        name="shared_grad",
    )(hid_t, gain, scale_rows, tab_t, tea)


STAT_TILE = 1024
STAT_ROWS = 128
PER_BLOCK = STAT_ROWS // GROUP


def stats_kernel(hid_ref, gain_ref, mask_ref, tab_ref, next_ref, tea_ref, x_ref, xt_ref, stat_ref,
                 stu_acc, tea_acc, z_even, z_odd, count_vmem, count_smem, groups, live, sem):
    step = pl.program_id(0)
    _, tokens = hid_ref.shape
    n_groups = tokens // GROUP

    def source(i):
        return pl.ds(pl.multiple_of(jnp.minimum(groups[i], n_groups - 1) * GROUP, GROUP), GROUP)

    def dest(i):
        return pl.ds(pl.multiple_of(groups[i] * GROUP, GROUP), GROUP)

    def logits(block, table, z_ref):
        rows = jnp.concatenate([x_ref[source(block * PER_BLOCK + i), :] for i in range(PER_BLOCK)], axis=0)
        z_ref[...] = jnp.dot(rows, table[...], preferred_element_type=F32)

    def exp_sum(val):
        val = jnp.exp2(jnp.tanh(val * INV_CAP) * CAP_LOG2E)
        total = val[:, :128]
        for lane in range(128, STAT_TILE, 128):
            total = total + val[:, lane:lane + 128]
        return total

    def accumulate(block, z_ref):
        for i in range(PER_BLOCK):
            at = block * PER_BLOCK + i
            tea_acc[dest(at), :] += exp_sum(tea_ref[source(at), :].astype(F32))
            stu_acc[dest(at), :] += exp_sum(z_ref[i * GROUP:(i + 1) * GROUP, :])

    @pl.when(step == 0)
    def _():
        stu_acc[...] = jnp.zeros_like(stu_acc)
        tea_acc[...] = jnp.zeros_like(tea_acc)
        rows = lax.broadcasted_iota(jnp.int32, (128, 128), 0) // GROUP
        cols = lax.broadcasted_iota(jnp.int32, (128, 128), 1)
        pick = jnp.where(rows == cols, 1.0, 0.0).astype(BF16)
        counts = jnp.dot(mask_ref[...].astype(BF16), pick, preferred_element_type=F32)
        count_vmem[...] = counts.astype(jnp.int32)
        copy = pltpu.make_async_copy(count_vmem, count_smem, sem)
        copy.start()
        make_x(hid_ref, gain_ref, x_ref, xt_ref)
        copy.wait()

        def add_group(g, n):
            groups[n] = g
            keep = count_smem[g // 8, g % 8] > 0
            return n + jnp.where(keep, 1, 0)

        n_live = lax.fori_loop(0, n_groups, add_group, 0)

        def pad(i, c):
            groups[n_live + i] = n_groups
            return c

        lax.fori_loop(0, 2 * PER_BLOCK, pad, 0)
        live[0] = n_live
        logits(0, tab_ref, z_even)

    n_blocks = jnp.maximum((live[0] + PER_BLOCK - 1) // PER_BLOCK, 1)
    more = (n_blocks - 1) // 2

    def pair(p, c):
        logits(2 * p + 1, tab_ref, z_odd)
        accumulate(2 * p, z_even)
        logits(2 * p + 2, tab_ref, z_even)
        accumulate(2 * p + 1, z_odd)
        return c

    lax.fori_loop(0, more, pair, 0)

    @pl.when(n_blocks % 2 == 0)
    def _():
        logits(2 * more + 1, tab_ref, z_odd)
        accumulate(2 * more, z_even)
        logits(0, next_ref, z_even)
        accumulate(2 * more + 1, z_odd)

    @pl.when(n_blocks % 2 == 1)
    def _():
        logits(0, next_ref, z_odd)
        accumulate(2 * more, z_even)
        z_even[...] = z_odd[...]

    @pl.when(step == pl.num_programs(0) - 1)
    def _():
        for blk in range(tokens // 128):
            for k, acc in enumerate((stu_acc, tea_acc)):
                part = acc[blk * 128:(blk + 1) * 128, :].T
                stat_ref[k * 16 + blk:k * 16 + blk + 1, :] = jnp.sum(part, axis=0, keepdims=True)


def stats(hid_t, gain, mask, tab_t, tea):
    dim, tokens = hid_t.shape
    vocab = tab_t.shape[1]
    n_groups = tokens // GROUP
    whole = pl.BlockSpec(memory_space=VMEM)
    return pl.pallas_call(
        stats_kernel,
        grid=(vocab // STAT_TILE,),
        in_specs=[
            whole, whole, whole,
            pl.BlockSpec((dim, STAT_TILE), lambda j: (0, j)),
            pl.BlockSpec((dim, STAT_TILE), lambda j: (0, jnp.minimum(j + 1, vocab // STAT_TILE - 1))),
            pl.BlockSpec((tokens, STAT_TILE), lambda j: (0, j)),
        ],
        out_specs=[whole, whole, whole],
        out_shape=[
            jax.ShapeDtypeStruct((tokens, dim), BF16),
            jax.ShapeDtypeStruct((dim, tokens), BF16),
            jax.ShapeDtypeStruct((32, 128), F32),
        ],
        scratch_shapes=[
            VMEM((tokens + GROUP, 128), F32), VMEM((tokens + GROUP, 128), F32),
            VMEM((STAT_ROWS, STAT_TILE), F32), VMEM((STAT_ROWS, STAT_TILE), F32),
            VMEM((16, 128), jnp.int32), pltpu.SMEM((16, 128), jnp.int32),
            pltpu.SMEM((n_groups + 4 * PER_BLOCK,), jnp.int32), pltpu.SMEM((1,), jnp.int32),
            pltpu.SemaphoreType.DMA,
        ],
        compiler_params=pltpu.CompilerParams(dimension_semantics=("arbitrary",), vmem_limit_bytes=46 * 2**20),
        cost_estimate=pl.CostEstimate(flops=50_000_000_000, bytes_accessed=70_000_000, transcendentals=0),
        name="stats",
    )(hid_t, gain, mask, tab_t, tab_t, tea)


GRAD_TILE = 256
GRAD_ROWS = 256
SLICE = 16


def head_kernel(n_tp, stat_ref, mask_ref, mask_other, x_ref, xt_ref, tab_hbm, tea_hbm, stu_col, tea_col, base_ref, row_ref, de_ref, kl_acc, g_ref,
                slots, tab_ref, tea_ref, stu_q, tea_q, z_even, z_odd, load_sem, send_sem, recv_sem):
    tp = lax.axis_index("tp")
    dp = lax.axis_index("dp")
    tokens = x_ref.shape[0]
    n_blocks = tokens // GRAD_ROWS
    load_tab = pltpu.make_async_copy(tab_hbm.at[:, 0:GRAD_TILE], tab_ref, load_sem.at[0])
    load_tea = pltpu.make_async_copy(tea_hbm.at[:, 0:GRAD_TILE], tea_ref, load_sem.at[1])
    load_tab.start()
    load_tea.start()
    barrier = pltpu.get_barrier_semaphore()
    peers = [(dp, lax.rem(tp + k, n_tp)) for k in range(1, n_tp)]
    for peer in peers:
        pl.semaphore_signal(barrier, inc=1, device_id=peer, device_id_type=MESH)
    pl.semaphore_wait(barrier, len(peers))
    copies = []
    for k, peer in enumerate(peers):
        copies.append(pltpu.make_async_remote_copy(
            src_ref=stat_ref, dst_ref=slots.at[k],
            send_sem=send_sem.at[k], recv_sem=recv_sem.at[k], device_id=peer, device_id_type=MESH))
        copies[-1].start()
    load_tab.wait()
    load_tea.wait()

    def window(b, size=GRAD_ROWS, skip=0):
        return pl.ds(pl.multiple_of(b * GRAD_ROWS + skip, size), size)

    def logits(b, z_ref):
        z_ref[...] = jnp.dot(x_ref[window(b), :], tab_ref[...], preferred_element_type=F32)

    def factors(b, z_ref):
        for skip in range(0, GRAD_ROWS, SLICE):
            rows = window(b, SLICE, skip)
            kl = 0.0
            for lane in range(0, GRAD_TILE, 128):
                stu = jnp.tanh(z_ref[skip:skip + SLICE, lane:lane + 128] * INV_CAP)
                tea = jnp.tanh(tea_ref[rows, lane:lane + 128].astype(F32) * INV_CAP)
                tea_e = jnp.exp2(tea * CAP_LOG2E)
                slope = 1.0 - stu * stu
                kl = kl + tea_e * (tea - stu)
                stu_q[rows, lane:lane + 128] = jnp.exp2(stu * CAP_LOG2E) * slope
                tea_q[rows, lane:lane + 128] = tea_e * slope
            kl_acc[rows, :] = kl

    logits(0, z_even)

    def pair(p, c):
        logits(2 * p + 1, z_odd)
        factors(2 * p, z_even)
        logits(lax.rem(2 * p + 2, n_blocks), z_even)
        factors(2 * p + 1, z_odd)
        return c

    lax.fori_loop(0, n_blocks // 2, pair, 0)

    for copy in copies:
        copy.wait()
    parts = [stat_ref[...]] + [slots[k] for k in range(n_tp - 1)]
    total = jnp.zeros_like(parts[0])
    for owner in range(n_tp):
        gap = lax.rem(tp - owner + n_tp, n_tp)
        part = parts[0]
        for k in range(1, n_tp):
            part = jnp.where(gap == k, parts[k], part)
        total = total + part
    total = jnp.where(total > 0.0, total, 1.0)
    mask = mask_ref[...]
    mask_sum = jnp.sum(mask) + jnp.sum(mask_other[...])
    weight = mask / mask_sum
    stu_sum, tea_sum = total[:16, :], total[16:, :]
    base = jnp.sum(weight * (jnp.log(stu_sum) - jnp.log(tea_sum)))
    base_ref[...] = jnp.full((8, 128), base, F32)
    stu_row, tea_row = weight / stu_sum, weight / tea_sum
    row_ref[:16, :] = stu_row
    row_ref[16:, :] = tea_row
    for blk in range(tokens // 128):
        rows = slice(blk * 128, (blk + 1) * 128)
        stu_scale = jnp.broadcast_to(stu_row[blk:blk + 1, :], (128, 128)).T
        tea_scale = jnp.broadcast_to(tea_row[blk:blk + 1, :], (128, 128)).T
        stu_col[rows, :] = stu_scale
        tea_col[rows, :] = tea_scale
        kl_acc[rows, :] = kl_acc[rows, :] * tea_scale
        for lane in range(0, GRAD_TILE, 128):
            lanes = slice(lane, lane + 128)
            g_ref[rows, lanes] = (stu_q[rows, lanes] * stu_scale - tea_q[rows, lanes] * tea_scale).astype(BF16)
    de_ref[...] = jnp.dot(xt_ref[...], g_ref[...], preferred_element_type=F32)


def head(stat, mask, mask_other, x, x_t, tab_t, tea, n_tp):
    tokens, dim = x.shape
    whole = pl.BlockSpec(memory_space=VMEM)
    hbm = pl.BlockSpec(memory_space=pl.ANY)
    return pl.pallas_call(
        functools.partial(head_kernel, n_tp),
        in_specs=[whole, whole, whole, whole, whole, hbm, hbm],
        out_specs=[whole] * 7,
        out_shape=[
            jax.ShapeDtypeStruct((tokens, 128), F32),
            jax.ShapeDtypeStruct((tokens, 128), F32),
            jax.ShapeDtypeStruct((8, 128), F32),
            jax.ShapeDtypeStruct((32, 128), F32),
            jax.ShapeDtypeStruct((dim, GRAD_TILE), F32),
            jax.ShapeDtypeStruct((tokens, 128), F32),
            jax.ShapeDtypeStruct((tokens, GRAD_TILE), BF16),
        ],
        scratch_shapes=[
            VMEM((n_tp - 1,) + stat.shape, F32),
            VMEM((dim, GRAD_TILE), BF16), VMEM((tokens, GRAD_TILE), BF16),
            VMEM((tokens, GRAD_TILE), F32), VMEM((tokens, GRAD_TILE), F32),
            VMEM((GRAD_ROWS, GRAD_TILE), F32), VMEM((GRAD_ROWS, GRAD_TILE), F32),
            pltpu.SemaphoreType.DMA((2,)), pltpu.SemaphoreType.DMA((n_tp - 1,)), pltpu.SemaphoreType.DMA((n_tp - 1,)),
        ],
        compiler_params=pltpu.CompilerParams(collective_id=0, has_side_effects=True, vmem_limit_bytes=40 * 2**20),
        cost_estimate=pl.CostEstimate(flops=5_000_000_000, bytes_accessed=2_000_000, transcendentals=0),
        name="head",
    )(stat, mask, mask_other, x, x_t, tab_t, tea)


def chunk_kernel(first, x_ref, xt_ref, stu_col, tea_col, tab_ref, tea_ref, _, *refs):
    if first:
        head_g, head_tab, de_ref, kl_acc, dx_acc, g_ref, z_even, z_odd = refs
    else:
        _, de_ref, kl_acc, dx_acc, g_ref, z_even, z_odd = refs
    tokens = x_ref.shape[0]
    n_blocks = tokens // GRAD_ROWS

    if first:
        @pl.when(pl.program_id(0) == 0)
        def _():
            def block(b, c):
                rows = pl.ds(pl.multiple_of(b * GRAD_ROWS, GRAD_ROWS), GRAD_ROWS)
                dx_acc[rows, :] = lax.dot_general(head_g[rows, :], head_tab[...], NT_DIMS, preferred_element_type=F32)
                return c

            lax.fori_loop(0, n_blocks, block, 0)

    def window(b, size=GRAD_ROWS, skip=0):
        return pl.ds(pl.multiple_of(b * GRAD_ROWS + skip, size), size)

    def logits(b, z_ref):
        z_ref[...] = jnp.dot(x_ref[window(b), :], tab_ref[...], preferred_element_type=F32)

    def grads(b, z_ref):
        for skip in range(0, GRAD_ROWS, SLICE):
            rows = window(b, SLICE, skip)
            stu_scale = stu_col[rows, :]
            tea_scale = tea_col[rows, :]
            kl = kl_acc[rows, :]
            parts = []
            for lane in range(0, GRAD_TILE, 128):
                stu = jnp.tanh(z_ref[skip:skip + SLICE, lane:lane + 128] * INV_CAP)
                tea = jnp.tanh(tea_ref[rows, lane:lane + 128].astype(F32) * INV_CAP)
                stu_p = jnp.exp2(stu * CAP_LOG2E) * stu_scale
                tea_p = jnp.exp2(tea * CAP_LOG2E) * tea_scale
                kl = kl + tea_p * (tea - stu)
                parts.append(((stu_p - tea_p) * (1.0 - stu * stu)).astype(BF16))
            kl_acc[rows, :] = kl
            g_ref[rows, :] = jnp.concatenate(parts, axis=1)

    def add_dx(b):
        dx_acc[window(b), :] += lax.dot_general(g_ref[window(b), :], tab_ref[...], NT_DIMS, preferred_element_type=F32)

    logits(0, z_even)
    logits(1, z_odd)
    grads(0, z_even)

    def pair(p, c):
        add_dx(2 * p)
        logits(2 * p + 2, z_even)
        grads(2 * p + 1, z_odd)
        add_dx(2 * p + 1)
        logits(2 * p + 3, z_odd)
        grads(2 * p + 2, z_even)
        return c

    lax.fori_loop(0, n_blocks // 2 - 1, pair, 0)
    add_dx(n_blocks - 2)
    grads(n_blocks - 1, z_odd)
    de_ref[...] = jnp.dot(xt_ref[...], g_ref[...], preferred_element_type=F32)
    add_dx(n_blocks - 1)


def chunk_grad(start, size, x, x_t, stu_col, tea_col, tab_t, tea, kl, dx, head_g):
    tokens, dim = x.shape
    off = start // GRAD_TILE
    whole = pl.BlockSpec(memory_space=VMEM)
    first = dx is None
    work = tokens * size
    return pl.pallas_call(
        functools.partial(chunk_kernel, first),
        grid=(size // GRAD_TILE,),
        in_specs=[
            whole, whole, whole, whole,
            pl.BlockSpec((dim, GRAD_TILE), lambda j: (0, j + off)),
            pl.BlockSpec((tokens, GRAD_TILE), lambda j: (0, j + off)),
            whole,
        ] + ([whole, pl.BlockSpec((dim, GRAD_TILE), lambda j: (0, 0))] if first else [whole]),
        out_specs=[pl.BlockSpec((dim, GRAD_TILE), lambda j: (0, j)), whole, whole],
        out_shape=[
            jax.ShapeDtypeStruct((dim, size), F32),
            jax.ShapeDtypeStruct((tokens, 128), F32),
            jax.ShapeDtypeStruct((tokens, dim), F32),
        ],
        scratch_shapes=[
            VMEM((tokens, GRAD_TILE), BF16), VMEM((GRAD_ROWS, GRAD_TILE), F32), VMEM((GRAD_ROWS, GRAD_TILE), F32),
        ],
        input_output_aliases={6: 1} if first else {6: 1, 7: 2},
        compiler_params=pltpu.CompilerParams(dimension_semantics=("arbitrary",), vmem_limit_bytes=32 * 2**20),
        cost_estimate=pl.CostEstimate(flops=work * 3 * 2 * dim, bytes_accessed=work * 2, transcendentals=0),
        name="chunk_grad",
    )(x, x_t, stu_col, tea_col, tab_t, tea, kl, *((head_g, tab_t) if first else (dx,)))


def dx_kernel(n_tp, dx_ref, kl_ref, base_ref, hid_ref, gain_ref, gh_ref, part_ref,
              slots, own, parts_buf, part_out, send_sem, recv_sem):
    tp = lax.axis_index("tp")
    dp = lax.axis_index("dp")
    dim, tokens = hid_ref.shape
    width = tokens // n_tp
    barrier = pltpu.get_barrier_semaphore()
    peers = [lax.rem(tp + k, n_tp) for k in range(1, n_tp)]
    for peer in peers:
        pl.semaphore_signal(barrier, inc=1, device_id=(dp, peer), device_id_type=MESH)
    pl.semaphore_wait(barrier, n_tp - 1)

    def window(index):
        return pl.ds(pl.multiple_of(index * width, width), width)

    reduce = []
    for k, peer in enumerate(peers):
        reduce.append(pltpu.make_async_remote_copy(
            src_ref=dx_ref.at[window(peer), :], dst_ref=slots.at[k],
            send_sem=send_sem.at[0, k], recv_sem=recv_sem.at[0, k], device_id=(dp, peer), device_id_type=MESH))
        reduce[-1].start()
    for copy in reduce:
        copy.wait()
    mine = window(tp)
    total = jnp.zeros((width, dim), F32)
    for owner in range(n_tp):
        gap = lax.rem(tp - owner + n_tp, n_tp)
        part = dx_ref[mine, :]
        for k in range(1, n_tp):
            part = jnp.where(gap == k, slots[k - 1], part)
        total = total + part
    grad_x = total.T
    gain = jnp.broadcast_to(1.0 + gain_ref[...], (128, gain_ref.shape[1])).T[:dim, :1]
    hid = hid_ref[:, mine].astype(F32)
    inv_rms = lax.rsqrt(jnp.sum(hid * hid, axis=0, keepdims=True) * (1.0 / dim) + NORM_EPS)
    normed = hid * inv_rms
    grad_n = grad_x * gain
    corr = jnp.sum(grad_n * normed, axis=0, keepdims=True) * (1.0 / dim)
    own[...] = inv_rms * (grad_n - normed * corr)

    prod = grad_x * normed
    col = prod[:, :128]
    for lane in range(128, width, 128):
        col = col + prod[:, lane:lane + 128]
    row = jnp.sum(col.T, axis=0, keepdims=True)
    part_out[0:1, :dim] = row
    part_out[0:1, dim:] = jnp.zeros((1, part_out.shape[1] - dim), F32)
    loss = SOFT_CAP * jnp.sum(kl_ref[...]) + jnp.sum(base_ref[0:1, 0:1]) * (1.0 / n_tp)
    part_out[1:2, :] = jnp.full((1, part_out.shape[1]), loss, F32)
    part_out[2:8, :] = jnp.zeros((6, part_out.shape[1]), F32)

    spread = []
    for k, peer in enumerate(peers):
        spread.append(pltpu.make_async_remote_copy(
            src_ref=own, dst_ref=gh_ref.at[:, mine],
            send_sem=send_sem.at[1, k], recv_sem=recv_sem.at[1, k], device_id=(dp, peer), device_id_type=MESH))
        spread.append(pltpu.make_async_remote_copy(
            src_ref=part_out, dst_ref=parts_buf.at[tp],
            send_sem=send_sem.at[2, k], recv_sem=recv_sem.at[2, k], device_id=(dp, peer), device_id_type=MESH))
    for copy in spread:
        copy.start()
    gh_ref[:, mine] = own[...]
    parts_buf[tp] = part_out[...]
    for copy in spread:
        copy.wait()
    share = parts_buf[0]
    for k in range(1, n_tp):
        share = share + parts_buf[k]
    part_ref[...] = share


def reduce_dx(dx, kl, base, hid_t, gain, n_tp):
    tokens, dim = dx.shape
    width = tokens // n_tp
    whole = pl.BlockSpec(memory_space=VMEM)
    return pl.pallas_call(
        functools.partial(dx_kernel, n_tp),
        in_specs=[whole, whole, whole, whole, whole],
        out_specs=[whole, whole],
        out_shape=[
            jax.ShapeDtypeStruct((dim, tokens), F32),
            jax.ShapeDtypeStruct((8, 640), F32),
        ],
        scratch_shapes=[
            VMEM((n_tp - 1, width, dim), F32), VMEM((dim, width), F32),
            VMEM((n_tp, 8, 640), F32), VMEM((8, 640), F32),
            pltpu.SemaphoreType.DMA((3, n_tp - 1)), pltpu.SemaphoreType.DMA((3, n_tp - 1)),
        ],
        compiler_params=pltpu.CompilerParams(collective_id=1, has_side_effects=True, vmem_limit_bytes=24 * 2**20),
        cost_estimate=pl.CostEstimate(flops=50_000_000_000, bytes_accessed=20_000_000, transcendentals=0),
        name="reduce_dx",
    )(dx, kl, base, hid_t, gain)


def add_kernel(*refs):
    a_ref, b_ref, out_ref = refs[-3], refs[-2], refs[-1]
    out_ref[...] = a_ref[...] + b_ref[...]


def add_chunk(start, size, vocab, own, other, out, after):
    dim = own.shape[0]
    tile = math.gcd(math.gcd(start, size), 512)
    off = start // tile
    hbm = pl.BlockSpec(memory_space=pl.ANY)
    block = pl.BlockSpec((dim, tile), lambda j: (0, j))
    lead = (after,) if out is None else (out,)
    return pl.pallas_call(
        add_kernel,
        grid=(size // tile,),
        in_specs=[hbm, block, block],
        out_specs=pl.BlockSpec((dim, tile), lambda j: (0, j + off)),
        out_shape=jax.ShapeDtypeStruct((dim, vocab), F32),
        input_output_aliases={} if out is None else {0: 0},
        compiler_params=pltpu.CompilerParams(dimension_semantics=("arbitrary",), vmem_limit_bytes=16 * 2**20),
        cost_estimate=pl.CostEstimate(flops=dim * size, bytes_accessed=12 * dim * size, transcendentals=0),
        name="add_chunk",
    )(*lead, own, other)


CHUNKS = (GRAD_TILE, 512, 1536, 3584, 3840, 2048, 256)


def solution(mesh):
    n_tp = mesh.shape["tp"]
    swap = [(0, 1), (1, 0)]

    def step(hid_rows, w_final, tab_rows, tea_rows, mask_rows):
        tokens, dim = hid_rows.shape
        vocab = tab_rows.shape[0]
        hid_t = hid_rows.T
        tab_t = tab_rows.T
        mask = mask_rows.reshape(tokens // 128, 128)
        gain = w_final.reshape(1, dim)
        hid_v, hid_own = lift_hidden(hid_t, n_tp)
        hid_part = lax.ppermute(hid_own, "dp", swap)
        mask_other = lax.ppermute(mask, "dp", swap)
        tea_own = lift_teacher(tea_rows)
        tea_other = lax.ppermute(tea_own, "dp", swap)
        x, x_t, stat = stats(hid_v, gain, mask, tab_t, tea_rows)
        stu_col, tea_col, base, scale_rows, part, kl, head_g = head(stat, mask, mask_other, x, x_t, tab_t, tea_rows, n_tp)
        dx = None
        own, other = [], []
        start = 0
        for c, size in enumerate(CHUNKS):
            if c:
                part, kl, dx = chunk_grad(start, size, x, x_t, stu_col, tea_col, tab_t, tea_rows, kl, dx, head_g)
            other.append(lax.ppermute(part, "dp", swap))
            own.append(part)
            start += size
        _, kl, dx = chunk_grad(start, SHARED, x, x_t, stu_col, tea_col, tab_t, tea_rows, kl, dx, head_g)
        rows_other = lax.ppermute(scale_rows, "dp", swap)
        parts = [hid_part]
        for k in range(1, n_tp):
            parts.append(lax.ppermute(hid_part, "tp", [(i, (i + k) % n_tp) for i in range(n_tp)]))
        gh_t, share = reduce_dx(dx, kl, base, hid_t, gain, n_tp)
        share_other = lax.ppermute(share, "dp", swap)
        share = share + share_other
        hid_other = join(parts, n_tp)
        term_own = shared_grad(hid_t, gain, scale_rows, tab_t, tea_own)
        term_other = shared_grad(hid_other, gain, rows_other, tab_t, tea_other)
        out = add_chunk(start, SHARED, vocab, term_own, term_other, None, gh_t)
        start = 0
        for size, a, b in zip(CHUNKS, own, other):
            out = add_chunk(start, size, vocab, a, b, out, gh_t)
            start += size
        return share[1, 0], gh_t.T.astype(BF16), share[0, :dim], out.T

    return jax.shard_map(
        step, mesh=mesh,
        in_specs=(P("dp", None), P(None), P("tp", None), P("dp", "tp"), P("dp")),
        out_specs=(P(), P("dp", None), P(None), P("tp", None)), check_vma=False)
```

```python
import functools
import math

import jax
import jax.numpy as jnp
from jax import lax
from jax.experimental import pallas as pl
from jax.experimental.pallas import tpu as pltpu
from jax.sharding import PartitionSpec as P

SOFT_CAP = 30.0
NORM_EPS = 1e-6
INV_CAP = 1.0 / SOFT_CAP
CAP_LOG2E = SOFT_CAP * math.log2(math.e)
MESH = pl.DeviceIdType.MESH
F32 = jnp.float32
BF16 = jnp.bfloat16
GROUP = 16
VMEM = pltpu.VMEM
NT_DIMS = (((1,), (1,)), ((), ()))


SHARED = 256


def lift_kernel(hid_hbm, tea_hbm, hid_ref, hid_out, tea_out, tea_ref, sem):
    tp = lax.axis_index("tp")
    width = hid_out.shape[1]
    start = tea_hbm.shape[1] - SHARED
    loads = [
        pltpu.make_async_copy(hid_hbm, hid_ref, sem.at[0]),
        pltpu.make_async_copy(tea_hbm.at[:, start:start + SHARED], tea_ref, sem.at[1]),
    ]
    for load in loads:
        load.start()
    loads[0].wait()
    hid_out[...] = hid_ref[:, pl.ds(pl.multiple_of(tp * width, width), width)].astype(F32)
    loads[1].wait()
    tea_out[...] = tea_ref[...].astype(F32)


def lift(hid_t, tea, n_tp):
    dim, tokens = hid_t.shape
    hbm = pl.BlockSpec(memory_space=pl.ANY)
    whole = pl.BlockSpec(memory_space=VMEM)
    return pl.pallas_call(
        lift_kernel,
        in_specs=[hbm, hbm],
        out_specs=[whole, whole, whole],
        out_shape=[
            jax.ShapeDtypeStruct((dim, tokens), BF16),
            jax.ShapeDtypeStruct((dim, tokens // n_tp), F32),
            jax.ShapeDtypeStruct((tokens, SHARED), F32),
        ],
        scratch_shapes=[VMEM((tokens, SHARED), BF16), pltpu.SemaphoreType.DMA((2,))],
        compiler_params=pltpu.CompilerParams(vmem_limit_bytes=48 * 2**20),
        cost_estimate=pl.CostEstimate(flops=3_000_000, bytes_accessed=5_000_000, transcendentals=0),
        name="lift",
    )(hid_t, tea)


def join_kernel(n_tp, *refs):
    out_ref = refs[-1]
    tp = lax.axis_index("tp")
    width = refs[0].shape[1]
    for k, ref in enumerate(refs[:-1]):
        owner = lax.rem(tp - k + n_tp, n_tp)
        out_ref[:, pl.ds(pl.multiple_of(owner * width, width), width)] = ref[...].astype(BF16)


def join(parts, n_tp):
    dim, width = parts[0].shape
    whole = pl.BlockSpec(memory_space=VMEM)
    return pl.pallas_call(
        functools.partial(join_kernel, n_tp),
        in_specs=[whole] * n_tp,
        out_specs=whole,
        out_shape=jax.ShapeDtypeStruct((dim, width * n_tp), BF16),
        compiler_params=pltpu.CompilerParams(vmem_limit_bytes=16 * 2**20),
        cost_estimate=pl.CostEstimate(flops=3_000_000, bytes_accessed=5_000_000, transcendentals=0),
        name="join",
    )(*parts)


def make_x(hid_ref, gain_ref, x_ref, xt_ref):
    dim, tokens = hid_ref.shape
    gain = jnp.broadcast_to(1.0 + gain_ref[...], (128, gain_ref.shape[1])).T[:dim, :]
    for blk in range(tokens // 128):
        hid = hid_ref[:, blk * 128:(blk + 1) * 128].astype(F32)
        inv_rms = lax.rsqrt(jnp.sum(hid * hid, axis=0, keepdims=True) * (1.0 / dim) + NORM_EPS)
        x_t = (hid * inv_rms * gain).astype(BF16)
        xt_ref[:, blk * 128:(blk + 1) * 128] = x_t
        x_ref[blk * 128:(blk + 1) * 128, :] = x_t.T


def shared_kernel(hid_ref, gain_ref, row_ref, tab_ref, tea_ref, de_ref, x_ref, xt_ref, g_ref):
    tokens = x_ref.shape[0]
    make_x(hid_ref, gain_ref, x_ref, xt_ref)
    for blk in range(tokens // 128):
        rows = slice(blk * 128, (blk + 1) * 128)
        stu_scale = jnp.broadcast_to(row_ref[blk:blk + 1, :], (128, 128)).T
        tea_scale = jnp.broadcast_to(row_ref[16 + blk:17 + blk, :], (128, 128)).T
        z = jnp.dot(x_ref[rows, :], tab_ref[...], preferred_element_type=F32)
        for lane in range(0, SHARED, 128):
            lanes = slice(lane, lane + 128)
            stu = jnp.tanh(z[:, lanes] * INV_CAP)
            tea = jnp.tanh(tea_ref[rows, lanes] * INV_CAP)
            stu_p = jnp.exp2(stu * CAP_LOG2E) * stu_scale
            tea_p = jnp.exp2(tea * CAP_LOG2E) * tea_scale
            g_ref[rows, lanes] = ((stu_p - tea_p) * (1.0 - stu * stu)).astype(BF16)
    de_ref[...] = jnp.dot(xt_ref[...], g_ref[...], preferred_element_type=F32)


def shared_grad(hid_t, gain, scale_rows, tab_t, tea):
    dim, tokens = hid_t.shape
    last = tab_t.shape[1] // SHARED - 1

    def spec(shape):
        return pl.BlockSpec(shape, lambda j: (0, 0))

    return pl.pallas_call(
        shared_kernel,
        grid=(1,),
        in_specs=[
            spec(hid_t.shape), spec(gain.shape), spec(scale_rows.shape),
            pl.BlockSpec((dim, SHARED), lambda j: (0, last)), spec(tea.shape),
        ],
        out_specs=spec((dim, SHARED)),
        out_shape=jax.ShapeDtypeStruct((dim, SHARED), F32),
        scratch_shapes=[VMEM((tokens, dim), BF16), VMEM((dim, tokens), BF16), VMEM((tokens, SHARED), BF16)],
        compiler_params=pltpu.CompilerParams(dimension_semantics=("arbitrary",), vmem_limit_bytes=40 * 2**20),
        cost_estimate=pl.CostEstimate(flops=tokens * SHARED * 4 * dim, bytes_accessed=tokens * SHARED * 4, transcendentals=0),
        name="shared_grad",
    )(hid_t, gain, scale_rows, tab_t, tea)


STAT_TILE = 1024
STAT_ROWS = 128
PER_BLOCK = STAT_ROWS // GROUP


def stats_kernel(hid_ref, gain_ref, mask_ref, tab_ref, next_ref, tea_ref, x_ref, xt_ref, stat_ref,
                 stu_acc, tea_acc, z_even, z_odd, count_vmem, count_smem, groups, live, sem):
    step = pl.program_id(0)
    _, tokens = hid_ref.shape
    n_groups = tokens // GROUP

    def source(i):
        return pl.ds(pl.multiple_of(jnp.minimum(groups[i], n_groups - 1) * GROUP, GROUP), GROUP)

    def dest(i):
        return pl.ds(pl.multiple_of(groups[i] * GROUP, GROUP), GROUP)

    def logits(block, table, z_ref):
        rows = jnp.concatenate([x_ref[source(block * PER_BLOCK + i), :] for i in range(PER_BLOCK)], axis=0)
        z_ref[...] = jnp.dot(rows, table[...], preferred_element_type=F32)

    def exp_sum(val):
        val = jnp.exp2(jnp.tanh(val * INV_CAP) * CAP_LOG2E)
        total = val[:, :128]
        for lane in range(128, STAT_TILE, 128):
            total = total + val[:, lane:lane + 128]
        return total

    def accumulate(block, z_ref):
        for i in range(PER_BLOCK):
            at = block * PER_BLOCK + i
            tea_acc[dest(at), :] += exp_sum(tea_ref[source(at), :].astype(F32))
            stu_acc[dest(at), :] += exp_sum(z_ref[i * GROUP:(i + 1) * GROUP, :])

    @pl.when(step == 0)
    def _():
        stu_acc[...] = jnp.zeros_like(stu_acc)
        tea_acc[...] = jnp.zeros_like(tea_acc)
        rows = lax.broadcasted_iota(jnp.int32, (128, 128), 0) // GROUP
        cols = lax.broadcasted_iota(jnp.int32, (128, 128), 1)
        pick = jnp.where(rows == cols, 1.0, 0.0).astype(BF16)
        counts = jnp.dot(mask_ref[...].astype(BF16), pick, preferred_element_type=F32)
        count_vmem[...] = counts.astype(jnp.int32)
        copy = pltpu.make_async_copy(count_vmem, count_smem, sem)
        copy.start()
        make_x(hid_ref, gain_ref, x_ref, xt_ref)
        copy.wait()

        def add_group(g, n):
            groups[n] = g
            keep = count_smem[g // 8, g % 8] > 0
            return n + jnp.where(keep, 1, 0)

        n_live = lax.fori_loop(0, n_groups, add_group, 0)

        def pad(i, c):
            groups[n_live + i] = n_groups
            return c

        lax.fori_loop(0, 2 * PER_BLOCK, pad, 0)
        live[0] = n_live
        logits(0, tab_ref, z_even)

    n_blocks = jnp.maximum((live[0] + PER_BLOCK - 1) // PER_BLOCK, 1)
    more = (n_blocks - 1) // 2

    def pair(p, c):
        logits(2 * p + 1, tab_ref, z_odd)
        accumulate(2 * p, z_even)
        logits(2 * p + 2, tab_ref, z_even)
        accumulate(2 * p + 1, z_odd)
        return c

    lax.fori_loop(0, more, pair, 0)

    @pl.when(n_blocks % 2 == 0)
    def _():
        logits(2 * more + 1, tab_ref, z_odd)
        accumulate(2 * more, z_even)
        logits(0, next_ref, z_even)
        accumulate(2 * more + 1, z_odd)

    @pl.when(n_blocks % 2 == 1)
    def _():
        logits(0, next_ref, z_odd)
        accumulate(2 * more, z_even)
        z_even[...] = z_odd[...]

    @pl.when(step == pl.num_programs(0) - 1)
    def _():
        for blk in range(tokens // 128):
            for k, acc in enumerate((stu_acc, tea_acc)):
                part = acc[blk * 128:(blk + 1) * 128, :].T
                stat_ref[k * 16 + blk:k * 16 + blk + 1, :] = jnp.sum(part, axis=0, keepdims=True)


def stats(hid_t, gain, mask, tab_t, tea):
    dim, tokens = hid_t.shape
    vocab = tab_t.shape[1]
    n_groups = tokens // GROUP
    whole = pl.BlockSpec(memory_space=VMEM)
    return pl.pallas_call(
        stats_kernel,
        grid=(vocab // STAT_TILE,),
        in_specs=[
            whole, whole, whole,
            pl.BlockSpec((dim, STAT_TILE), lambda j: (0, j)),
            pl.BlockSpec((dim, STAT_TILE), lambda j: (0, jnp.minimum(j + 1, vocab // STAT_TILE - 1))),
            pl.BlockSpec((tokens, STAT_TILE), lambda j: (0, j)),
        ],
        out_specs=[whole, whole, whole],
        out_shape=[
            jax.ShapeDtypeStruct((tokens, dim), BF16),
            jax.ShapeDtypeStruct((dim, tokens), BF16),
            jax.ShapeDtypeStruct((32, 128), F32),
        ],
        scratch_shapes=[
            VMEM((tokens + GROUP, 128), F32), VMEM((tokens + GROUP, 128), F32),
            VMEM((STAT_ROWS, STAT_TILE), F32), VMEM((STAT_ROWS, STAT_TILE), F32),
            VMEM((16, 128), jnp.int32), pltpu.SMEM((16, 128), jnp.int32),
            pltpu.SMEM((n_groups + 4 * PER_BLOCK,), jnp.int32), pltpu.SMEM((1,), jnp.int32),
            pltpu.SemaphoreType.DMA,
        ],
        compiler_params=pltpu.CompilerParams(dimension_semantics=("arbitrary",), vmem_limit_bytes=46 * 2**20),
        cost_estimate=pl.CostEstimate(flops=50_000_000_000, bytes_accessed=70_000_000, transcendentals=0),
        name="stats",
    )(hid_t, gain, mask, tab_t, tab_t, tea)


GRAD_TILE = 256
GRAD_ROWS = 256
SLICE = 16


def head_kernel(n_tp, stat_ref, mask_ref, mask_other, x_ref, xt_ref, tab_hbm, tea_hbm, stu_col, tea_col, base_ref, row_ref, de_ref, kl_acc, g_ref,
                slots, tab_ref, tea_ref, stu_q, tea_q, z_even, z_odd, load_sem, send_sem, recv_sem):
    tp = lax.axis_index("tp")
    dp = lax.axis_index("dp")
    tokens = x_ref.shape[0]
    n_blocks = tokens // GRAD_ROWS
    load_tab = pltpu.make_async_copy(tab_hbm.at[:, 0:GRAD_TILE], tab_ref, load_sem.at[0])
    load_tea = pltpu.make_async_copy(tea_hbm.at[:, 0:GRAD_TILE], tea_ref, load_sem.at[1])
    load_tab.start()
    load_tea.start()
    barrier = pltpu.get_barrier_semaphore()
    peers = [(dp, lax.rem(tp + k, n_tp)) for k in range(1, n_tp)]
    for peer in peers:
        pl.semaphore_signal(barrier, inc=1, device_id=peer, device_id_type=MESH)
    pl.semaphore_wait(barrier, len(peers))
    copies = []
    for k, peer in enumerate(peers):
        copies.append(pltpu.make_async_remote_copy(
            src_ref=stat_ref, dst_ref=slots.at[k],
            send_sem=send_sem.at[k], recv_sem=recv_sem.at[k], device_id=peer, device_id_type=MESH))
        copies[-1].start()
    load_tab.wait()
    load_tea.wait()

    def window(b, size=GRAD_ROWS, skip=0):
        return pl.ds(pl.multiple_of(b * GRAD_ROWS + skip, size), size)

    def logits(b, z_ref):
        z_ref[...] = jnp.dot(x_ref[window(b), :], tab_ref[...], preferred_element_type=F32)

    def factors(b, z_ref):
        for skip in range(0, GRAD_ROWS, SLICE):
            rows = window(b, SLICE, skip)
            kl = 0.0
            for lane in range(0, GRAD_TILE, 128):
                stu = jnp.tanh(z_ref[skip:skip + SLICE, lane:lane + 128] * INV_CAP)
                tea = jnp.tanh(tea_ref[rows, lane:lane + 128].astype(F32) * INV_CAP)
                tea_e = jnp.exp2(tea * CAP_LOG2E)
                slope = 1.0 - stu * stu
                kl = kl + tea_e * (tea - stu)
                stu_q[rows, lane:lane + 128] = jnp.exp2(stu * CAP_LOG2E) * slope
                tea_q[rows, lane:lane + 128] = tea_e * slope
            kl_acc[rows, :] = kl

    logits(0, z_even)

    def pair(p, c):
        logits(2 * p + 1, z_odd)
        factors(2 * p, z_even)
        logits(lax.rem(2 * p + 2, n_blocks), z_even)
        factors(2 * p + 1, z_odd)
        return c

    lax.fori_loop(0, n_blocks // 2, pair, 0)

    for copy in copies:
        copy.wait()
    parts = [stat_ref[...]] + [slots[k] for k in range(n_tp - 1)]
    total = jnp.zeros_like(parts[0])
    for owner in range(n_tp):
        gap = lax.rem(tp - owner + n_tp, n_tp)
        part = parts[0]
        for k in range(1, n_tp):
            part = jnp.where(gap == k, parts[k], part)
        total = total + part
    total = jnp.where(total > 0.0, total, 1.0)
    mask = mask_ref[...]
    mask_sum = jnp.sum(mask) + jnp.sum(mask_other[...])
    weight = mask / mask_sum
    stu_sum, tea_sum = total[:16, :], total[16:, :]
    base = jnp.sum(weight * (jnp.log(stu_sum) - jnp.log(tea_sum)))
    base_ref[...] = jnp.full((8, 128), base, F32)
    stu_row, tea_row = weight / stu_sum, weight / tea_sum
    row_ref[:16, :] = stu_row
    row_ref[16:, :] = tea_row
    for blk in range(tokens // 128):
        rows = slice(blk * 128, (blk + 1) * 128)
        stu_scale = jnp.broadcast_to(stu_row[blk:blk + 1, :], (128, 128)).T
        tea_scale = jnp.broadcast_to(tea_row[blk:blk + 1, :], (128, 128)).T
        stu_col[rows, :] = stu_scale
        tea_col[rows, :] = tea_scale
        kl_acc[rows, :] = kl_acc[rows, :] * tea_scale
        for lane in range(0, GRAD_TILE, 128):
            lanes = slice(lane, lane + 128)
            g_ref[rows, lanes] = (stu_q[rows, lanes] * stu_scale - tea_q[rows, lanes] * tea_scale).astype(BF16)
    de_ref[...] = jnp.dot(xt_ref[...], g_ref[...], preferred_element_type=F32)


def head(stat, mask, mask_other, x, x_t, tab_t, tea, n_tp):
    tokens, dim = x.shape
    whole = pl.BlockSpec(memory_space=VMEM)
    hbm = pl.BlockSpec(memory_space=pl.ANY)
    return pl.pallas_call(
        functools.partial(head_kernel, n_tp),
        in_specs=[whole, whole, whole, whole, whole, hbm, hbm],
        out_specs=[whole] * 7,
        out_shape=[
            jax.ShapeDtypeStruct((tokens, 128), F32),
            jax.ShapeDtypeStruct((tokens, 128), F32),
            jax.ShapeDtypeStruct((8, 128), F32),
            jax.ShapeDtypeStruct((32, 128), F32),
            jax.ShapeDtypeStruct((dim, GRAD_TILE), F32),
            jax.ShapeDtypeStruct((tokens, 128), F32),
            jax.ShapeDtypeStruct((tokens, GRAD_TILE), BF16),
        ],
        scratch_shapes=[
            VMEM((n_tp - 1,) + stat.shape, F32),
            VMEM((dim, GRAD_TILE), BF16), VMEM((tokens, GRAD_TILE), BF16),
            VMEM((tokens, GRAD_TILE), F32), VMEM((tokens, GRAD_TILE), F32),
            VMEM((GRAD_ROWS, GRAD_TILE), F32), VMEM((GRAD_ROWS, GRAD_TILE), F32),
            pltpu.SemaphoreType.DMA((2,)), pltpu.SemaphoreType.DMA((n_tp - 1,)), pltpu.SemaphoreType.DMA((n_tp - 1,)),
        ],
        compiler_params=pltpu.CompilerParams(collective_id=0, has_side_effects=True, vmem_limit_bytes=40 * 2**20),
        cost_estimate=pl.CostEstimate(flops=5_000_000_000, bytes_accessed=2_000_000, transcendentals=0),
        name="head",
    )(stat, mask, mask_other, x, x_t, tab_t, tea)


def chunk_kernel(first, x_ref, xt_ref, stu_col, tea_col, tab_ref, tea_ref, _, *refs):
    if first:
        head_g, head_tab, de_ref, kl_acc, dx_acc, g_ref, z_even, z_odd = refs
    else:
        _, de_ref, kl_acc, dx_acc, g_ref, z_even, z_odd = refs
    tokens = x_ref.shape[0]
    n_blocks = tokens // GRAD_ROWS

    if first:
        @pl.when(pl.program_id(0) == 0)
        def _():
            def block(b, c):
                rows = pl.ds(pl.multiple_of(b * GRAD_ROWS, GRAD_ROWS), GRAD_ROWS)
                dx_acc[rows, :] = lax.dot_general(head_g[rows, :], head_tab[...], NT_DIMS, preferred_element_type=F32)
                return c

            lax.fori_loop(0, n_blocks, block, 0)

    def window(b, size=GRAD_ROWS, skip=0):
        return pl.ds(pl.multiple_of(b * GRAD_ROWS + skip, size), size)

    def logits(b, z_ref):
        z_ref[...] = jnp.dot(x_ref[window(b), :], tab_ref[...], preferred_element_type=F32)

    def grads(b, z_ref):
        for skip in range(0, GRAD_ROWS, SLICE):
            rows = window(b, SLICE, skip)
            stu_scale = stu_col[rows, :]
            tea_scale = tea_col[rows, :]
            kl = kl_acc[rows, :]
            parts = []
            for lane in range(0, GRAD_TILE, 128):
                stu = jnp.tanh(z_ref[skip:skip + SLICE, lane:lane + 128] * INV_CAP)
                tea = jnp.tanh(tea_ref[rows, lane:lane + 128].astype(F32) * INV_CAP)
                stu_p = jnp.exp2(stu * CAP_LOG2E) * stu_scale
                tea_p = jnp.exp2(tea * CAP_LOG2E) * tea_scale
                kl = kl + tea_p * (tea - stu)
                parts.append(((stu_p - tea_p) * (1.0 - stu * stu)).astype(BF16))
            kl_acc[rows, :] = kl
            g_ref[rows, :] = jnp.concatenate(parts, axis=1)

    def add_dx(b):
        dx_acc[window(b), :] += lax.dot_general(g_ref[window(b), :], tab_ref[...], NT_DIMS, preferred_element_type=F32)

    logits(0, z_even)
    logits(1, z_odd)
    grads(0, z_even)

    def pair(p, c):
        add_dx(2 * p)
        logits(2 * p + 2, z_even)
        grads(2 * p + 1, z_odd)
        add_dx(2 * p + 1)
        logits(2 * p + 3, z_odd)
        grads(2 * p + 2, z_even)
        return c

    lax.fori_loop(0, n_blocks // 2 - 1, pair, 0)
    add_dx(n_blocks - 2)
    grads(n_blocks - 1, z_odd)
    de_ref[...] = jnp.dot(xt_ref[...], g_ref[...], preferred_element_type=F32)
    add_dx(n_blocks - 1)


def chunk_grad(start, size, x, x_t, stu_col, tea_col, tab_t, tea, kl, dx, head_g):
    tokens, dim = x.shape
    off = start // GRAD_TILE
    whole = pl.BlockSpec(memory_space=VMEM)
    first = dx is None
    work = tokens * size
    return pl.pallas_call(
        functools.partial(chunk_kernel, first),
        grid=(size // GRAD_TILE,),
        in_specs=[
            whole, whole, whole, whole,
            pl.BlockSpec((dim, GRAD_TILE), lambda j: (0, j + off)),
            pl.BlockSpec((tokens, GRAD_TILE), lambda j: (0, j + off)),
            whole,
        ] + ([whole, pl.BlockSpec((dim, GRAD_TILE), lambda j: (0, 0))] if first else [whole]),
        out_specs=[pl.BlockSpec((dim, GRAD_TILE), lambda j: (0, j)), whole, whole],
        out_shape=[
            jax.ShapeDtypeStruct((dim, size), F32),
            jax.ShapeDtypeStruct((tokens, 128), F32),
            jax.ShapeDtypeStruct((tokens, dim), F32),
        ],
        scratch_shapes=[
            VMEM((tokens, GRAD_TILE), BF16), VMEM((GRAD_ROWS, GRAD_TILE), F32), VMEM((GRAD_ROWS, GRAD_TILE), F32),
        ],
        input_output_aliases={6: 1} if first else {6: 1, 7: 2},
        compiler_params=pltpu.CompilerParams(dimension_semantics=("arbitrary",), vmem_limit_bytes=32 * 2**20),
        cost_estimate=pl.CostEstimate(flops=work * 3 * 2 * dim, bytes_accessed=work * 2, transcendentals=0),
        name="chunk_grad",
    )(x, x_t, stu_col, tea_col, tab_t, tea, kl, *((head_g, tab_t) if first else (dx,)))


def dx_kernel(n_tp, dx_ref, kl_ref, base_ref, hid_ref, gain_ref, gh_ref, part_ref,
              slots, own, parts_buf, part_out, send_sem, recv_sem):
    tp = lax.axis_index("tp")
    dp = lax.axis_index("dp")
    dim, tokens = hid_ref.shape
    width = tokens // n_tp
    barrier = pltpu.get_barrier_semaphore()
    peers = [lax.rem(tp + k, n_tp) for k in range(1, n_tp)]
    for peer in peers:
        pl.semaphore_signal(barrier, inc=1, device_id=(dp, peer), device_id_type=MESH)
    pl.semaphore_wait(barrier, n_tp - 1)

    def window(index):
        return pl.ds(pl.multiple_of(index * width, width), width)

    reduce = []
    for k, peer in enumerate(peers):
        reduce.append(pltpu.make_async_remote_copy(
            src_ref=dx_ref.at[window(peer), :], dst_ref=slots.at[k],
            send_sem=send_sem.at[0, k], recv_sem=recv_sem.at[0, k], device_id=(dp, peer), device_id_type=MESH))
        reduce[-1].start()
    for copy in reduce:
        copy.wait()
    mine = window(tp)
    total = jnp.zeros((width, dim), F32)
    for owner in range(n_tp):
        gap = lax.rem(tp - owner + n_tp, n_tp)
        part = dx_ref[mine, :]
        for k in range(1, n_tp):
            part = jnp.where(gap == k, slots[k - 1], part)
        total = total + part
    grad_x = total.T
    gain = jnp.broadcast_to(1.0 + gain_ref[...], (128, gain_ref.shape[1])).T[:dim, :1]
    hid = hid_ref[:, mine].astype(F32)
    inv_rms = lax.rsqrt(jnp.sum(hid * hid, axis=0, keepdims=True) * (1.0 / dim) + NORM_EPS)
    normed = hid * inv_rms
    grad_n = grad_x * gain
    corr = jnp.sum(grad_n * normed, axis=0, keepdims=True) * (1.0 / dim)
    own[...] = inv_rms * (grad_n - normed * corr)

    prod = grad_x * normed
    col = prod[:, :128]
    for lane in range(128, width, 128):
        col = col + prod[:, lane:lane + 128]
    row = jnp.sum(col.T, axis=0, keepdims=True)
    part_out[0:1, :dim] = row
    part_out[0:1, dim:] = jnp.zeros((1, part_out.shape[1] - dim), F32)
    loss = SOFT_CAP * jnp.sum(kl_ref[...]) + jnp.sum(base_ref[0:1, 0:1]) * (1.0 / n_tp)
    part_out[1:2, :] = jnp.full((1, part_out.shape[1]), loss, F32)
    part_out[2:8, :] = jnp.zeros((6, part_out.shape[1]), F32)

    spread = []
    for k, peer in enumerate(peers):
        spread.append(pltpu.make_async_remote_copy(
            src_ref=own, dst_ref=gh_ref.at[:, mine],
            send_sem=send_sem.at[1, k], recv_sem=recv_sem.at[1, k], device_id=(dp, peer), device_id_type=MESH))
        spread.append(pltpu.make_async_remote_copy(
            src_ref=part_out, dst_ref=parts_buf.at[tp],
            send_sem=send_sem.at[2, k], recv_sem=recv_sem.at[2, k], device_id=(dp, peer), device_id_type=MESH))
    for copy in spread:
        copy.start()
    gh_ref[:, mine] = own[...]
    parts_buf[tp] = part_out[...]
    for copy in spread:
        copy.wait()
    share = parts_buf[0]
    for k in range(1, n_tp):
        share = share + parts_buf[k]
    part_ref[...] = share


def reduce_dx(dx, kl, base, hid_t, gain, n_tp):
    tokens, dim = dx.shape
    width = tokens // n_tp
    whole = pl.BlockSpec(memory_space=VMEM)
    return pl.pallas_call(
        functools.partial(dx_kernel, n_tp),
        in_specs=[whole, whole, whole, whole, whole],
        out_specs=[whole, whole],
        out_shape=[
            jax.ShapeDtypeStruct((dim, tokens), F32),
            jax.ShapeDtypeStruct((8, 640), F32),
        ],
        scratch_shapes=[
            VMEM((n_tp - 1, width, dim), F32), VMEM((dim, width), F32),
            VMEM((n_tp, 8, 640), F32), VMEM((8, 640), F32),
            pltpu.SemaphoreType.DMA((3, n_tp - 1)), pltpu.SemaphoreType.DMA((3, n_tp - 1)),
        ],
        compiler_params=pltpu.CompilerParams(collective_id=1, has_side_effects=True, vmem_limit_bytes=24 * 2**20),
        cost_estimate=pl.CostEstimate(flops=50_000_000_000, bytes_accessed=20_000_000, transcendentals=0),
        name="reduce_dx",
    )(dx, kl, base, hid_t, gain)


def add_kernel(*refs):
    a_ref, b_ref, out_ref = refs[-3], refs[-2], refs[-1]
    out_ref[...] = a_ref[...] + b_ref[...]


def add_chunk(start, size, vocab, own, other, out, after):
    dim = own.shape[0]
    tile = math.gcd(math.gcd(start, size), 512)
    off = start // tile
    hbm = pl.BlockSpec(memory_space=pl.ANY)
    block = pl.BlockSpec((dim, tile), lambda j: (0, j))
    lead = (after,) if out is None else (out,)
    return pl.pallas_call(
        add_kernel,
        grid=(size // tile,),
        in_specs=[hbm, block, block],
        out_specs=pl.BlockSpec((dim, tile), lambda j: (0, j + off)),
        out_shape=jax.ShapeDtypeStruct((dim, vocab), F32),
        input_output_aliases={} if out is None else {0: 0},
        compiler_params=pltpu.CompilerParams(dimension_semantics=("arbitrary",), vmem_limit_bytes=16 * 2**20),
        cost_estimate=pl.CostEstimate(flops=dim * size, bytes_accessed=12 * dim * size, transcendentals=0),
        name="add_chunk",
    )(*lead, own, other)


CHUNKS = (GRAD_TILE, 512, 1536, 3584, 3584, 2048, 256, 256)


def solution(mesh):
    n_tp = mesh.shape["tp"]
    swap = [(0, 1), (1, 0)]

    def step(hid_rows, w_final, tab_rows, tea_rows, mask_rows):
        tokens, dim = hid_rows.shape
        vocab = tab_rows.shape[0]
        hid_t = hid_rows.T
        tab_t = tab_rows.T
        mask = mask_rows.reshape(tokens // 128, 128)
        gain = w_final.reshape(1, dim)
        hid_v, hid_own, tea_own = lift(hid_t, tea_rows, n_tp)
        hid_part = lax.ppermute(hid_own, "dp", swap)
        mask_other = lax.ppermute(mask, "dp", swap)
        tea_other = lax.ppermute(tea_own, "dp", swap)
        x, x_t, stat = stats(hid_v, gain, mask, tab_t, tea_rows)
        stu_col, tea_col, base, scale_rows, part, kl, head_g = head(stat, mask, mask_other, x, x_t, tab_t, tea_rows, n_tp)
        dx = None
        own, other = [], []
        start = 0
        for c, size in enumerate(CHUNKS):
            if c:
                part, kl, dx = chunk_grad(start, size, x, x_t, stu_col, tea_col, tab_t, tea_rows, kl, dx, head_g)
            other.append(lax.ppermute(part, "dp", swap))
            own.append(part)
            start += size
        _, kl, dx = chunk_grad(start, SHARED, x, x_t, stu_col, tea_col, tab_t, tea_rows, kl, dx, head_g)
        rows_other = lax.ppermute(scale_rows, "dp", swap)
        parts = [hid_part]
        for k in range(1, n_tp):
            parts.append(lax.ppermute(hid_part, "tp", [(i, (i + k) % n_tp) for i in range(n_tp)]))
        gh_t, share = reduce_dx(dx, kl, base, hid_t, gain, n_tp)
        share_other = lax.ppermute(share, "dp", swap)
        share = share + share_other
        hid_other = join(parts, n_tp)
        term_own = shared_grad(hid_t, gain, scale_rows, tab_t, tea_own)
        term_other = shared_grad(hid_other, gain, rows_other, tab_t, tea_other)
        out = add_chunk(start, SHARED, vocab, term_own, term_other, None, gh_t)
        start = 0
        for size, a, b in zip(CHUNKS, own, other):
            out = add_chunk(start, size, vocab, a, b, out, gh_t)
            start += size
        return share[1, 0], gh_t.T.astype(BF16), share[0, :dim], out.T

    return jax.shard_map(
        step, mesh=mesh,
        in_specs=(P("dp", None), P(None), P("tp", None), P("dp", "tp"), P("dp")),
        out_specs=(P(), P("dp", None), P(None), P("tp", None)), check_vma=False)
```

```python
import functools
import math

import jax
import jax.numpy as jnp
from jax import lax
from jax.experimental import pallas as pl
from jax.experimental.pallas import tpu as pltpu
from jax.sharding import PartitionSpec as P

SOFT_CAP = 30.0
NORM_EPS = 1e-6
INV_CAP = 1.0 / SOFT_CAP
CAP_LOG2E = SOFT_CAP * math.log2(math.e)
MESH = pl.DeviceIdType.MESH
F32 = jnp.float32
BF16 = jnp.bfloat16
GROUP = 16
VMEM = pltpu.VMEM
NT_DIMS = (((1,), (1,)), ((), ()))


SHARED = 256


LIFT_PARTS = 4


def lift_kernel(hid_hbm, tea_hbm, hid_ref, hid_out, tea_out, run_ref, tea_ref, run_f32, tea_f32, load_sem, save_sem):
    tp = lax.axis_index("tp")
    width = run_ref.shape[1]
    vocab = tea_hbm.shape[1]
    rows = tea_ref.shape[0] // LIFT_PARTS
    run = pltpu.make_async_copy(hid_hbm.at[:, pl.ds(pl.multiple_of(tp * width, width), width)], run_ref, load_sem.at[0])
    run.start()
    parts = [slice(p * rows, (p + 1) * rows) for p in range(LIFT_PARTS)]
    loads = [pltpu.make_async_copy(tea_hbm.at[part, vocab - SHARED:vocab], tea_ref.at[part, :], load_sem.at[2 + p])
             for p, part in enumerate(parts)]
    for load in loads:
        load.start()
    hid = pltpu.make_async_copy(hid_hbm, hid_ref, load_sem.at[1])
    hid.start()
    run.wait()
    run_f32[...] = run_ref[...].astype(F32)
    saves = [pltpu.make_async_copy(run_f32, hid_out, save_sem.at[0])]
    saves[0].start()
    for p, part in enumerate(parts):
        loads[p].wait()
        tea_f32[part, :] = tea_ref[part, :].astype(F32)
        saves.append(pltpu.make_async_copy(tea_f32.at[part, :], tea_out.at[part, :], save_sem.at[1 + p]))
        saves[-1].start()
    hid.wait()
    for save in saves:
        save.wait()


def lift(hid_t, tea, n_tp):
    dim, tokens = hid_t.shape
    width = tokens // n_tp
    hbm = pl.BlockSpec(memory_space=pl.ANY)
    return pl.pallas_call(
        lift_kernel,
        in_specs=[hbm, hbm],
        out_specs=[pl.BlockSpec(memory_space=VMEM), hbm, hbm],
        out_shape=[
            jax.ShapeDtypeStruct((dim, tokens), BF16),
            jax.ShapeDtypeStruct((dim, width), F32),
            jax.ShapeDtypeStruct((tokens, SHARED), F32),
        ],
        scratch_shapes=[
            VMEM((dim, width), BF16), VMEM((tokens, SHARED), BF16), VMEM((dim, width), F32), VMEM((tokens, SHARED), F32),
            pltpu.SemaphoreType.DMA((2 + LIFT_PARTS,)), pltpu.SemaphoreType.DMA((1 + LIFT_PARTS,)),
        ],
        compiler_params=pltpu.CompilerParams(vmem_limit_bytes=97 * 2**19),
        cost_estimate=pl.CostEstimate(flops=3_000_000, bytes_accessed=5_000_000, transcendentals=0),
        name="lift",
    )(hid_t, tea)


def join_kernel(n_tp, *refs):
    out_ref = refs[-1]
    tp = lax.axis_index("tp")
    width = refs[0].shape[1]
    for k, ref in enumerate(refs[:-1]):
        owner = lax.rem(tp - k + n_tp, n_tp)
        out_ref[:, pl.ds(pl.multiple_of(owner * width, width), width)] = ref[...].astype(BF16)


def join(parts, n_tp):
    dim, width = parts[0].shape
    whole = pl.BlockSpec(memory_space=VMEM)
    return pl.pallas_call(
        functools.partial(join_kernel, n_tp),
        in_specs=[whole] * n_tp,
        out_specs=whole,
        out_shape=jax.ShapeDtypeStruct((dim, width * n_tp), BF16),
        compiler_params=pltpu.CompilerParams(vmem_limit_bytes=16 * 2**20),
        cost_estimate=pl.CostEstimate(flops=3_000_000, bytes_accessed=5_000_000, transcendentals=0),
        name="join",
    )(*parts)


def make_x(hid_ref, gain_ref, x_ref, xt_ref):
    dim, tokens = hid_ref.shape
    gain = jnp.broadcast_to(1.0 + gain_ref[...], (128, gain_ref.shape[1])).T[:dim, :]
    for blk in range(tokens // 128):
        hid = hid_ref[:, blk * 128:(blk + 1) * 128].astype(F32)
        inv_rms = lax.rsqrt(jnp.sum(hid * hid, axis=0, keepdims=True) * (1.0 / dim) + NORM_EPS)
        x_t = (hid * inv_rms * gain).astype(BF16)
        xt_ref[:, blk * 128:(blk + 1) * 128] = x_t
        x_ref[blk * 128:(blk + 1) * 128, :] = x_t.T


def shared_kernel(hid_ref, gain_ref, row_ref, tab_ref, tea_ref, de_ref, x_ref, xt_ref, g_ref):
    tokens = x_ref.shape[0]
    make_x(hid_ref, gain_ref, x_ref, xt_ref)
    for blk in range(tokens // 128):
        rows = slice(blk * 128, (blk + 1) * 128)
        stu_scale = jnp.broadcast_to(row_ref[blk:blk + 1, :], (128, 128)).T
        tea_scale = jnp.broadcast_to(row_ref[16 + blk:17 + blk, :], (128, 128)).T
        z = jnp.dot(x_ref[rows, :], tab_ref[...], preferred_element_type=F32)
        for lane in range(0, SHARED, 128):
            lanes = slice(lane, lane + 128)
            stu = jnp.tanh(z[:, lanes] * INV_CAP)
            tea = jnp.tanh(tea_ref[rows, lanes] * INV_CAP)
            stu_p = jnp.exp2(stu * CAP_LOG2E) * stu_scale
            tea_p = jnp.exp2(tea * CAP_LOG2E) * tea_scale
            g_ref[rows, lanes] = ((stu_p - tea_p) * (1.0 - stu * stu)).astype(BF16)
    de_ref[...] = jnp.dot(xt_ref[...], g_ref[...], preferred_element_type=F32)


def shared_grad(hid_t, gain, scale_rows, tab_t, tea):
    dim, tokens = hid_t.shape
    last = tab_t.shape[1] // SHARED - 1

    def spec(shape):
        return pl.BlockSpec(shape, lambda j: (0, 0))

    return pl.pallas_call(
        shared_kernel,
        grid=(1,),
        in_specs=[
            spec(hid_t.shape), spec(gain.shape), spec(scale_rows.shape),
            pl.BlockSpec((dim, SHARED), lambda j: (0, last)), spec(tea.shape),
        ],
        out_specs=spec((dim, SHARED)),
        out_shape=jax.ShapeDtypeStruct((dim, SHARED), F32),
        scratch_shapes=[VMEM((tokens, dim), BF16), VMEM((dim, tokens), BF16), VMEM((tokens, SHARED), BF16)],
        compiler_params=pltpu.CompilerParams(dimension_semantics=("arbitrary",), vmem_limit_bytes=40 * 2**20),
        cost_estimate=pl.CostEstimate(flops=tokens * SHARED * 4 * dim, bytes_accessed=tokens * SHARED * 4, transcendentals=0),
        name="shared_grad",
    )(hid_t, gain, scale_rows, tab_t, tea)


STAT_TILE = 1024
STAT_ROWS = 128
PER_BLOCK = STAT_ROWS // GROUP


def stats_kernel(hid_ref, gain_ref, mask_ref, tab_ref, next_ref, tea_ref, x_ref, xt_ref, stat_ref,
                 stu_acc, tea_acc, z_even, z_odd, count_vmem, count_smem, groups, live, sem):
    step = pl.program_id(0)
    _, tokens = hid_ref.shape
    n_groups = tokens // GROUP

    def source(i):
        return pl.ds(pl.multiple_of(jnp.minimum(groups[i], n_groups - 1) * GROUP, GROUP), GROUP)

    def dest(i):
        return pl.ds(pl.multiple_of(groups[i] * GROUP, GROUP), GROUP)

    def logits(block, table, z_ref):
        rows = jnp.concatenate([x_ref[source(block * PER_BLOCK + i), :] for i in range(PER_BLOCK)], axis=0)
        z_ref[...] = jnp.dot(rows, table[...], preferred_element_type=F32)

    def exp_sum(val):
        val = jnp.exp2(jnp.tanh(val * INV_CAP) * CAP_LOG2E)
        total = val[:, :128]
        for lane in range(128, STAT_TILE, 128):
            total = total + val[:, lane:lane + 128]
        return total

    def accumulate(block, z_ref, count=PER_BLOCK):
        for i in range(count):
            at = block * PER_BLOCK + i
            tea_acc[dest(at), :] += exp_sum(tea_ref[source(at), :].astype(F32))
            stu_acc[dest(at), :] += exp_sum(z_ref[i * GROUP:(i + 1) * GROUP, :])

    @pl.when(step == 0)
    def _():
        stu_acc[...] = jnp.zeros_like(stu_acc)
        tea_acc[...] = jnp.zeros_like(tea_acc)
        rows = lax.broadcasted_iota(jnp.int32, (128, 128), 0) // GROUP
        cols = lax.broadcasted_iota(jnp.int32, (128, 128), 1)
        pick = jnp.where(rows == cols, 1.0, 0.0).astype(BF16)
        counts = jnp.dot(mask_ref[...].astype(BF16), pick, preferred_element_type=F32)
        count_vmem[...] = counts.astype(jnp.int32)
        copy = pltpu.make_async_copy(count_vmem, count_smem, sem)
        copy.start()
        make_x(hid_ref, gain_ref, x_ref, xt_ref)
        copy.wait()

        def add_group(g, n):
            groups[n] = g
            keep = count_smem[g // 8, g % 8] > 0
            return n + jnp.where(keep, 1, 0)

        n_live = lax.fori_loop(0, n_groups, add_group, 0)

        def pad(i, c):
            groups[n_live + i] = n_groups
            return c

        lax.fori_loop(0, 2 * PER_BLOCK, pad, 0)
        live[0] = n_live
        logits(0, tab_ref, z_even)

    n_blocks = jnp.maximum((live[0] + PER_BLOCK - 1) // PER_BLOCK, 1)
    more = (n_blocks - 1) // 2

    def pair(p, c):
        logits(2 * p + 1, tab_ref, z_odd)
        accumulate(2 * p, z_even)
        logits(2 * p + 2, tab_ref, z_even)
        accumulate(2 * p + 1, z_odd)
        return c

    lax.fori_loop(0, more, pair, 0)

    is_half = n_blocks * PER_BLOCK - live[0] >= PER_BLOCK // 2
    for half, count in ((False, PER_BLOCK), (True, PER_BLOCK // 2)):
        chosen = is_half if half else jnp.logical_not(is_half)

        @pl.when(jnp.logical_and(n_blocks % 2 == 0, chosen))
        def _():
            logits(2 * more + 1, tab_ref, z_odd)
            accumulate(2 * more, z_even)
            logits(0, next_ref, z_even)
            accumulate(2 * more + 1, z_odd, count)

        @pl.when(jnp.logical_and(n_blocks % 2 == 1, chosen))
        def _():
            logits(0, next_ref, z_odd)
            accumulate(2 * more, z_even, count)
            z_even[...] = z_odd[...]

    @pl.when(step == pl.num_programs(0) - 1)
    def _():
        for blk in range(tokens // 128):
            for k, acc in enumerate((stu_acc, tea_acc)):
                part = acc[blk * 128:(blk + 1) * 128, :].T
                stat_ref[k * 16 + blk:k * 16 + blk + 1, :] = jnp.sum(part, axis=0, keepdims=True)


def stats(hid_t, gain, mask, tab_t, tea):
    dim, tokens = hid_t.shape
    vocab = tab_t.shape[1]
    n_groups = tokens // GROUP
    whole = pl.BlockSpec(memory_space=VMEM)
    return pl.pallas_call(
        stats_kernel,
        grid=(vocab // STAT_TILE,),
        in_specs=[
            whole, whole, whole,
            pl.BlockSpec((dim, STAT_TILE), lambda j: (0, j)),
            pl.BlockSpec((dim, STAT_TILE), lambda j: (0, jnp.minimum(j + 1, vocab // STAT_TILE - 1))),
            pl.BlockSpec((tokens, STAT_TILE), lambda j: (0, j)),
        ],
        out_specs=[whole, whole, whole],
        out_shape=[
            jax.ShapeDtypeStruct((tokens, dim), BF16),
            jax.ShapeDtypeStruct((dim, tokens), BF16),
            jax.ShapeDtypeStruct((32, 128), F32),
        ],
        scratch_shapes=[
            VMEM((tokens + GROUP, 128), F32), VMEM((tokens + GROUP, 128), F32),
            VMEM((STAT_ROWS, STAT_TILE), F32), VMEM((STAT_ROWS, STAT_TILE), F32),
            VMEM((16, 128), jnp.int32), pltpu.SMEM((16, 128), jnp.int32),
            pltpu.SMEM((n_groups + 4 * PER_BLOCK,), jnp.int32), pltpu.SMEM((1,), jnp.int32),
            pltpu.SemaphoreType.DMA,
        ],
        compiler_params=pltpu.CompilerParams(dimension_semantics=("arbitrary",), vmem_limit_bytes=46 * 2**20),
        cost_estimate=pl.CostEstimate(flops=50_000_000_000, bytes_accessed=70_000_000, transcendentals=0),
        name="stats",
    )(hid_t, gain, mask, tab_t, tab_t, tea)


GRAD_TILE = 256
GRAD_ROWS = 256
SLICE = 16


def head_kernel(n_tp, stat_ref, mask_ref, mask_other, x_ref, xt_ref, tab_hbm, tea_hbm, stu_col, tea_col, base_ref, row_ref, de_ref, kl_acc, g_ref,
                slots, tab_ref, tea_ref, stu_q, tea_q, z_even, z_odd, load_sem, send_sem, recv_sem):
    tp = lax.axis_index("tp")
    dp = lax.axis_index("dp")
    tokens = x_ref.shape[0]
    n_blocks = tokens // GRAD_ROWS
    load_tab = pltpu.make_async_copy(tab_hbm.at[:, 0:GRAD_TILE], tab_ref, load_sem.at[0])
    load_tea = pltpu.make_async_copy(tea_hbm.at[:, 0:GRAD_TILE], tea_ref, load_sem.at[1])
    load_tab.start()
    load_tea.start()
    barrier = pltpu.get_barrier_semaphore()
    peers = [(dp, lax.rem(tp + k, n_tp)) for k in range(1, n_tp)]
    for peer in peers:
        pl.semaphore_signal(barrier, inc=1, device_id=peer, device_id_type=MESH)
    pl.semaphore_wait(barrier, len(peers))
    copies = []
    for k, peer in enumerate(peers):
        copies.append(pltpu.make_async_remote_copy(
            src_ref=stat_ref, dst_ref=slots.at[k],
            send_sem=send_sem.at[k], recv_sem=recv_sem.at[k], device_id=peer, device_id_type=MESH))
        copies[-1].start()
    load_tab.wait()
    load_tea.wait()

    def window(b, size=GRAD_ROWS, skip=0):
        return pl.ds(pl.multiple_of(b * GRAD_ROWS + skip, size), size)

    def logits(b, z_ref):
        z_ref[...] = jnp.dot(x_ref[window(b), :], tab_ref[...], preferred_element_type=F32)

    def factors(b, z_ref):
        for skip in range(0, GRAD_ROWS, SLICE):
            rows = window(b, SLICE, skip)
            kl = 0.0
            for lane in range(0, GRAD_TILE, 128):
                stu = jnp.tanh(z_ref[skip:skip + SLICE, lane:lane + 128] * INV_CAP)
                tea = jnp.tanh(tea_ref[rows, lane:lane + 128].astype(F32) * INV_CAP)
                tea_e = jnp.exp2(tea * CAP_LOG2E)
                slope = 1.0 - stu * stu
                kl = kl + tea_e * (tea - stu)
                stu_q[rows, lane:lane + 128] = jnp.exp2(stu * CAP_LOG2E) * slope
                tea_q[rows, lane:lane + 128] = tea_e * slope
            kl_acc[rows, :] = kl

    logits(0, z_even)

    def pair(p, c):
        logits(2 * p + 1, z_odd)
        factors(2 * p, z_even)
        logits(lax.rem(2 * p + 2, n_blocks), z_even)
        factors(2 * p + 1, z_odd)
        return c

    lax.fori_loop(0, n_blocks // 2, pair, 0)

    for copy in copies:
        copy.wait()
    parts = [stat_ref[...]] + [slots[k] for k in range(n_tp - 1)]
    total = jnp.zeros_like(parts[0])
    for owner in range(n_tp):
        gap = lax.rem(tp - owner + n_tp, n_tp)
        part = parts[0]
        for k in range(1, n_tp):
            part = jnp.where(gap == k, parts[k], part)
        total = total + part
    total = jnp.where(total > 0.0, total, 1.0)
    mask = mask_ref[...]
    mask_sum = jnp.sum(mask) + jnp.sum(mask_other[...])
    weight = mask / mask_sum
    stu_sum, tea_sum = total[:16, :], total[16:, :]
    base = jnp.sum(weight * (jnp.log(stu_sum) - jnp.log(tea_sum)))
    base_ref[...] = jnp.full((8, 128), base, F32)
    stu_row, tea_row = weight / stu_sum, weight / tea_sum
    row_ref[:16, :] = stu_row
    row_ref[16:, :] = tea_row
    for blk in range(tokens // 128):
        rows = slice(blk * 128, (blk + 1) * 128)
        stu_scale = jnp.broadcast_to(stu_row[blk:blk + 1, :], (128, 128)).T
        tea_scale = jnp.broadcast_to(tea_row[blk:blk + 1, :], (128, 128)).T
        stu_col[rows, :] = stu_scale
        tea_col[rows, :] = tea_scale
        kl_acc[rows, :] = kl_acc[rows, :] * tea_scale
        for lane in range(0, GRAD_TILE, 128):
            lanes = slice(lane, lane + 128)
            g_ref[rows, lanes] = (stu_q[rows, lanes] * stu_scale - tea_q[rows, lanes] * tea_scale).astype(BF16)
    de_ref[...] = jnp.dot(xt_ref[...], g_ref[...], preferred_element_type=F32)


def head(stat, mask, mask_other, x, x_t, tab_t, tea, n_tp):
    tokens, dim = x.shape
    whole = pl.BlockSpec(memory_space=VMEM)
    hbm = pl.BlockSpec(memory_space=pl.ANY)
    return pl.pallas_call(
        functools.partial(head_kernel, n_tp),
        in_specs=[whole, whole, whole, whole, whole, hbm, hbm],
        out_specs=[whole] * 7,
        out_shape=[
            jax.ShapeDtypeStruct((tokens, 128), F32),
            jax.ShapeDtypeStruct((tokens, 128), F32),
            jax.ShapeDtypeStruct((8, 128), F32),
            jax.ShapeDtypeStruct((32, 128), F32),
            jax.ShapeDtypeStruct((dim, GRAD_TILE), F32),
            jax.ShapeDtypeStruct((tokens, 128), F32),
            jax.ShapeDtypeStruct((tokens, GRAD_TILE), BF16),
        ],
        scratch_shapes=[
            VMEM((n_tp - 1,) + stat.shape, F32),
            VMEM((dim, GRAD_TILE), BF16), VMEM((tokens, GRAD_TILE), BF16),
            VMEM((tokens, GRAD_TILE), F32), VMEM((tokens, GRAD_TILE), F32),
            VMEM((GRAD_ROWS, GRAD_TILE), F32), VMEM((GRAD_ROWS, GRAD_TILE), F32),
            pltpu.SemaphoreType.DMA((2,)), pltpu.SemaphoreType.DMA((n_tp - 1,)), pltpu.SemaphoreType.DMA((n_tp - 1,)),
        ],
        compiler_params=pltpu.CompilerParams(collective_id=0, has_side_effects=True, vmem_limit_bytes=40 * 2**20),
        cost_estimate=pl.CostEstimate(flops=5_000_000_000, bytes_accessed=2_000_000, transcendentals=0),
        name="head",
    )(stat, mask, mask_other, x, x_t, tab_t, tea)


def chunk_kernel(first, x_ref, xt_ref, stu_col, tea_col, tab_ref, tea_ref, _, *refs):
    if first:
        head_g, head_tab, de_ref, kl_acc, dx_acc, g_ref, z_even, z_odd = refs
    else:
        _, de_ref, kl_acc, dx_acc, g_ref, z_even, z_odd = refs
    tokens = x_ref.shape[0]
    n_blocks = tokens // GRAD_ROWS

    if first:
        @pl.when(pl.program_id(0) == 0)
        def _():
            def block(b, c):
                rows = pl.ds(pl.multiple_of(b * GRAD_ROWS, GRAD_ROWS), GRAD_ROWS)
                dx_acc[rows, :] = lax.dot_general(head_g[rows, :], head_tab[...], NT_DIMS, preferred_element_type=F32)
                return c

            lax.fori_loop(0, n_blocks, block, 0)

    def window(b, size=GRAD_ROWS, skip=0):
        return pl.ds(pl.multiple_of(b * GRAD_ROWS + skip, size), size)

    def logits(b, z_ref):
        z_ref[...] = jnp.dot(x_ref[window(b), :], tab_ref[...], preferred_element_type=F32)

    def grads(b, z_ref):
        for skip in range(0, GRAD_ROWS, SLICE):
            rows = window(b, SLICE, skip)
            stu_scale = stu_col[rows, :]
            tea_scale = tea_col[rows, :]
            kl = kl_acc[rows, :]
            parts = []
            for lane in range(0, GRAD_TILE, 128):
                stu = jnp.tanh(z_ref[skip:skip + SLICE, lane:lane + 128] * INV_CAP)
                tea = jnp.tanh(tea_ref[rows, lane:lane + 128].astype(F32) * INV_CAP)
                stu_p = jnp.exp2(stu * CAP_LOG2E) * stu_scale
                tea_p = jnp.exp2(tea * CAP_LOG2E) * tea_scale
                kl = kl + tea_p * (tea - stu)
                parts.append(((stu_p - tea_p) * (1.0 - stu * stu)).astype(BF16))
            kl_acc[rows, :] = kl
            g_ref[rows, :] = jnp.concatenate(parts, axis=1)

    def add_dx(b):
        dx_acc[window(b), :] += lax.dot_general(g_ref[window(b), :], tab_ref[...], NT_DIMS, preferred_element_type=F32)

    logits(0, z_even)
    logits(1, z_odd)
    grads(0, z_even)

    def pair(p, c):
        add_dx(2 * p)
        logits(2 * p + 2, z_even)
        grads(2 * p + 1, z_odd)
        add_dx(2 * p + 1)
        logits(2 * p + 3, z_odd)
        grads(2 * p + 2, z_even)
        return c

    lax.fori_loop(0, n_blocks // 2 - 1, pair, 0)
    add_dx(n_blocks - 2)
    grads(n_blocks - 1, z_odd)
    de_ref[...] = jnp.dot(xt_ref[...], g_ref[...], preferred_element_type=F32)
    add_dx(n_blocks - 1)


def chunk_grad(start, size, x, x_t, stu_col, tea_col, tab_t, tea, kl, dx, head_g):
    tokens, dim = x.shape
    off = start // GRAD_TILE
    whole = pl.BlockSpec(memory_space=VMEM)
    first = dx is None
    work = tokens * size
    return pl.pallas_call(
        functools.partial(chunk_kernel, first),
        grid=(size // GRAD_TILE,),
        in_specs=[
            whole, whole, whole, whole,
            pl.BlockSpec((dim, GRAD_TILE), lambda j: (0, j + off)),
            pl.BlockSpec((tokens, GRAD_TILE), lambda j: (0, j + off)),
            whole,
        ] + ([whole, pl.BlockSpec((dim, GRAD_TILE), lambda j: (0, 0))] if first else [whole]),
        out_specs=[pl.BlockSpec((dim, GRAD_TILE), lambda j: (0, j)), whole, whole],
        out_shape=[
            jax.ShapeDtypeStruct((dim, size), F32),
            jax.ShapeDtypeStruct((tokens, 128), F32),
            jax.ShapeDtypeStruct((tokens, dim), F32),
        ],
        scratch_shapes=[
            VMEM((tokens, GRAD_TILE), BF16), VMEM((GRAD_ROWS, GRAD_TILE), F32), VMEM((GRAD_ROWS, GRAD_TILE), F32),
        ],
        input_output_aliases={6: 1} if first else {6: 1, 7: 2},
        compiler_params=pltpu.CompilerParams(dimension_semantics=("arbitrary",), vmem_limit_bytes=32 * 2**20),
        cost_estimate=pl.CostEstimate(flops=work * 3 * 2 * dim, bytes_accessed=work * 2, transcendentals=0),
        name="chunk_grad",
    )(x, x_t, stu_col, tea_col, tab_t, tea, kl, *((head_g, tab_t) if first else (dx,)))


def dx_kernel(n_tp, dx_ref, kl_ref, base_ref, hid_ref, gain_ref, gh_ref, part_ref,
              slots, own, parts_buf, part_out, send_sem, recv_sem):
    tp = lax.axis_index("tp")
    dp = lax.axis_index("dp")
    dim, tokens = hid_ref.shape
    width = tokens // n_tp
    barrier = pltpu.get_barrier_semaphore()
    peers = [lax.rem(tp + k, n_tp) for k in range(1, n_tp)]
    for peer in peers:
        pl.semaphore_signal(barrier, inc=1, device_id=(dp, peer), device_id_type=MESH)
    pl.semaphore_wait(barrier, n_tp - 1)

    def window(index):
        return pl.ds(pl.multiple_of(index * width, width), width)

    reduce = []
    for k, peer in enumerate(peers):
        reduce.append(pltpu.make_async_remote_copy(
            src_ref=dx_ref.at[window(peer), :], dst_ref=slots.at[k],
            send_sem=send_sem.at[0, k], recv_sem=recv_sem.at[0, k], device_id=(dp, peer), device_id_type=MESH))
        reduce[-1].start()
    for copy in reduce:
        copy.wait()
    mine = window(tp)
    total = jnp.zeros((width, dim), F32)
    for owner in range(n_tp):
        gap = lax.rem(tp - owner + n_tp, n_tp)
        part = dx_ref[mine, :]
        for k in range(1, n_tp):
            part = jnp.where(gap == k, slots[k - 1], part)
        total = total + part
    grad_x = total.T
    gain = jnp.broadcast_to(1.0 + gain_ref[...], (128, gain_ref.shape[1])).T[:dim, :1]
    hid = hid_ref[:, mine].astype(F32)
    inv_rms = lax.rsqrt(jnp.sum(hid * hid, axis=0, keepdims=True) * (1.0 / dim) + NORM_EPS)
    normed = hid * inv_rms
    grad_n = grad_x * gain
    corr = jnp.sum(grad_n * normed, axis=0, keepdims=True) * (1.0 / dim)
    own[...] = inv_rms * (grad_n - normed * corr)

    prod = grad_x * normed
    col = prod[:, :128]
    for lane in range(128, width, 128):
        col = col + prod[:, lane:lane + 128]
    row = jnp.sum(col.T, axis=0, keepdims=True)
    part_out[0:1, :dim] = row
    part_out[0:1, dim:] = jnp.zeros((1, part_out.shape[1] - dim), F32)
    loss = SOFT_CAP * jnp.sum(kl_ref[...]) + jnp.sum(base_ref[0:1, 0:1]) * (1.0 / n_tp)
    part_out[1:2, :] = jnp.full((1, part_out.shape[1]), loss, F32)
    part_out[2:8, :] = jnp.zeros((6, part_out.shape[1]), F32)

    spread = []
    for k, peer in enumerate(peers):
        spread.append(pltpu.make_async_remote_copy(
            src_ref=own, dst_ref=gh_ref.at[:, mine],
            send_sem=send_sem.at[1, k], recv_sem=recv_sem.at[1, k], device_id=(dp, peer), device_id_type=MESH))
        spread.append(pltpu.make_async_remote_copy(
            src_ref=part_out, dst_ref=parts_buf.at[tp],
            send_sem=send_sem.at[2, k], recv_sem=recv_sem.at[2, k], device_id=(dp, peer), device_id_type=MESH))
    for copy in spread:
        copy.start()
    gh_ref[:, mine] = own[...]
    parts_buf[tp] = part_out[...]
    for copy in spread:
        copy.wait()
    share = parts_buf[0]
    for k in range(1, n_tp):
        share = share + parts_buf[k]
    part_ref[...] = share


def reduce_dx(dx, kl, base, hid_t, gain, n_tp):
    tokens, dim = dx.shape
    width = tokens // n_tp
    whole = pl.BlockSpec(memory_space=VMEM)
    return pl.pallas_call(
        functools.partial(dx_kernel, n_tp),
        in_specs=[whole, whole, whole, whole, whole],
        out_specs=[whole, whole],
        out_shape=[
            jax.ShapeDtypeStruct((dim, tokens), F32),
            jax.ShapeDtypeStruct((8, 640), F32),
        ],
        scratch_shapes=[
            VMEM((n_tp - 1, width, dim), F32), VMEM((dim, width), F32),
            VMEM((n_tp, 8, 640), F32), VMEM((8, 640), F32),
            pltpu.SemaphoreType.DMA((3, n_tp - 1)), pltpu.SemaphoreType.DMA((3, n_tp - 1)),
        ],
        compiler_params=pltpu.CompilerParams(collective_id=1, has_side_effects=True, vmem_limit_bytes=24 * 2**20),
        cost_estimate=pl.CostEstimate(flops=50_000_000_000, bytes_accessed=20_000_000, transcendentals=0),
        name="reduce_dx",
    )(dx, kl, base, hid_t, gain)


def add_kernel(*refs):
    a_ref, b_ref, out_ref = refs[-3], refs[-2], refs[-1]
    out_ref[...] = a_ref[...] + b_ref[...]


def add_chunk(start, size, vocab, own, other, out, after):
    dim = own.shape[0]
    tile = math.gcd(math.gcd(start, size), 512)
    off = start // tile
    hbm = pl.BlockSpec(memory_space=pl.ANY)
    block = pl.BlockSpec((dim, tile), lambda j: (0, j))
    lead = (after,) if out is None else (out,)
    return pl.pallas_call(
        add_kernel,
        grid=(size // tile,),
        in_specs=[hbm, block, block],
        out_specs=pl.BlockSpec((dim, tile), lambda j: (0, j + off)),
        out_shape=jax.ShapeDtypeStruct((dim, vocab), F32),
        input_output_aliases={} if out is None else {0: 0},
        compiler_params=pltpu.CompilerParams(dimension_semantics=("arbitrary",), vmem_limit_bytes=16 * 2**20),
        cost_estimate=pl.CostEstimate(flops=dim * size, bytes_accessed=12 * dim * size, transcendentals=0),
        name="add_chunk",
    )(*lead, own, other)


CHUNKS = (GRAD_TILE, 512, 1280, 3584, 3840, 2048, 256, 256)


def solution(mesh):
    n_tp = mesh.shape["tp"]
    swap = [(0, 1), (1, 0)]

    def step(hid_rows, w_final, tab_rows, tea_rows, mask_rows):
        tokens, dim = hid_rows.shape
        vocab = tab_rows.shape[0]
        hid_t = hid_rows.T
        tab_t = tab_rows.T
        mask = mask_rows.reshape(tokens // 128, 128)
        gain = w_final.reshape(1, dim)
        hid_v, hid_own, tea_own = lift(hid_t, tea_rows, n_tp)
        hid_part = lax.ppermute(hid_own, "dp", swap)
        mask_other = lax.ppermute(mask, "dp", swap)
        tea_other = lax.ppermute(tea_own, "dp", swap)
        x, x_t, stat = stats(hid_v, gain, mask, tab_t, tea_rows)
        stu_col, tea_col, base, scale_rows, part, kl, head_g = head(stat, mask, mask_other, x, x_t, tab_t, tea_rows, n_tp)
        dx = None
        own, other = [], []
        start = 0
        for c, size in enumerate(CHUNKS):
            if c:
                part, kl, dx = chunk_grad(start, size, x, x_t, stu_col, tea_col, tab_t, tea_rows, kl, dx, head_g)
            other.append(lax.ppermute(part, "dp", swap))
            own.append(part)
            start += size
        _, kl, dx = chunk_grad(start, SHARED, x, x_t, stu_col, tea_col, tab_t, tea_rows, kl, dx, head_g)
        rows_other = lax.ppermute(scale_rows, "dp", swap)
        parts = [hid_part]
        for k in range(1, n_tp):
            parts.append(lax.ppermute(hid_part, "tp", [(i, (i + k) % n_tp) for i in range(n_tp)]))
        gh_t, share = reduce_dx(dx, kl, base, hid_t, gain, n_tp)
        share_other = lax.ppermute(share, "dp", swap)
        share = share + share_other
        hid_other = join(parts, n_tp)
        term_own = shared_grad(hid_t, gain, scale_rows, tab_t, tea_own)
        term_other = shared_grad(hid_other, gain, rows_other, tab_t, tea_other)
        out = add_chunk(start, SHARED, vocab, term_own, term_other, None, gh_t)
        start = 0
        for size, a, b in zip(CHUNKS, own, other):
            out = add_chunk(start, size, vocab, a, b, out, gh_t)
            start += size
        return share[1, 0], gh_t.T.astype(BF16), share[0, :dim], out.T

    return jax.shard_map(
        step, mesh=mesh,
        in_specs=(P("dp", None), P(None), P("tp", None), P("dp", "tp"), P("dp")),
        out_specs=(P(), P("dp", None), P(None), P("tp", None)), check_vma=False)
```
